32 devices in a mesh: sweep: 1 (over z), data: 4 (over y), ent: 8 (over x, core).
Axes of the slice: x: 4, y: 4, z: 1, core: 2. Of those that a mesh axis runs over, the one named last changes fastest.
The devices are a block of a 4x4x8 slice.
Arguments:
- ent_table: float32 [32768, 400], P(('sweep', 'ent'))
- ent_state: float32 [32768], P(('sweep', 'ent'))
- rel_table: float32 [107, 400], P('sweep')
- head_idx: int32 [8, 8, 8192], P(('sweep', 'ent'), None, 'data')
- tail_idx: int32 [8, 8, 8192], P(('sweep', 'ent'), None, 'data')
- rel_idx: int32 [8, 8, 8192], P(('sweep', 'ent'), None, 'data')
- edge_mask: int32 [8, 8, 8192], P(('sweep', 'ent'), None, 'data')
- neg_idx: int32 [8, 8, 1024], P(('sweep', 'ent'))
Outputs:
- output 1: float32 [32768, 400], P(('sweep', 'ent'))
- output 2: float32 [32768], P(('sweep', 'ent'))
- output 3: float32 [107, 400], P('sweep')
- output 4: float32 [8, 8], P(('sweep', 'ent'))
All inputs are finite; a program needn't handle non-finite values.
Results may differ from the reference program's by a relative error of at most 0.001.
Values are sent between devices in bfloat16 or wider.
A program may use at most 768 MiB of HBM per device.

```python
import jax
import jax.numpy as jnp
from jax import lax

ENT_GROUP = 8
DATA_REPS = 4
ROWS_DEV = 4096
EDGES_DEV = 2048
NEG_COUNT = 1024
EMBED_DIM = 400
REL_COUNT = 107
HOT_IDS = 16

TOTAL_ROWS = ENT_GROUP * ROWS_DEV
BUCKET_EDGES = DATA_REPS * EDGES_DEV
LR_SCALE = 0.2
EPSILON = 1e-8


def draw_edges(edge_key):
    subkeys = jax.random.split(edge_key, 14)
    edge_shape = (ENT_GROUP, ENT_GROUP, BUCKET_EDGES)
    hot_ent = jax.random.randint(subkeys[0], (ENT_GROUP, HOT_IDS), 0, ROWS_DEV)
    hot_rel = jax.random.randint(subkeys[1], (HOT_IDS,), 0, REL_COUNT)
    group_ids = jnp.arange(ENT_GROUP)
    tail_group = (group_ids[:, None] + group_ids[None, :]) % ENT_GROUP
    head_hot = jnp.broadcast_to(hot_ent[:, None, :], (ENT_GROUP, ENT_GROUP, HOT_IDS))
    tail_hot = hot_ent[tail_group]

    def pick_rows(key_use, key_slot, key_uni, hot_rows):
        use_hot = jax.random.randint(key_use, edge_shape, 0, 4) == 0
        hot_slot = jax.random.randint(key_slot, edge_shape, 0, HOT_IDS)
        hot_pick = jnp.take_along_axis(hot_rows, hot_slot, axis=2)
        uni_pick = jax.random.randint(key_uni, edge_shape, 0, ROWS_DEV)
        return jnp.where(use_hot, hot_pick, uni_pick)

    head_idx = pick_rows(subkeys[2], subkeys[3], subkeys[4], head_hot)
    tail_idx = pick_rows(subkeys[5], subkeys[6], subkeys[7], tail_hot)
    rel_use = jax.random.randint(subkeys[8], edge_shape, 0, 2) == 0
    rel_slot = jax.random.randint(subkeys[9], edge_shape, 0, HOT_IDS)
    rel_uni = jax.random.randint(subkeys[10], edge_shape, 0, REL_COUNT)
    rel_idx = jnp.where(rel_use, hot_rel[rel_slot], rel_uni)
    keep_level = jax.random.randint(subkeys[11], (ENT_GROUP, ENT_GROUP, 1), 1, 17)
    edge_mask = (jax.random.randint(subkeys[12], edge_shape, 0, 16) < keep_level).astype(jnp.int32)
    neg_idx = jax.random.randint(subkeys[13], (ENT_GROUP, ENT_GROUP, NEG_COUNT), 0, ROWS_DEV)
    head_idx = head_idx.at[:, :, 0].set(ROWS_DEV - 1)
    tail_idx = tail_idx.at[:, :, 0].set(ROWS_DEV - 1)
    neg_idx = neg_idx.at[:, :, 0].set(ROWS_DEV - 1)
    rel_idx = rel_idx.at[:, :, 0].set(REL_COUNT - 1)
    return head_idx, tail_idx, rel_idx, edge_mask, neg_idx


def setup_inputs(seed: int = 0, part: int = 0) -> dict:
    part_key = jax.random.fold_in(jax.random.key(seed), part)
    subkeys = jax.random.split(part_key, 4)
    emb_scale = EMBED_DIM ** -0.25
    ent_table = jax.random.normal(subkeys[0], (TOTAL_ROWS, EMBED_DIM), jnp.float32) * emb_scale
    ent_state = jax.random.uniform(subkeys[1], (TOTAL_ROWS,), jnp.float32, 0.01, 0.1) * EMBED_DIM ** -0.5
    rel_table = jax.random.normal(subkeys[2], (REL_COUNT, EMBED_DIM), jnp.float32) * 0.7
    head_idx, tail_idx, rel_idx, edge_mask, neg_idx = draw_edges(subkeys[3])
    return {'ent_table': ent_table, 'ent_state': ent_state, 'rel_table': rel_table, 'head_idx': head_idx, 'tail_idx': tail_idx, 'rel_idx': rel_idx, 'edge_mask': edge_mask, 'neg_idx': neg_idx}


def adagrad(param_rows, accum_rows, grad_rows, learn_rate):
    accum_new = accum_rows + jnp.mean(grad_rows * grad_rows, axis=-1)
    step_rows = grad_rows / jnp.sqrt(accum_new + EPSILON)[..., None]
    return param_rows - learn_rate * step_rows, accum_new


def bucket_terms(head_rows, rel_rows, tail_bf, neg_bf, weight):
    half_dim = head_rows.shape[1] // 2
    re_h = head_rows[:, :half_dim]
    im_h = head_rows[:, half_dim:]
    re_r = rel_rows[:, :half_dim]
    im_r = rel_rows[:, half_dim:]
    query_vec = jnp.concatenate([re_h * re_r - im_h * im_r, re_h * im_r + im_h * re_r], axis=1)
    query_bf = query_vec.astype(jnp.bfloat16)
    query_wide = query_bf.astype(jnp.float32)
    tail_wide = tail_bf.astype(jnp.float32)
    pos_score = jnp.sum(query_wide * tail_wide, axis=1)
    neg_score = jnp.dot(query_bf, neg_bf.T, preferred_element_type=jnp.float32)
    top_score = jnp.maximum(jnp.max(neg_score, axis=1), pos_score)
    pos_exp = jnp.exp(pos_score - top_score)
    neg_exp = jnp.exp(neg_score - top_score[:, None])
    exp_total = pos_exp + jnp.sum(neg_exp, axis=1)
    log_total = top_score + jnp.log(exp_total)
    loss_sum = jnp.sum(weight * (log_total - pos_score))
    d_pos = weight * (pos_exp / exp_total - 1.0)
    d_neg = ((weight / exp_total)[:, None] * neg_exp).astype(jnp.bfloat16)
    grad_query = d_pos[:, None] * tail_wide + jnp.dot(d_neg, neg_bf, preferred_element_type=jnp.float32)
    grad_tail = d_pos[:, None] * query_wide
    grad_neg = jnp.dot(d_neg.T, query_bf, preferred_element_type=jnp.float32)
    re_g = grad_query[:, :half_dim]
    im_g = grad_query[:, half_dim:]
    grad_head = jnp.concatenate([re_g * re_r + im_g * im_r, im_g * re_r - re_g * im_r], axis=1)
    grad_rel = jnp.concatenate([re_g * re_h + im_g * im_h, im_g * re_h - re_g * im_h], axis=1)
    return loss_sum, grad_head, grad_rel, grad_tail, grad_neg


def reference(ent_table, ent_state, rel_table, head_idx, tail_idx, rel_idx, edge_mask, neg_idx):
    groups = head_idx.shape[0]
    part_rows = ent_table.shape[0] // groups
    emb_width = ent_table.shape[1]
    rel_rows = rel_table.shape[0]
    bucket_edges = head_idx.shape[2]
    share_edges = bucket_edges // DATA_REPS
    learn_rate = LR_SCALE * emb_width ** -0.25
    pair_ids = jnp.arange(groups * DATA_REPS)

    def one_pass(pass_carry, step_idx):
        table_now, state_now, rel_now, rel_state = pass_carry
        table_bf = table_now.astype(jnp.bfloat16)

        def one_share(grad_acc, pair_id):
            ent_grad, rel_grad = grad_acc
            group_id = pair_id // DATA_REPS
            edge_start = (pair_id % DATA_REPS) * share_edges
            tail_base = ((group_id + step_idx) % groups) * part_rows
            h_ids = lax.dynamic_slice_in_dim(head_idx[group_id, step_idx], edge_start, share_edges) + group_id * part_rows
            t_ids = lax.dynamic_slice_in_dim(tail_idx[group_id, step_idx], edge_start, share_edges) + tail_base
            r_ids = lax.dynamic_slice_in_dim(rel_idx[group_id, step_idx], edge_start, share_edges)
            weight = lax.dynamic_slice_in_dim(edge_mask[group_id, step_idx], edge_start, share_edges).astype(jnp.float32)
            n_ids = neg_idx[group_id, step_idx] + tail_base
            loss_sum, g_head, g_rel, g_tail, g_neg = bucket_terms(table_now[h_ids], rel_now[r_ids], table_bf[t_ids], table_bf[n_ids], weight)
            ent_grad = ent_grad.at[h_ids].add(g_head).at[t_ids].add(g_tail).at[n_ids].add(g_neg)
            rel_grad = rel_grad.at[r_ids].add(g_rel)
            return (ent_grad, rel_grad), loss_sum

        share_init = (jnp.zeros_like(table_now), jnp.zeros_like(rel_now))
        grads_end, share_loss = lax.scan(one_share, share_init, pair_ids)
        ent_grad, rel_grad = grads_end
        table_now, state_now = adagrad(table_now, state_now, ent_grad, learn_rate)
        rel_now, rel_state = adagrad(rel_now, rel_state, rel_grad, learn_rate)
        bucket_loss = share_loss.reshape(groups, DATA_REPS).sum(axis=1) / bucket_edges
        return (table_now, state_now, rel_now, rel_state), bucket_loss

    pass_init = (ent_table, ent_state, rel_table, jnp.zeros((rel_rows,), jnp.float32))
    pass_end, losses = lax.scan(one_pass, pass_init, jnp.arange(groups))
    return pass_end[0], pass_end[1], pass_end[2], losses.T
```

```python
import functools

import jax
import jax.numpy as jnp
from jax import lax
from jax.experimental import pallas as pl
from jax.experimental.pallas import tpu as pltpu
from jax.sharding import PartitionSpec as P

LR_SCALE = 0.2
EPSILON = 1e-8
LANES = 128
HALF = 64
LEFT = 8
BLOCK = 256
CHUNK = 256
UNROLL = 128
REL_PAD = 128
F32 = jnp.float32
BF16 = jnp.bfloat16
VMEM_LIMIT = 60 * 2**20


def wire_rows(rows):
    return 3 * rows + rows // LEFT


def columns_to_tiles(rows):
    half = rows.shape[-1] // 2
    re, im = rows[..., :half], rows[..., half:]
    zero = jnp.zeros((*rows.shape[:-1], HALF - (half - LANES - HALF)), rows.dtype)
    cut = LANES + HALF
    return jnp.concatenate([re[..., :LANES], im[..., :LANES], re[..., LANES:cut], im[..., LANES:cut], re[..., cut:], zero, im[..., cut:], zero], axis=-1)


def tiles_to_wire(rows, size):
    n = rows.shape[0] // size
    blocks = rows.reshape(n, size, 4, LANES)
    main = blocks[:, :, :3].transpose(0, 2, 1, 3).reshape(n, 3 * size, LANES)
    last = blocks[:, :, 3].reshape(n, LEFT, size // LEFT, 2, HALF)[..., :LEFT]
    last = last.transpose(0, 2, 3, 1, 4).reshape(n, size // LEFT, LANES)
    return jnp.concatenate([main, last], axis=1)


def wire_to_columns(wire, size):
    n = wire.shape[0]
    a, b, c = (wire[:, t * size:(t + 1) * size].reshape(n * size, LANES) for t in range(3))
    last = wire[:, 3 * size:wire_rows(size)].reshape(n, size // LEFT, 2, LEFT, LEFT)
    last = last.transpose(0, 3, 1, 2, 4).reshape(n * size, 2, LEFT)
    return jnp.concatenate([a, c[:, :HALF], last[:, 0], b, c[:, HALF:], last[:, 1]], axis=-1)


def each_row(count, body):
    for u in range(count):
        body(u)


def fold_last(tile):
    n = tile.shape[0] // LEFT
    out = tile[:n]
    for k in range(1, LEFT):
        out = out + pltpu.roll(tile[k * n:(k + 1) * n], LEFT * k, 1)
    return out


def unfold_last(packed):
    keep = lax.broadcasted_iota(jnp.int32, packed.shape, 1) % HALF < LEFT
    return [jnp.where(keep, packed if k == 0 else pltpu.roll(packed, LANES - LEFT * k, 1), 0.0) for k in range(LEFT)]


def tiles_of(x):
    return [x[:, t * LANES:(t + 1) * LANES] for t in range(4)]


def times(x, y):
    out = [x[0] * y[0] - x[1] * y[1], x[0] * y[1] + x[1] * y[0]]
    for a, b in zip(x[2:], y[2:]):
        low = lax.broadcasted_iota(jnp.int32, a.shape, 1) < HALF
        a_swap, b_swap = pltpu.roll(a, HALF, 1), pltpu.roll(b, HALF, 1)
        out.append(jnp.where(low, a * b - a_swap * b_swap, a_swap * b + a * b_swap))
    return out


def times_conj(x, y):
    out = [x[0] * y[0] + x[1] * y[1], x[1] * y[0] - x[0] * y[1]]
    for a, b in zip(x[2:], y[2:]):
        low = lax.broadcasted_iota(jnp.int32, a.shape, 1) < HALF
        a_swap, b_swap = pltpu.roll(a, HALF, 1), pltpu.roll(b, HALF, 1)
        out.append(jnp.where(low, a * b + a_swap * b_swap, a * b_swap - a_swap * b))
    return out


def bucket_kernel(bits, edge_ref, count_ref, neg_ref, rel_id_ref, ent_ref, rel_ref, table_ref, tail_out, head_out, rel_out,
                  tail_rows, tail_buf, head_buf, rel_buf, neg_rows, neg_grad, gt_buf, gh_buf, tail_acc0, tail_acc1, head_acc0, head_acc1, rel_acc, loss_acc):
    head_bits, tail_bits = bits
    chunk = CHUNK
    part = chunk // LEFT
    tail_acc, head_acc = (tail_acc0, tail_acc1), (head_acc0, head_acc1)
    count = count_ref[0]
    negs = neg_ref.shape[0]

    def head_of(e):
        return pl.ds(e & (2**head_bits - 1), 1)

    def tail_of(e):
        return pl.ds((e >> head_bits) & (2**tail_bits - 1), 1)

    def widen(n, carry):
        base = pl.multiple_of(n * chunk, chunk)
        for t in range(3):
            tail_rows[pl.ds(base, chunk), t * LANES:(t + 1) * LANES] = table_ref[n, t * chunk:(t + 1) * chunk, :].astype(F32)
        for k, piece in enumerate(unfold_last(table_ref[n, 3 * chunk:, :].astype(F32))):
            tail_rows[pl.ds(base + k * part, part), 3 * LANES:] = piece
        for acc in tail_acc:
            acc[pl.ds(base, chunk), :] = jnp.zeros((chunk, 4 * LANES), F32)
        return carry

    lax.fori_loop(0, table_ref.shape[0], widen, 0)

    def clear(n, carry):
        base = pl.multiple_of(n * UNROLL, UNROLL)
        for acc in head_acc:
            acc[pl.ds(base, UNROLL), :] = jnp.zeros((UNROLL, 4 * LANES), F32)
        return carry

    lax.fori_loop(0, ent_ref.shape[0] // UNROLL, clear, 0)
    neg_grad[...] = jnp.zeros_like(neg_grad)
    rel_acc[...] = jnp.zeros_like(rel_acc)
    loss_acc[...] = jnp.zeros_like(loss_acc)

    def take_negs(n, carry):
        base = pl.multiple_of(n * UNROLL, UNROLL)

        def take(u):
            gt_buf[pl.ds(u, 1), :] = tail_rows[pl.ds(neg_ref[base + u], 1), :]

        each_row(UNROLL, take)
        neg_rows[pl.ds(base, UNROLL), :] = gt_buf[:UNROLL, :].astype(BF16)
        return carry

    lax.fori_loop(0, negs // UNROLL, take_negs, 0)

    def block(n, carry):
        base = n * BLOCK

        def take(u):
            e = edge_ref[base + u]
            head_buf[pl.ds(u, 1), :] = ent_ref[head_of(e), :]
            tail_buf[pl.ds(u, 1), :] = tail_rows[tail_of(e), :]
            rel_buf[pl.ds(u, 1), :] = rel_ref[pl.ds(e >> (head_bits + tail_bits), 1), :]

        each_row(BLOCK, take)
        hot = lax.broadcasted_iota(jnp.int32, (REL_PAD, BLOCK), 0) == rel_id_ref[pl.ds(n, 1), :]
        hot = jnp.where(hot, 1.0, 0.0).astype(BF16)
        weight = jnp.where(lax.broadcasted_iota(jnp.int32, (BLOCK, 1), 0) + base < count, 1.0, 0.0)
        head, rel, tail = tiles_of(head_buf[...]), tiles_of(rel_buf[...]), tiles_of(tail_buf[...])
        query_bf = [t.astype(BF16) for t in times(head, rel)]
        query = [t.astype(F32) for t in query_bf]
        pos = jnp.sum(query[0] * tail[0] + query[1] * tail[1] + query[2] * tail[2] + query[3] * tail[3], axis=1, keepdims=True)
        query_bf = jnp.concatenate(query_bf, axis=1)
        score = lax.dot_general(query_bf, neg_rows[...], (((1,), (1,)), ((), ())), preferred_element_type=F32)
        top = jnp.maximum(jnp.max(score, axis=1, keepdims=True), pos)
        pos_exp = jnp.exp(pos - top)
        neg_exp = jnp.exp(score - top)
        total = pos_exp + jnp.sum(neg_exp, axis=1, keepdims=True)
        loss_acc[...] += jnp.sum(weight * (top + jnp.log(total) - pos), axis=0, keepdims=True)
        d_pos = weight * (pos_exp / total - 1.0)
        d_neg = ((weight / total) * neg_exp).astype(BF16)
        grad_q = lax.dot_general(d_neg, neg_rows[...], (((1,), (0,)), ((), ())), preferred_element_type=F32)
        neg_grad[...] += lax.dot_general(d_neg, query_bf, (((0,), (0,)), ((), ())), preferred_element_type=F32)
        grad_q = [d_pos * a + b for a, b in zip(tail, tiles_of(grad_q))]
        for t in range(4):
            gt_buf[:, t * LANES:(t + 1) * LANES] = d_pos * query[t]
        for t, grad in enumerate(times_conj(grad_q, rel)):
            gh_buf[:, t * LANES:(t + 1) * LANES] = grad
        rest = jnp.concatenate(times_conj(grad_q, head), axis=1)
        rel_sum = rel_acc[...]
        for _ in range(3):
            piece = rest.astype(BF16)
            rest = rest - piece.astype(F32)
            rel_sum = rel_sum + lax.dot_general(hot, piece, (((1,), (0,)), ((), ())), preferred_element_type=F32)
        rel_acc[...] = rel_sum

        def put(pair):
            for lane in range(2):
                u = 2 * pair + lane
                e = edge_ref[base + u]
                head_acc[lane][head_of(e), :] += gh_buf[pl.ds(u, 1), :]
                tail_acc[lane][tail_of(e), :] += gt_buf[pl.ds(u, 1), :]

        each_row(BLOCK // 2, put)
        return carry

    lax.fori_loop(0, pl.cdiv(count, BLOCK), block, 0)

    def put_negs(n, carry):
        base = pl.multiple_of(n * UNROLL, UNROLL)

        def put(pair):
            for lane in range(2):
                u = base + 2 * pair + lane
                tail_acc[lane][pl.ds(neg_ref[u], 1), :] += neg_grad[pl.ds(u, 1), :]

        each_row(UNROLL // 2, put)
        return carry

    lax.fori_loop(0, negs // UNROLL, put_negs, 0)

    def emit(out_ref, acc):
        def one(n, carry):
            base = pl.multiple_of(n * chunk, chunk)
            for t in range(4):
                cols = slice(t * LANES, (t + 1) * LANES)
                rows = acc[0][pl.ds(base, chunk), cols] + acc[1][pl.ds(base, chunk), cols]
                if t < 3:
                    out_ref[n, t * chunk:(t + 1) * chunk, :] = rows
                else:
                    out_ref[n, 3 * chunk:, :] = fold_last(rows)
            return carry

        lax.fori_loop(0, out_ref.shape[0], one, 0)

    emit(tail_out, tail_acc)
    emit(head_out, head_acc)
    group = lax.axis_index('ent') // 2 * 2 + lax.axis_index('data') // 2
    row = lax.broadcasted_iota(jnp.int32, (REL_PAD, LANES), 0)
    lane = lax.broadcasted_iota(jnp.int32, (REL_PAD, LANES), 1)
    loss = jnp.where(lane == group, loss_acc[...], 0.0)
    for t in range(3):
        rows = rel_acc[:, t * LANES:(t + 1) * LANES]
        rel_out[t * REL_PAD:(t + 1) * REL_PAD, :] = jnp.where(row == REL_PAD - 1, loss, rows) if t == 0 else rows
    rel_out[3 * REL_PAD:, :] = fold_last(rel_acc[:, 3 * LANES:])


def bucket_call(bits, edges, count, neg, rel_ids, ent, rel, table):
    smem, vmem = pl.BlockSpec(memory_space=pltpu.SMEM), pl.BlockSpec(memory_space=pltpu.VMEM)
    rows, negs, chunks = ent.shape[0], neg.shape[0], table.shape[0]
    width = 4 * LANES
    wire = wire_rows(CHUNK)
    block = pltpu.VMEM((BLOCK, width), F32)
    return pl.pallas_call(
        functools.partial(bucket_kernel, bits),
        out_shape=(
            jax.ShapeDtypeStruct((chunks, wire, LANES), F32),
            jax.ShapeDtypeStruct((rows // CHUNK, wire, LANES), F32),
            jax.ShapeDtypeStruct((wire_rows(REL_PAD), LANES), F32),
        ),
        in_specs=[smem, smem, smem, vmem, vmem, vmem, vmem],
        out_specs=(vmem, vmem, vmem),
        scratch_shapes=[
            pltpu.VMEM((chunks * CHUNK, width), F32), block, block, block,
            pltpu.VMEM((negs, width), BF16), pltpu.VMEM((negs, width), F32), block, block,
            pltpu.VMEM((chunks * CHUNK, width), F32), pltpu.VMEM((chunks * CHUNK, width), F32),
            pltpu.VMEM((rows, width), F32), pltpu.VMEM((rows, width), F32),
            pltpu.VMEM((REL_PAD, width), F32), pltpu.VMEM((1, 1), F32),
        ],
        compiler_params=pltpu.CompilerParams(vmem_limit_bytes=VMEM_LIMIT),
        name='bucket',
    )(edges, count, neg, rel_ids, ent, rel, table)


def adagrad(rows, state, grad, mean_of, learn_rate):
    square = grad[0] * grad[0] + grad[1] * grad[1] + grad[2] * grad[2] + grad[3] * grad[3]
    state = state + jnp.sum(square, axis=1, keepdims=True) / mean_of
    root = jnp.sqrt(state + EPSILON)
    return [r - learn_rate * (g / root) for r, g in zip(rows, grad)], state


def exchange_kernel(cfg, *refs):
    step, groups, chunks, emb_width, last = cfg
    (tail_ref, head_ref, rel_grad_ref, ent_ref, state_ref, rel_ref, rel_state_ref) = refs[:7]
    if last:
        ent_wire, rel_out, loss_out = refs[7:10]
        rest = refs[10:]
    else:
        ent_out, state_out, rel_out, rel_state_out, loss_out, table = refs[7:13]
        rest = refs[13:]
    (own, from_core, from_y, from_group, rel_sum, rel_from, send_buf,
     own_sem, core_send, core_recv, y_send, y_recv, group_send, group_recv, rel_send, rel_recv, out_send, out_recv) = rest
    learn_rate = LR_SCALE * emb_width ** -0.25
    chunk = CHUNK
    part = chunk // LEFT
    y, ent = lax.axis_index('data'), lax.axis_index('ent')
    x, core = ent // 2, ent % 2
    top, bot = y // 2, y % 2
    mine = 2 * x + top
    x_size = groups // 2

    def place(group, low, c):
        return {'data': 2 * (group % 2) + low, 'ent': 2 * (group // 2) + c}

    def at(dy, dx, c):
        return {'data': dy, 'ent': 2 * dx + c}

    def turned(shift):
        return (bot + shift) % 2

    other_core = at(y, x, 1 - core)
    other_y = at(2 * top + 1 - bot, x, core)
    rel_peers = (other_core, other_y, at(3 - y, x, core), at(y, x + 1 - 2 * (x % 2), core), at(y, x_size - 1 - x, core))
    grad_to = place((mine + step) % groups, turned(step), core)
    grad_from = place((mine + groups - step) % groups, turned(step), core)
    nxt = step + 1
    table_to = place((mine + groups - nxt) % groups, turned(nxt), core)
    table_from = place((mine + nxt) % groups, turned(nxt), core)
    peers = list(rel_peers)
    if step:
        peers += [grad_to, grad_from]
    if last:
        for turn in range(4):
            peers.append(at((y + turn) % 4, x, top))
        senders = [at((2 * core + d), x, c) for d in range(2) for c in range(2)]
        peers += senders
    else:
        peers += [table_to, table_from]
    barrier = pltpu.get_barrier_semaphore()
    for peer in peers:
        pl.semaphore_signal(barrier, inc=1, device_id=peer, device_id_type=pl.DeviceIdType.MESH)
    pl.semaphore_wait(barrier, len(peers))

    def remote(src, dst, send, recv, peer):
        return pltpu.make_async_remote_copy(src_ref=src, dst_ref=dst, send_sem=send, recv_sem=recv, device_id=peer, device_id_type=pl.DeviceIdType.MESH)

    keep = turned(step)
    pending = []

    def start(copy):
        copy.start()
        pending.append(copy)
        return copy

    shards = [(1 - keep, k) for k in range(chunks)] + [(keep, k) for k in range(chunks)]
    loads, cores = [], []
    rel_copies = [start(remote(rel_grad_ref, rel_from.at[0], rel_send.at[0], rel_recv.at[0], rel_peers[0]))]
    for n, (low, k) in enumerate(shards):
        cores.append(start(remote(tail_ref.at[(low * 2 + 1 - core) * chunks + k], from_core.at[n], core_send.at[n], core_recv.at[n], other_core)))
        load = pltpu.make_async_copy(tail_ref.at[(low * 2 + core) * chunks + k], own.at[n], own_sem.at[n])
        load.start()
        loads.append(load)

    def rel_step(n):
        rel_copies[n].wait_recv()
        rel_sum[n] = (rel_grad_ref[...] if n == 0 else rel_sum[n - 1]) + rel_from[n]
        if n + 1 < len(rel_peers):
            rel_copies.append(start(remote(rel_sum.at[n], rel_from.at[n + 1], rel_send.at[n + 1], rel_recv.at[n + 1], rel_peers[n + 1])))

    rel_step(0)
    ys = []
    for k in range(chunks):
        loads[k].wait()
        cores[k].wait_recv()
        own[k] = own[k] + from_core[k]
        ys.append(start(remote(own.at[k], from_y.at[k], y_send.at[k], y_recv.at[k], other_y)))
    rel_step(1)
    for k in range(chunks, 2 * chunks):
        loads[k].wait()
        cores[k].wait_recv()
        own[k] = own[k] + from_core[k]
    rel_step(2)
    gs, outs, forwards, crosses = [], [], [], []

    def stage_group(k):
        ys[k].wait_recv()
        own[chunks + k] = own[chunks + k] + from_y[k]
        if step:
            gs.append(start(remote(own.at[chunks + k], from_group.at[k], group_send.at[k], group_recv.at[k], grad_to)))

    def stage_update(k):
        if step:
            gs[k].wait_recv()
        total = from_group if step else own
        base = k if step else chunks + k
        grad = [total[base, t * chunk:(t + 1) * chunk, :] + head_ref[k, t * chunk:(t + 1) * chunk, :] for t in range(3)]
        grad.append(jnp.concatenate(unfold_last(total[base, 3 * chunk:, :] + head_ref[k, 3 * chunk:, :]), axis=0))
        span = slice(k * chunk, (k + 1) * chunk)
        rows, state = adagrad(tiles_of(ent_ref[span, :]), state_ref[span, :], grad, emb_width, learn_rate)
        wire = rows[:3] + [fold_last(rows[3])]
        if last:
            lane = lax.broadcasted_iota(jnp.int32, (chunk, LANES), 1)
            wire.append(fold_last(jnp.where(lane < 1, state, 0.0)))
        else:
            for t in range(4):
                ent_out[span, t * LANES:(t + 1) * LANES] = rows[t]
            state_out[span, :] = state
        offset = 0
        for piece in wire:
            send_buf[k, offset:offset + piece.shape[0], :] = piece.astype(send_buf.dtype)
            offset += piece.shape[0]
        slot = (bot * 2 + core) * chunks + k
        if last:
            for turn in range(1, 4):
                start(remote(send_buf.at[k], ent_wire.at[slot], out_send.at[turn * chunks + k], out_recv.at[slot], at((y + turn) % 4, x, top)))

            @pl.when(core == top)
            def _():
                pltpu.make_async_copy(send_buf.at[k], ent_wire.at[slot], out_recv.at[slot]).start()

            @pl.when(core != top)
            def _():
                remote(send_buf.at[k], ent_wire.at[slot], out_send.at[k], out_recv.at[slot], other_core).start()
        else:
            outs.append(start(remote(send_buf.at[k], table.at[slot], out_send.at[k], out_recv.at[k], table_to)))

    def forward(n, low, k, peer):
        slot = (low * 2 + core) * chunks + k
        return start(remote(table.at[slot], table.at[slot], out_send.at[n * chunks + k], out_recv.at[n * chunks + k], peer))

    def stage_forward(k):
        if last:
            return
        outs[k].wait_recv()
        forwards.append(forward(1, turned(nxt), k, other_y))
        crosses.append(forward(2, turned(nxt), k, other_core))

    def stage_cross(k):
        if last:
            return
        forwards[k].wait_recv()
        crosses.append(forward(3, 1 - turned(nxt), k, other_core))

    stages = (stage_group, stage_update, stage_forward, stage_cross)
    for tick in range(chunks + len(stages) - 1):
        for lag, stage in enumerate(stages):
            if 0 <= tick - lag < chunks:
                stage(tick - lag)
        if tick in (0, 1):
            rel_step(3 + tick)

    summed = rel_sum[len(rel_peers) - 1]
    rel_grad = [summed[t * REL_PAD:(t + 1) * REL_PAD] for t in range(3)] + [jnp.concatenate(unfold_last(summed[3 * REL_PAD:]), axis=0)]
    loss_out[...] = rel_grad[0][REL_PAD - 1:, :]
    row = lax.broadcasted_iota(jnp.int32, (REL_PAD, LANES), 0)
    rel_grad[0] = jnp.where(row < REL_PAD - 1, rel_grad[0], 0.0)
    rel_rows, rel_state = adagrad(tiles_of(rel_ref[...]), rel_state_ref[...], rel_grad, emb_width, learn_rate)
    for t in range(4):
        rel_out[:, t * LANES:(t + 1) * LANES] = rel_rows[t]
    if not last:
        rel_state_out[...] = rel_state

    if last:
        for slot in range(4 * chunks):
            remote(ent_wire.at[slot], ent_wire.at[slot], out_send.at[0], out_recv.at[slot], other_core).wait_recv()

        @pl.when(core != top)
        def _():
            for k in range(chunks):
                remote(send_buf.at[k], send_buf.at[k], out_send.at[k], out_recv.at[k], other_core).wait_send()
    else:
        for copy in crosses:
            copy.wait_recv()
    for copy in pending:
        copy.wait_send()


def exchange_call(step, groups, emb_width, tail, head, rel_grad, ent, state, rel, rel_state):
    vmem, hbm = pl.BlockSpec(memory_space=pltpu.VMEM), pl.BlockSpec(memory_space=pl.ANY)
    chunks = head.shape[0]
    wire = wire_rows(CHUNK)
    last = step == groups - 1
    like = lambda x: jax.ShapeDtypeStruct(x.shape, x.dtype)
    loss = jax.ShapeDtypeStruct((1, LANES), F32)
    out_wire = wire + (CHUNK // LEFT if last else 0)
    out_type = F32 if last else BF16
    gathered = jax.ShapeDtypeStruct((4 * chunks, out_wire, LANES), out_type)
    out_shape = (gathered, like(rel), loss) if last else (like(ent), like(state), like(rel), like(rel_state), loss, gathered)
    sems = lambda n: pltpu.SemaphoreType.DMA((n,))
    return pl.pallas_call(
        functools.partial(exchange_kernel, (step, groups, chunks, emb_width, last)),
        out_shape=out_shape,
        in_specs=[hbm] + [vmem] * 6,
        out_specs=tuple(vmem for _ in out_shape),
        scratch_shapes=[
            pltpu.VMEM((2 * chunks, wire, LANES), F32), pltpu.VMEM((2 * chunks, wire, LANES), F32),
            pltpu.VMEM((chunks, wire, LANES), F32), pltpu.VMEM((chunks, wire, LANES), F32),
            pltpu.VMEM((5, *rel_grad.shape), F32), pltpu.VMEM((5, *rel_grad.shape), F32),
            pltpu.VMEM((chunks, out_wire, LANES), out_type),
            sems(2 * chunks), sems(2 * chunks), sems(2 * chunks), sems(chunks), sems(chunks), sems(chunks), sems(chunks),
            sems(5), sems(5), sems(4 * chunks), sems(4 * chunks),
        ],
        compiler_params=pltpu.CompilerParams(vmem_limit_bytes=VMEM_LIMIT, collective_id=step, has_side_effects=True),
        name='exchange',
    )(tail, head, rel_grad, ent, state, rel, rel_state)


def solution(mesh):
    groups = mesh.shape['ent']
    data_reps = mesh.shape['data']
    row_spec = P(('sweep', 'ent'), None)
    edge_spec = P(('sweep', 'ent'), None, 'data')

    def device_fn(ent_table, ent_state, rel_table, head_idx, tail_idx, rel_idx, edge_mask, neg_idx):
        part_rows, emb_width = ent_table.shape
        rel_rows = rel_table.shape[0]
        bucket_edges = head_idx.shape[2] * data_reps
        shard = part_rows // 4
        tail_bits = (part_rows - 1).bit_length()
        head_bits = (shard - 1).bit_length()
        spare = 2**(REL_PAD - 1).bit_length() - 1
        y, ent = lax.axis_index('data'), lax.axis_index('ent')
        core, top, bot = ent % 2, y // 2, y % 2
        is_home = core == top

        packed = head_idx[0] | (tail_idx[0] << tail_bits) | (rel_idx[0] << (2 * tail_bits))
        packed = jnp.where(edge_mask[0] > 0, packed, spare << (2 * tail_bits))
        packed = lax.all_gather(packed, 'data', axis=1, tiled=True)
        own_tiles = columns_to_tiles(ent_table)
        own_table = tiles_to_wire(own_tiles.astype(BF16), CHUNK)
        to_core = lambda c: (lax.dynamic_slice_in_dim(own_tiles, (2 * bot + c) * shard, shard), lax.dynamic_slice_in_dim(ent_state, (2 * bot + c) * shard, shard))
        away = [(d * groups + 2 * (n // 2) + d // 2, d * groups + 2 * (n // 2) + 1 - d // 2) for d in range(data_reps) for n in range(0, groups, 2)]
        other_ent, other_state = to_core(1 - core)
        mine_ent, mine_state = to_core(core)
        pick = lambda here, sent: jnp.where(is_home, here, lax.ppermute(sent, ('data', 'ent'), away))
        packed = pick(packed, packed)
        neg = pick(neg_idx[0], neg_idx[0])
        table = pick(own_table, own_table)
        ent_now = pick(mine_ent, other_ent)
        state_now = pick(mine_state, other_state)[:, None]

        is_mine = ((packed >> head_bits) & 3 == 2 * bot + core) & (packed >> (2 * tail_bits) != spare)
        local = (packed & (shard - 1)) | (packed >> tail_bits << head_bits)
        keys = lax.sort(jnp.where(is_mine, local, spare << (head_bits + tail_bits)), dimension=1)
        counts = jnp.sum(is_mine, axis=1, dtype=jnp.int32)
        rel_ids = (keys >> (head_bits + tail_bits)).reshape(groups, -1, BLOCK)

        rel_now = jnp.pad(columns_to_tiles(rel_table), ((0, REL_PAD - rel_rows), (0, 0)))
        rel_state = jnp.zeros((REL_PAD, 1), F32)
        losses = []
        for step in range(groups):
            tail, head, rel_grad = bucket_call((head_bits, tail_bits), keys[step], counts[step:step + 1], neg[step], rel_ids[step], ent_now, rel_now, table)
            out = exchange_call(step, groups, emb_width, tail, head, rel_grad, ent_now, state_now, rel_now, rel_state)
            if step + 1 < groups:
                ent_now, state_now, rel_now, rel_state, loss, table = out
            else:
                wire, rel_now, loss = out
            losses.append(loss)
        ent_out = wire_to_columns(wire, CHUNK)
        state_out = wire[:, wire_rows(CHUNK):, :HALF:LEFT].transpose(0, 2, 1).reshape(part_rows)
        half = emb_width // 2
        cut = LANES + HALF
        rel_out = jnp.concatenate([rel_now[:, :LANES], rel_now[:, 2 * LANES:cut + LANES], rel_now[:, 3 * LANES:3 * LANES + half - cut],
                                   rel_now[:, LANES:2 * LANES], rel_now[:, cut + LANES:3 * LANES], rel_now[:, 3 * LANES + HALF:3 * LANES + HALF + half - cut]], axis=1)[:rel_rows]
        loss_rows = jnp.concatenate(losses, axis=0) / bucket_edges
        bucket_loss = lax.dynamic_slice_in_dim(loss_rows, ent, 1, axis=1).reshape(1, groups)
        return ent_out, state_out, rel_out, bucket_loss

    return jax.shard_map(device_fn, mesh=mesh, in_specs=(row_spec, P(('sweep', 'ent')), P('sweep', None), edge_spec, edge_spec, edge_spec, edge_spec, P(('sweep', 'ent'), None, None)), out_specs=(row_spec, P(('sweep', 'ent')), P('sweep', None), row_spec), check_vma=False)
```

```python
import functools

import jax
import jax.numpy as jnp
from jax import lax
from jax.experimental import pallas as pl
from jax.experimental.pallas import tpu as pltpu
from jax.sharding import PartitionSpec as P

LR_SCALE = 0.2
EPSILON = 1e-8
LANES = 128
HALF = 64
LEFT = 8
BLOCK = 256
CHUNK = 128
UNROLL = 128
STRIP = 32
REL_PAD = 128
TILES = range(4)
ROW_COL, ROW_ROW, COL_COL = (((1,), (0,)), ((1,), (1,)), ((0,), (0,)))
F32 = jnp.float32
BF16 = jnp.bfloat16
VMEM_LIMIT = 60 * 2**20


def wire_rows(rows):
    return 3 * rows + rows // LEFT


def columns_to_tiles(x):
    lane = lax.broadcasted_iota(jnp.int32, (x.shape[0], LANES), 1)
    end = x.shape[1] - 3 * LANES
    t0, t1, t2 = (x[:, band(t, LANES)] for t in TILES[:-1])
    t3 = jnp.concatenate([x[:, 3 * LANES:], jnp.zeros((x.shape[0], LANES - end), x.dtype)], axis=1)
    im = x.shape[1] // 2 - LANES
    cut = LANES - im
    b = jnp.where(lane < cut, pltpu.roll(t1, cut, 1), pltpu.roll(t2, cut, 1))
    c = jnp.where(lane < HALF, t1, jnp.where(lane < LANES - LEFT, pltpu.roll(t2, LANES - LEFT, 1), pltpu.roll(t3, LANES - LEFT, 1)))
    low, high = pltpu.roll(t1, HALF, 1), pltpu.roll(t3, cut, 1)
    d = jnp.where(lane < LEFT, low, jnp.where((lane >= HALF) & (lane < HALF + LEFT), high, 0.0))
    return [t0, b, c, d]


def tiles_to_columns(tiles, width):
    a, b, c, d = tiles
    lane = lax.broadcasted_iota(jnp.int32, a.shape, 1)
    im = width // 2 - LANES
    b, c, low, high = pltpu.roll(b, im, 1), pltpu.roll(c, LEFT, 1), pltpu.roll(d, HALF, 1), pltpu.roll(d, im, 1)
    t1 = jnp.where(lane < HALF, tiles[2], jnp.where(lane < im, low, b))
    t2 = jnp.where(lane < im, b, c)
    t3 = jnp.where(lane < LEFT, c, high)
    return jnp.concatenate([a, t1, t2, t3[:, :width - 3 * LANES]], axis=1)


def each_row(count, body):
    for u in range(count):
        body(u)


def band(n, size):
    return slice(n * size, (n + 1) * size)


def where_here():
    y, ent = lax.axis_index('data'), lax.axis_index('ent')
    return y, ent // 2, ent % 2, y // 2, y % 2


def fold_last(tile):
    n = tile.shape[0] // LEFT
    out = tile[:n]
    for k in range(1, LEFT):
        out = out + pltpu.roll(tile[band(k, n)], LEFT * k, 1)
    return out


def unfold_last(packed):
    keep = lax.broadcasted_iota(jnp.int32, packed.shape, 1) % HALF < LEFT
    return [jnp.where(keep, packed if k == 0 else pltpu.roll(packed, LANES - LEFT * k, 1), 0.0) for k in range(LEFT)]


def tiles_of(x):
    return [x[:, band(t, LANES)] for t in TILES]


def times(x, y):
    out = [x[0] * y[0] - x[1] * y[1], x[0] * y[1] + x[1] * y[0]]
    for a, b in zip(x[2:], y[2:]):
        low = lax.broadcasted_iota(jnp.int32, a.shape, 1) < HALF
        a_swap, b_swap = pltpu.roll(a, HALF, 1), pltpu.roll(b, HALF, 1)
        out.append(jnp.where(low, a * b - a_swap * b_swap, a_swap * b + a * b_swap))
    return out


def times_conj(x, y):
    out = [x[0] * y[0] + x[1] * y[1], x[1] * y[0] - x[0] * y[1]]
    for a, b in zip(x[2:], y[2:]):
        low = lax.broadcasted_iota(jnp.int32, a.shape, 1) < HALF
        a_swap, b_swap = pltpu.roll(a, HALF, 1), pltpu.roll(b, HALF, 1)
        out.append(jnp.where(low, a * b + a_swap * b_swap, a * b_swap - a_swap * b))
    return out


def tiles_at(ref, row, rows):
    block = ref[pl.ds(row * 4, rows * 4), :].reshape(rows // 8, 32, LANES)
    return [block[:, 8 * t:8 * t + 8].reshape(rows, LANES) for t in TILES]


def stack_tiles(tiles):
    rows = tiles[0].shape[0]
    return jnp.concatenate([t.reshape(rows // 8, 8, LANES) for t in tiles], axis=1).reshape(rows * 4, LANES)


def row_at(address):
    return pl.ds(address, 4, stride=8)


def row_address(row):
    return (row >> 3 << 5) | (row & 7)


def in_three(x):
    pieces = []
    for _ in range(3):
        piece = x.astype(BF16)
        pieces.append(piece)
        x = x - piece.astype(F32)
    return pieces


def dot(x, y, dims):
    return lax.dot_general(x, y, (dims, ((), ())), preferred_element_type=F32)


def bucket_kernel(cfg, edges_hbm, count_ref, negs_hbm, rel_ids_hbm, ent_ref, rel_ref, table_ref, tail_out, head_out, rel_out,
                  tail_rows, head_next, tail_next, head_buf, tail_buf, gh_last, gt_last, rel_buf, query_buf, pos_buf, score_buf, d_neg_buf, grad_buf, piece_buf,
                  neg_rows, neg_grad, rel_three, tail_acc0, tail_acc1, head_acc0, head_acc1, rel_acc, loss_acc,
                  edge_ref, neg_ref, rel_id_ref, sems):
    step, tail_bits = cfg
    chunk = CHUNK
    part = chunk // LEFT
    tail_acc, head_acc = (tail_acc0, tail_acc1), (head_acc0, head_acc1)
    count = count_ref[step]
    negs = neg_ref.shape[0]
    loads = [
        pltpu.make_async_copy(negs_hbm.at[step, 0], neg_ref, sems.at[0]),
        pltpu.make_async_copy(edges_hbm.at[step, 0], edge_ref, sems.at[1]),
        pltpu.make_async_copy(rel_ids_hbm.at[step], rel_id_ref, sems.at[2]),
    ]
    for load in loads:
        load.start()

    def head_of(e):
        return row_at(e >> tail_bits)

    def tail_of(e):
        return row_at(e & (2**tail_bits - 1))

    def widen(n, carry):
        base = pl.multiple_of(n * chunk, chunk)
        tiles = [table_ref[n, band(t, chunk), :].astype(F32) for t in TILES[:-1]]
        tiles.append(jnp.concatenate(unfold_last(table_ref[n, 3 * chunk:, :].astype(F32)), axis=0))
        tail_rows[pl.ds(base * 4, chunk * 4), :] = stack_tiles(tiles)
        for acc in tail_acc:
            acc[pl.ds(base * 4, chunk * 4), :] = jnp.zeros((chunk * 4, LANES), F32)
        return carry

    lax.fori_loop(0, table_ref.shape[0], widen, 0)

    def clear(n, carry):
        base = pl.multiple_of(n * chunk * 4, chunk * 4)
        for acc in head_acc:
            acc[pl.ds(base, chunk * 4), :] = jnp.zeros((chunk * 4, LANES), F32)
        return carry

    lax.fori_loop(0, head_out.shape[0], clear, 0)
    neg_grad[...] = jnp.zeros_like(neg_grad)
    gh_last[...] = jnp.zeros_like(gh_last)
    gt_last[...] = jnp.zeros_like(gt_last)
    rel_acc[...] = jnp.zeros_like(rel_acc)
    loss_acc[...] = jnp.zeros_like(loss_acc)
    for n, piece in enumerate(in_three(rel_ref[...])):
        rel_three[band(n, REL_PAD), :] = piece
    for load in loads:
        load.wait()

    def take_negs(n, carry):
        base = pl.multiple_of(n * UNROLL, UNROLL)

        def take(u):
            head_buf[row_at(row_address(u)), :] = tail_rows[row_at(neg_ref[base + u]), :]

        each_row(UNROLL, take)
        for t, tile in enumerate(tiles_at(head_buf, 0, UNROLL)):
            neg_rows[pl.ds(base, UNROLL), band(t, LANES)] = tile.astype(BF16)
        return carry

    lax.fori_loop(0, negs // UNROLL, take_negs, 0)

    def take_edges(base):
        def take(u):
            e = edge_ref[base + u]
            head_next[row_at(row_address(u)), :] = ent_ref[head_of(e), :]
            tail_next[row_at(row_address(u)), :] = tail_rows[tail_of(e), :]

        return take

    def put_edges(base):
        def put(pair):
            for lane in range(2):
                u = 2 * pair + lane
                e = edge_ref[base + u]
                row = row_at(row_address(u))
                head_acc[lane][head_of(e), :] += gh_last[row, :]
                tail_acc[lane][tail_of(e), :] += gt_last[row, :]

        return put

    each_row(BLOCK, take_edges(BLOCK))
    spans = [slice(r, r + STRIP) for r in range(0, BLOCK, STRIP)]

    def block(n, carry):
        base = pl.multiple_of(n * BLOCK, BLOCK)
        hot = lax.broadcasted_iota(jnp.int32, (REL_PAD, BLOCK), 0) == rel_id_ref[pl.ds(n, 1), :]
        hot = jnp.where(hot, 1.0, 0.0).astype(BF16)
        rel_buf[...] = dot(jnp.concatenate([hot] * 3, axis=0), rel_three[...], COL_COL)
        for span in spans:
            head, tail, rel = tiles_at(head_next, span.start, STRIP), tiles_at(tail_next, span.start, STRIP), tiles_of(rel_buf[span, :])
            wide = slice(4 * span.start, 4 * span.stop)
            head_buf[wide, :], tail_buf[wide, :] = stack_tiles(head), stack_tiles(tail)
            total = None
            for t, q in enumerate(times(head, rel)):
                q = q.astype(BF16)
                query_buf[span, band(t, LANES)] = q
                product = q.astype(F32) * tail[t]
                total = product if total is None else total + product
            pos_buf[span, :] = jnp.sum(total, axis=1, keepdims=True)
        each_row(BLOCK, take_edges(base + 2 * BLOCK))
        each_row(BLOCK // 2, put_edges(base))
        score_buf[...] = dot(query_buf[...], neg_rows[...], ROW_ROW)
        for span in spans:
            weight = jnp.where(lax.broadcasted_iota(jnp.int32, (STRIP, 1), 0) + (base + span.start) < count, 1.0, 0.0)
            score, pos = score_buf[span, :], pos_buf[span, :]
            top = jnp.maximum(jnp.max(score, axis=1, keepdims=True), pos)
            pos_exp = jnp.exp(pos - top)
            neg_exp = jnp.exp(score - top)
            total = pos_exp + jnp.sum(neg_exp, axis=1, keepdims=True)
            loss_acc[...] += jnp.sum(weight * (top + jnp.log(total) - pos), axis=0, keepdims=True)
            pos_buf[span, :] = weight * (pos_exp / total - 1.0)
            d_neg_buf[span, :] = ((weight / total) * neg_exp).astype(BF16)
        grad_buf[...] = dot(d_neg_buf[...], neg_rows[...], ROW_COL)
        neg_grad[...] += dot(d_neg_buf[...], query_buf[...], COL_COL)
        for span in spans:
            wide = slice(4 * span.start, 4 * span.stop)
            d_pos = pos_buf[span, :]
            tail, rel = tiles_at(tail_buf, span.start, STRIP), tiles_of(rel_buf[span, :])
            grad_q = [d_pos * x + y for x, y in zip(tail, tiles_of(grad_buf[span, :]))]
            gt_last[wide, :] = stack_tiles([d_pos * q.astype(F32) for q in tiles_of(query_buf[span, :])])
            gh_last[wide, :] = stack_tiles(times_conj(grad_q, rel))
            for t, grad in enumerate(times_conj(grad_q, tiles_at(head_buf, span.start, STRIP))):
                for k, piece in enumerate(in_three(grad)):
                    piece_buf[k * BLOCK + span.start:k * BLOCK + span.stop, band(t, LANES)] = piece
        rel_acc[...] += dot(jnp.concatenate([hot] * 3, axis=1), piece_buf[...], ROW_COL)
        return carry

    blocks = pl.cdiv(count, BLOCK)
    lax.fori_loop(0, blocks, block, 0)
    each_row(BLOCK // 2, put_edges(pl.multiple_of(blocks * BLOCK, BLOCK)))

    def put_negs(n, carry):
        base = pl.multiple_of(n * UNROLL, UNROLL)
        gt_last[:4 * UNROLL, :] = stack_tiles(tiles_of(neg_grad[pl.ds(base, UNROLL), :]))

        def put(pair):
            for lane in range(2):
                u = 2 * pair + lane
                tail_acc[lane][row_at(neg_ref[base + u]), :] += gt_last[row_at(row_address(u)), :]

        each_row(UNROLL // 2, put)
        return carry

    lax.fori_loop(0, negs // UNROLL, put_negs, 0)

    def emit(out_ref, acc):
        def one(n, carry):
            base = pl.multiple_of(n * chunk, chunk)
            tiles = [a + b for a, b in zip(tiles_at(acc[0], base, chunk), tiles_at(acc[1], base, chunk))]
            for t in TILES[:-1]:
                out_ref[n, band(t, chunk), :] = tiles[t]
            out_ref[n, 3 * chunk:, :] = fold_last(tiles[3])
            return carry

        lax.fori_loop(0, out_ref.shape[0], one, 0)

    emit(tail_out, tail_acc)
    emit(head_out, head_acc)
    _, x, _, top, _ = where_here()
    group = 2 * x + top
    row = lax.broadcasted_iota(jnp.int32, (REL_PAD, LANES), 0)
    lane = lax.broadcasted_iota(jnp.int32, (REL_PAD, LANES), 1)
    loss = jnp.where(lane == group, loss_acc[...], 0.0)
    for t in TILES[:-1]:
        rows = rel_acc[:, band(t, LANES)]
        rel_out[band(t, REL_PAD), :] = jnp.where(row == REL_PAD - 1, loss, rows) if t == 0 else rows
    rel_out[3 * REL_PAD:, :] = fold_last(rel_acc[:, 3 * LANES:])


def bucket_call(step, tail_bits, edges, counts, negs, rel_ids, ent, rel, table):
    smem, vmem, hbm = (pl.BlockSpec(memory_space=m) for m in (pltpu.SMEM, pltpu.VMEM, pl.ANY))
    rows, neg_count, chunks = ent.shape[0] // 4, negs.shape[-1], table.shape[0]
    width = 4 * LANES
    wire = wire_rows(CHUNK)
    block = pltpu.VMEM((BLOCK * 4, LANES), F32)
    table_rows = pltpu.VMEM((chunks * CHUNK * 4, LANES), F32)
    head_rows = pltpu.VMEM((rows * 4, LANES), F32)
    return pl.pallas_call(
        functools.partial(bucket_kernel, (step, tail_bits)),
        out_shape=(
            jax.ShapeDtypeStruct((chunks, wire, LANES), F32),
            jax.ShapeDtypeStruct((rows // CHUNK, wire, LANES), F32),
            jax.ShapeDtypeStruct((wire_rows(REL_PAD), LANES), F32),
        ),
        in_specs=[hbm, smem, hbm, hbm, vmem, vmem, vmem],
        out_specs=(vmem, vmem, vmem),
        scratch_shapes=[
            table_rows, *[block] * 6, pltpu.VMEM((BLOCK, width), F32), pltpu.VMEM((BLOCK, width), BF16), pltpu.VMEM((BLOCK, 1), F32),
            pltpu.VMEM((BLOCK, neg_count), F32), pltpu.VMEM((BLOCK, neg_count), BF16), pltpu.VMEM((BLOCK, width), F32), pltpu.VMEM((3 * BLOCK, width), BF16),
            pltpu.VMEM((neg_count, width), BF16), pltpu.VMEM((neg_count, width), F32), pltpu.VMEM((3 * REL_PAD, width), BF16),
            table_rows, table_rows, head_rows, head_rows,
            pltpu.VMEM((REL_PAD, width), F32), pltpu.VMEM((1, 1), F32),
            pltpu.SMEM((edges.shape[-1],), jnp.int32), pltpu.SMEM((neg_count,), jnp.int32), pltpu.VMEM(rel_ids.shape[1:], jnp.int32), pltpu.SemaphoreType.DMA((3,)),
        ],
        compiler_params=pltpu.CompilerParams(vmem_limit_bytes=VMEM_LIMIT),
        name='bucket',
    )(edges, counts, negs, rel_ids, ent, rel, table)


def entry(peers):
    barrier = pltpu.get_barrier_semaphore()
    for peer in peers:
        pl.semaphore_signal(barrier, inc=1, device_id=peer, device_id_type=pl.DeviceIdType.MESH)
    pl.semaphore_wait(barrier, len(peers))


def remote(src, dst, send, recv, peer):
    return pltpu.make_async_remote_copy(src_ref=src, dst_ref=dst, send_sem=send, recv_sem=recv, device_id=peer, device_id_type=pl.DeviceIdType.MESH)


def adagrad(rows, state, grad, mean_of, learn_rate):
    square = grad[0] * grad[0] + grad[1] * grad[1] + grad[2] * grad[2] + grad[3] * grad[3]
    state = state + jnp.sum(square, axis=1, keepdims=True) / mean_of
    root = jnp.sqrt(state + EPSILON)
    return [r - learn_rate * (g / root) for r, g in zip(rows, grad)], state


def exchange_kernel(cfg, tail_ref, head_ref, rel_grad_ref, ent_ref, state_ref, rel_ref, rel_state_ref, *refs):
    step, groups, chunks, emb_width, last = cfg
    if last:
        ent_wire, rel_out, loss_out, *refs = refs
    else:
        ent_out, state_out, rel_out, rel_state_out, loss_out, table, *refs = refs
    (own, from_core, from_y, from_group, rel_sum, rel_from, send_buf,
     own_sem, core_send, core_recv, y_send, y_recv, group_send, group_recv, rel_send, rel_recv, out_send, out_recv) = refs
    learn_rate = LR_SCALE * emb_width ** -0.25
    chunk = CHUNK
    y, x, core, top, bot = where_here()
    mine = 2 * x + top
    x_size = groups // 2

    def place(group, low, c):
        return {'data': 2 * (group % 2) + low, 'ent': 2 * (group // 2) + c}

    def at(dy, dx, c):
        return {'data': dy, 'ent': 2 * dx + c}

    def turned(shift):
        return (bot + shift) % 2

    other_core = at(y, x, 1 - core)
    other_y = at(2 * top + 1 - bot, x, core)
    rel_peers = (other_core, other_y, at(3 - y, x, core), at(y, x + 1 - 2 * (x % 2), core), at(y, x_size - 1 - x, core))
    grad_to = place((mine + step) % groups, turned(step), core)
    grad_from = place((mine + groups - step) % groups, turned(step), core)
    nxt = step + 1
    table_to = place((mine + groups - nxt) % groups, turned(nxt), core)
    table_from = place((mine + nxt) % groups, turned(nxt), core)
    peers = list(rel_peers)
    if step:
        peers += [grad_to, grad_from]
    if last:
        for turn in range(4):
            peers.append(at((y + turn) % 4, x, top))
        senders = [at((2 * core + d), x, c) for d in range(2) for c in range(2)]
        peers += senders
    else:
        peers += [table_to, table_from]
    entry(peers)
    keep = turned(step)
    pending = []

    def start(copy):
        copy.start()
        pending.append(copy)
        return copy

    shards = [(1 - keep, k) for k in range(chunks)] + [(keep, k) for k in range(chunks)]
    loads, cores = [], []
    rel_copies = [start(remote(rel_grad_ref, rel_from.at[0], rel_send.at[0], rel_recv.at[0], rel_peers[0]))]
    for n, (low, k) in enumerate(shards):
        cores.append(start(remote(tail_ref.at[(low * 2 + 1 - core) * chunks + k], from_core.at[n], core_send.at[n], core_recv.at[n], other_core)))
        load = pltpu.make_async_copy(tail_ref.at[(low * 2 + core) * chunks + k], own.at[n], own_sem.at[n])
        load.start()
        loads.append(load)

    def rel_step(n):
        rel_copies[n].wait_recv()
        rel_sum[n] = (rel_grad_ref[...] if n == 0 else rel_sum[n - 1]) + rel_from[n]
        if n + 1 < len(rel_peers):
            rel_copies.append(start(remote(rel_sum.at[n], rel_from.at[n + 1], rel_send.at[n + 1], rel_recv.at[n + 1], rel_peers[n + 1])))

    rel_step(0)
    ys = []
    for k in range(chunks):
        loads[k].wait()
        cores[k].wait_recv()
        own[k] = own[k] + from_core[k]
        ys.append(start(remote(own.at[k], from_y.at[k], y_send.at[k], y_recv.at[k], other_y)))
    rel_step(1)
    for k in range(chunks, 2 * chunks):
        loads[k].wait()
        cores[k].wait_recv()
        own[k] = own[k] + from_core[k]
    rel_step(2)
    gs, outs, forwards, crosses = [], [], [], []

    def stage_group(k):
        ys[k].wait_recv()
        own[chunks + k] = own[chunks + k] + from_y[k]
        if step:
            gs.append(start(remote(own.at[chunks + k], from_group.at[k], group_send.at[k], group_recv.at[k], grad_to)))

    def stage_update(k):
        if step:
            gs[k].wait_recv()
        total = from_group if step else own
        base = k if step else chunks + k
        grad = [total[base, band(t, chunk), :] + head_ref[k, band(t, chunk), :] for t in TILES[:-1]]
        grad.append(jnp.concatenate(unfold_last(total[base, 3 * chunk:, :] + head_ref[k, 3 * chunk:, :]), axis=0))
        span = band(k, chunk)
        rows, state = adagrad(tiles_at(ent_ref, k * chunk, chunk), state_ref[span, :], grad, emb_width, learn_rate)
        wire = rows[:3] + [fold_last(rows[3])]
        if last:
            lane = lax.broadcasted_iota(jnp.int32, (chunk, LANES), 1)
            wire.append(fold_last(jnp.where(lane < 1, state, 0.0)))
        else:
            ent_out[band(k, 4 * chunk), :] = stack_tiles(rows)
            state_out[span, :] = state
        offset = 0
        for piece in wire:
            send_buf[k, offset:offset + piece.shape[0], :] = piece.astype(send_buf.dtype)
            offset += piece.shape[0]
        slot = (bot * 2 + core) * chunks + k
        if last:
            for turn in range(1, 4):
                start(remote(send_buf.at[k], ent_wire.at[slot], out_send.at[turn * chunks + k], out_recv.at[slot], at((y + turn) % 4, x, top)))

            @pl.when(core == top)
            def _():
                pltpu.make_async_copy(send_buf.at[k], ent_wire.at[slot], out_recv.at[slot]).start()

            @pl.when(core != top)
            def _():
                remote(send_buf.at[k], ent_wire.at[slot], out_send.at[k], out_recv.at[slot], other_core).start()
        else:
            outs.append(start(remote(send_buf.at[k], table.at[slot], out_send.at[k], out_recv.at[k], table_to)))

    def forward(n, low, k, peer):
        slot = (low * 2 + core) * chunks + k
        return start(remote(table.at[slot], table.at[slot], out_send.at[n * chunks + k], out_recv.at[n * chunks + k], peer))

    def stage_forward(k):
        if last:
            return
        outs[k].wait_recv()
        forwards.append(forward(1, turned(nxt), k, other_y))
        crosses.append(forward(2, turned(nxt), k, other_core))

    def stage_cross(k):
        if last:
            return
        forwards[k].wait_recv()
        crosses.append(forward(3, 1 - turned(nxt), k, other_core))

    stages = (stage_group, stage_update, stage_forward, stage_cross)
    for tick in range(chunks + len(stages) - 1):
        for lag, stage in enumerate(stages):
            if 0 <= tick - lag < chunks:
                stage(tick - lag)
        if tick in (0, 1):
            rel_step(3 + tick)

    summed = rel_sum[len(rel_peers) - 1]
    rel_grad = [summed[band(t, REL_PAD)] for t in TILES[:-1]] + [jnp.concatenate(unfold_last(summed[3 * REL_PAD:]), axis=0)]
    loss_out[...] = rel_grad[0][REL_PAD - 1:, :]
    row = lax.broadcasted_iota(jnp.int32, (REL_PAD, LANES), 0)
    rel_grad[0] = jnp.where(row < REL_PAD - 1, rel_grad[0], 0.0)
    rel_rows, rel_state = adagrad(tiles_of(rel_ref[...]), rel_state_ref[...], rel_grad, emb_width, learn_rate)
    for t in TILES:
        rel_out[:, band(t, LANES)] = rel_rows[t]
    if not last:
        rel_state_out[...] = rel_state

    if last:
        for slot in range(4 * chunks):
            remote(ent_wire.at[slot], ent_wire.at[slot], out_send.at[0], out_recv.at[slot], other_core).wait_recv()

        @pl.when(core != top)
        def _():
            for k in range(chunks):
                remote(send_buf.at[k], send_buf.at[k], out_send.at[k], out_recv.at[k], other_core).wait_send()
    else:
        for copy in crosses:
            copy.wait_recv()
    for copy in pending:
        copy.wait_send()


def exchange_call(step, groups, emb_width, tail, head, rel_grad, ent, state, rel, rel_state):
    vmem, hbm = pl.BlockSpec(memory_space=pltpu.VMEM), pl.BlockSpec(memory_space=pl.ANY)
    chunks = head.shape[0]
    wire = wire_rows(CHUNK)
    last = step == groups - 1
    like = lambda x: jax.ShapeDtypeStruct(x.shape, x.dtype)
    loss = jax.ShapeDtypeStruct((1, LANES), F32)
    out_wire = wire + (CHUNK // LEFT if last else 0)
    out_type = F32 if last else BF16
    gathered = jax.ShapeDtypeStruct((4 * chunks, out_wire, LANES), out_type)
    out_shape = (gathered, like(rel), loss) if last else (like(ent), like(state), like(rel), like(rel_state), loss, gathered)
    sems = lambda n: pltpu.SemaphoreType.DMA((n,))
    return pl.pallas_call(
        functools.partial(exchange_kernel, (step, groups, chunks, emb_width, last)),
        out_shape=out_shape,
        in_specs=[hbm] + [vmem] * 6,
        out_specs=tuple(vmem for _ in out_shape),
        scratch_shapes=[
            pltpu.VMEM((2 * chunks, wire, LANES), F32), pltpu.VMEM((2 * chunks, wire, LANES), F32),
            pltpu.VMEM((chunks, wire, LANES), F32), pltpu.VMEM((chunks, wire, LANES), F32),
            pltpu.VMEM((5, *rel_grad.shape), F32), pltpu.VMEM((5, *rel_grad.shape), F32),
            pltpu.VMEM((chunks, out_wire, LANES), out_type),
            sems(2 * chunks), sems(2 * chunks), sems(2 * chunks), sems(chunks), sems(chunks), sems(chunks), sems(chunks),
            sems(5), sems(5), sems(4 * chunks), sems(4 * chunks),
        ],
        compiler_params=pltpu.CompilerParams(vmem_limit_bytes=VMEM_LIMIT, collective_id=step, has_side_effects=True),
        name='exchange',
    )(tail, head, rel_grad, ent, state, rel, rel_state)


def index_kernel(cfg, head_ref, tail_ref, rel_ref, mask_ref, neg_ref, key_out, count_out, neg_out, packed, shares, neg_buf, send_sem, recv_sem, neg_send, neg_recv):
    head_bits, tail_bits, spare = cfg
    y, x, core, top, bot = where_here()
    own = 2 * x + core
    other_core = {'data': y, 'ent': 2 * x + 1 - core}
    users = [(c, 2 * core + d) for c in range(2) for d in range(2)]
    users = [({'data': row, 'ent': 2 * x + c}, (core == c) & (y == row)) for c, row in users]
    entry([peer for peer, _ in users] + [{'data': row, 'ent': 2 * x + top} for row in range(4)] + [other_core])
    edges = head_ref[...] | (tail_ref[...] << tail_bits) | (rel_ref[...] << (2 * tail_bits))
    packed[...] = jnp.where(mask_ref[...] > 0, edges, spare << (2 * tail_bits))
    neg_buf[...] = row_address(neg_ref[...])
    to_users = [remote(packed, shares.at[y], send_sem.at[n], recv_sem.at[y], peer) for n, (peer, _) in enumerate(users)]
    for copy, (_, here) in zip(to_users, users):
        @pl.when(jnp.logical_not(here))
        def _():
            copy.start()

    @pl.when(core == top)
    def _():
        pltpu.make_async_copy(packed, shares.at[y], recv_sem.at[y]).start()
        remote(neg_buf, neg_out, neg_send, neg_recv, other_core).start()
        neg_out[...] = neg_buf[...]

    count = jnp.zeros((packed.shape[0], 1), jnp.int32)
    width = packed.shape[1]
    for row in range(4):
        remote(packed, shares.at[row], send_sem.at[0], recv_sem.at[row], other_core).wait_recv()
        share = shares[row]
        mine = ((share >> head_bits) & 3 == 2 * bot + core) & (share >> (2 * tail_bits) != spare)
        local = (share & (2**head_bits - 1)) | (share >> tail_bits << head_bits)
        key_out[:, band(row, width)] = jnp.where(mine, local, spare << (head_bits + tail_bits))
        count = count + jnp.sum(jnp.where(mine, 1, 0), axis=1, keepdims=True)
    count_out[...] = jnp.broadcast_to(count, count_out.shape)
    for copy, (_, here) in zip(to_users, users):
        @pl.when(jnp.logical_not(here))
        def _():
            copy.wait_send()

    @pl.when(core == top)
    def _():
        remote(neg_buf, neg_out, neg_send, neg_recv, other_core).wait_send()

    @pl.when(core != top)
    def _():
        remote(neg_buf, neg_out, neg_send, neg_recv, other_core).wait_recv()


def index_call(cfg, head, tail, rel, mask, neg, reps):
    vmem = pl.BlockSpec(memory_space=pltpu.VMEM)
    groups, share = head.shape
    return pl.pallas_call(
        functools.partial(index_kernel, cfg),
        out_shape=(jax.ShapeDtypeStruct((groups, reps * share), jnp.int32), jax.ShapeDtypeStruct((groups, LANES), jnp.int32), jax.ShapeDtypeStruct(neg.shape, jnp.int32)),
        in_specs=[vmem] * 5,
        out_specs=(vmem,) * 3,
        scratch_shapes=[pltpu.VMEM(head.shape, jnp.int32), pltpu.VMEM((reps, *head.shape), jnp.int32), pltpu.VMEM(neg.shape, jnp.int32),
                        pltpu.SemaphoreType.DMA((4,)), pltpu.SemaphoreType.DMA((4,)), pltpu.SemaphoreType.DMA, pltpu.SemaphoreType.DMA],
        compiler_params=pltpu.CompilerParams(collective_id=20, has_side_effects=True),
        name='setup_index',
    )(head, tail, rel, mask, neg)


def rows_kernel(ent_hbm, rel_ref, table, ent_out, rel_out, rows_buf, away, load_sem, table_send, table_recv, ent_send, ent_recv):
    y, x, core, top, bot = where_here()
    other_core = {'data': y, 'ent': 2 * x + 1 - core}
    chunks, chunk = table.shape[0], CHUNK
    shard = chunks // 4
    entry([other_core])
    rel_rows = rel_ref.shape[0]
    pad = jnp.zeros((REL_PAD - rel_rows, rel_ref.shape[1]), F32)
    for t, tile in enumerate(columns_to_tiles(jnp.concatenate([rel_ref[...], pad], axis=0))):
        rel_out[:, band(t, LANES)] = tile

    def load(n):
        return pltpu.make_async_copy(ent_hbm.at[pl.ds(pl.multiple_of(n * chunk, chunk), chunk), :], rows_buf.at[n % 4], load_sem.at[n % 4])

    def table_copy(q):
        part = table.at[pl.ds(q * shard, shard)]
        return remote(part, part, table_send.at[q], table_recv.at[q], other_core)

    ent_copy = remote(away, ent_out, ent_send, ent_recv, other_core)

    @pl.when(core == top)
    def _():
        for n in range(3):
            load(n).start()
        for q in range(4):
            def one(k, carry):
                n = q * shard + k

                @pl.when(n + 3 < chunks)
                def _():
                    load(n + 3).start()

                load(n).wait()
                tiles = columns_to_tiles(rows_buf[n % 4])
                for t in TILES[:-1]:
                    table[n, band(t, chunk), :] = tiles[t].astype(BF16)
                table[n, 3 * chunk:, :] = fold_last(tiles[3]).astype(BF16)
                place = pl.ds(pl.multiple_of(k * chunk * 4, chunk * 4), chunk * 4)

                @pl.when(2 * bot + core == q)
                def _():
                    ent_out[place, :] = stack_tiles(tiles)

                @pl.when(2 * bot + 1 - core == q)
                def _():
                    away[place, :] = stack_tiles(tiles)

                return carry

            lax.fori_loop(0, shard, one, 0)
            table_copy(q).start()

            @pl.when(2 * bot + 1 - core == q)
            def _():
                ent_copy.start()

        for q in range(4):
            table_copy(q).wait_send()
        ent_copy.wait_send()

    @pl.when(core != top)
    def _():
        for q in range(4):
            table_copy(q).wait_recv()
        ent_copy.wait_recv()


def rows_call(ent, rel):
    vmem, hbm = pl.BlockSpec(memory_space=pltpu.VMEM), pl.BlockSpec(memory_space=pl.ANY)
    rows, width = ent.shape
    chunks = rows // CHUNK
    dma = pltpu.SemaphoreType.DMA
    return pl.pallas_call(
        rows_kernel,
        out_shape=(jax.ShapeDtypeStruct((chunks, wire_rows(CHUNK), LANES), BF16), jax.ShapeDtypeStruct((rows, LANES), F32), jax.ShapeDtypeStruct((REL_PAD, 4 * LANES), F32)),
        in_specs=[hbm, vmem],
        out_specs=(vmem,) * 3,
        scratch_shapes=[pltpu.VMEM((4, CHUNK, width), F32), pltpu.VMEM((rows, LANES), F32), dma((4,)), dma((4,)), dma((4,)), dma, dma],
        compiler_params=pltpu.CompilerParams(collective_id=21, has_side_effects=True),
        cost_estimate=pl.CostEstimate(flops=10**9, bytes_accessed=2 * 10**7, transcendentals=0),
        name='setup_rows',
    )(ent, rel)


def finish_kernel(width, rel_rows, wire_ref, rel_ref, ent_out, rel_out):
    chunk = CHUNK
    tiles = [wire_ref[0, band(t, chunk), :] for t in TILES[:-1]]
    tiles.append(jnp.concatenate(unfold_last(wire_ref[0, 3 * chunk:wire_rows(chunk), :]), axis=0))
    ent_out[...] = tiles_to_columns(tiles, width)

    @pl.when(pl.program_id(0) == 0)
    def _():
        rel_out[...] = tiles_to_columns(tiles_of(rel_ref[...]), width)[:rel_rows]


def finish_call(wire, rel, width, rel_rows):
    chunks = wire.shape[0]
    return pl.pallas_call(
        functools.partial(finish_kernel, width, rel_rows),
        out_shape=(jax.ShapeDtypeStruct((chunks * CHUNK, width), F32), jax.ShapeDtypeStruct((rel_rows, width), F32)),
        grid=(chunks,),
        in_specs=[pl.BlockSpec((1, *wire.shape[1:]), lambda n: (n, 0, 0)), pl.BlockSpec(rel.shape, lambda n: (0, 0))],
        out_specs=(pl.BlockSpec((CHUNK, width), lambda n: (n, 0)), pl.BlockSpec((rel_rows, width), lambda n: (0, 0))),
        name='finish',
    )(wire, rel)


def solution(mesh):
    groups = mesh.shape['ent']
    data_reps = mesh.shape['data']
    row_spec = P(('sweep', 'ent'), None)
    edge_spec = P(('sweep', 'ent'), None, 'data')

    def device_fn(ent_table, ent_state, rel_table, head_idx, tail_idx, rel_idx, edge_mask, neg_idx):
        part_rows, emb_width = ent_table.shape
        rel_rows = rel_table.shape[0]
        bucket_edges = head_idx.shape[2] * data_reps
        shard = part_rows // 4
        tail_bits = (part_rows - 1).bit_length()
        head_bits = (shard - 1).bit_length()
        spare = 2**(REL_PAD - 1).bit_length() - 1
        ent = lax.axis_index('ent')
        _, _, core, top, bot = where_here()

        keys, counts, neg = index_call((head_bits, tail_bits, spare), head_idx[0], tail_idx[0], rel_idx[0], edge_mask[0], neg_idx[0], data_reps)
        keys = lax.sort(keys, dimension=1)
        counts = counts[:, 0]
        neg = neg[:, None]
        rel_ids = (keys >> (head_bits + tail_bits)).reshape(groups, -1, BLOCK)
        words = (row_address(keys & (shard - 1)) << (tail_bits + 2)) | row_address((keys >> head_bits) & (part_rows - 1))
        words = jnp.pad(words, ((0, 0), (BLOCK, BLOCK)))[:, None]

        table, ent_now, rel_now = rows_call(ent_table, rel_table)
        to_core = lambda c: lax.dynamic_slice_in_dim(ent_state, (2 * bot + c) * shard, shard)
        away = [(d * groups + 2 * (n // 2) + d // 2, d * groups + 2 * (n // 2) + 1 - d // 2) for d in range(data_reps) for n in range(0, groups, 2)]
        state_now = jnp.where(core == top, to_core(core), lax.ppermute(to_core(1 - core), ('data', 'ent'), away))[:, None]
        rel_state = jnp.zeros((REL_PAD, 1), F32)
        losses = []
        for step in range(groups):
            tail, head, rel_grad = bucket_call(step, tail_bits + 2, words, counts, neg, rel_ids, ent_now, rel_now, table)
            out = exchange_call(step, groups, emb_width, tail, head, rel_grad, ent_now, state_now, rel_now, rel_state)
            if step + 1 < groups:
                ent_now, state_now, rel_now, rel_state, loss, table = out
            else:
                wire, rel_now, loss = out
            losses.append(loss)
        ent_out, rel_out = finish_call(wire, rel_now, emb_width, rel_rows)
        state_out = wire[:, wire_rows(CHUNK):, :HALF:LEFT].transpose(0, 2, 1).reshape(part_rows)
        loss_rows = jnp.concatenate(losses, axis=0) / bucket_edges
        bucket_loss = lax.dynamic_slice_in_dim(loss_rows, ent, 1, axis=1).reshape(1, groups)
        return ent_out, state_out, rel_out, bucket_loss

    return jax.shard_map(device_fn, mesh=mesh, in_specs=(row_spec, P(('sweep', 'ent')), P('sweep', None), edge_spec, edge_spec, edge_spec, edge_spec, P(('sweep', 'ent'), None, None)), out_specs=(row_spec, P(('sweep', 'ent')), P('sweep', None), row_spec), check_vma=False)
```

```python
import functools

import jax
import jax.numpy as jnp
from jax import lax
from jax.experimental import pallas as pl
from jax.experimental.pallas import tpu as pltpu
from jax.sharding import PartitionSpec as P

LR_SCALE = 0.2
EPSILON = 1e-8
LANES = 128
HALF = 64
LEFT = 8
BLOCK = 256
CHUNK = 128
UNROLL = 128
LAG = 2
REL_HOPS = 6
STRIP = 32
REL_PAD = 128
TILES = range(4)
CORES = range(2)
ROW_COL, ROW_ROW, COL_COL = (((1,), (0,)), ((1,), (1,)), ((0,), (0,)))
F32 = jnp.float32
BF16 = jnp.bfloat16
VMEM_LIMIT = 60 * 2**20


def wire_rows(rows):
    return 3 * rows + rows // LEFT


def columns_to_tiles(x):
    half = x.shape[0] // 2
    a, c, d = slice(0, LANES), slice(LANES, LANES + HALF), slice(LANES + HALF, half)
    re, im = x[:half], x[half:]
    zero = jnp.zeros((HALF - LEFT, x.shape[1]), x.dtype)
    return [t.T for t in (re[a], im[a], jnp.concatenate([re[c], im[c]], axis=0), jnp.concatenate([re[d], zero, im[d], zero], axis=0))]


def tiles_to_columns(tiles):
    a, b, c, d = (t.T for t in tiles)
    high = slice(HALF, HALF + LEFT)
    return jnp.concatenate([a, c[:HALF], d[:LEFT], b, c[HALF:], d[high]], axis=0)


def each_row(count, body):
    for u in range(count):
        body(u)


def band(n, size):
    return slice(n * size, (n + 1) * size)


def where_here():
    y, ent = lax.axis_index('data'), lax.axis_index('ent')
    return y, ent // 2, ent % 2, y // 2, y % 2


def fold_last(tile):
    n = tile.shape[0] // LEFT
    out = tile[:n]
    for k in range(1, LEFT):
        out = out + pltpu.roll(tile[band(k, n)], LEFT * k, 1)
    return out


def unfold_last(packed):
    keep = lax.broadcasted_iota(jnp.int32, packed.shape, 1) % HALF < LEFT
    return [jnp.where(keep, packed if k == 0 else pltpu.roll(packed, LANES - LEFT * k, 1), 0.0) for k in range(LEFT)]


def tiles_of(x):
    return [x[:, band(t, LANES)] for t in TILES]


def times(x, y):
    out = [x[0] * y[0] - x[1] * y[1], x[0] * y[1] + x[1] * y[0]]
    for a, b in zip(x[2:], y[2:]):
        low = lax.broadcasted_iota(jnp.int32, a.shape, 1) < HALF
        a_swap, b_swap = pltpu.roll(a, HALF, 1), pltpu.roll(b, HALF, 1)
        out.append(jnp.where(low, a * b - a_swap * b_swap, a_swap * b + a * b_swap))
    return out


def times_conj(x, y):
    out = [x[0] * y[0] + x[1] * y[1], x[1] * y[0] - x[0] * y[1]]
    for a, b in zip(x[2:], y[2:]):
        low = lax.broadcasted_iota(jnp.int32, a.shape, 1) < HALF
        a_swap, b_swap = pltpu.roll(a, HALF, 1), pltpu.roll(b, HALF, 1)
        out.append(jnp.where(low, a * b + a_swap * b_swap, a * b_swap - a_swap * b))
    return out


def tiles_at(ref, row, rows):
    block = ref[pl.ds(row * 4, rows * 4), :].reshape(rows // 8, 32, LANES)
    return [block[:, 8 * t:8 * t + 8].reshape(rows, LANES) for t in TILES]


def stack_tiles(tiles):
    rows = tiles[0].shape[0]
    return jnp.concatenate([t.reshape(rows // 8, 8, LANES) for t in tiles], axis=1).reshape(rows * 4, LANES)


def row_at(address):
    return pl.ds(address, 4, stride=8)


def row_address(row):
    return (row >> 3 << 5) | (row & 7)


def in_three(x):
    pieces = []
    for _ in range(3):
        piece = x.astype(BF16)
        pieces.append(piece)
        x = x - piece.astype(F32)
    return pieces


def dot(x, y, dims):
    return lax.dot_general(x, y, (dims, ((), ())), preferred_element_type=F32)


def bucket_kernel(cfg, edges_hbm, count_ref, negs_hbm, rel_ids_hbm, ent_ref, rel_ref, table_ref, tail_out, head_out, rel_out,
                  tail_rows, head_next, tail_next, head_buf, tail_buf, gh_last, gt_last, rel_buf, query_buf, pos_buf, score_buf, d_neg_buf, grad_buf, piece_buf,
                  neg_rows, neg_grad, rel_three, tail_acc0, tail_acc1, head_acc0, head_acc1, rel_acc, loss_acc,
                  edge_ref, neg_ref, rel_id_ref, sems):
    step, tail_bits = cfg
    chunk = CHUNK
    part = chunk // LEFT
    tail_acc, head_acc = (tail_acc0, tail_acc1), (head_acc0, head_acc1)
    count = count_ref[step]
    negs = neg_ref.shape[0]
    loads = [
        pltpu.make_async_copy(negs_hbm.at[step, 0], neg_ref, sems.at[0]),
        pltpu.make_async_copy(edges_hbm.at[step, 0], edge_ref, sems.at[1]),
        pltpu.make_async_copy(rel_ids_hbm.at[step], rel_id_ref, sems.at[2]),
    ]
    for load in loads:
        load.start()

    def head_of(e):
        return row_at(e >> tail_bits)

    def tail_of(e):
        return row_at(e & (2**tail_bits - 1))

    def widen(n, carry):
        base = pl.multiple_of(n * chunk, chunk)
        tiles = [table_ref[n, band(t, chunk), :].astype(F32) for t in TILES[:-1]]
        tiles.append(jnp.concatenate(unfold_last(table_ref[n, 3 * chunk:, :].astype(F32)), axis=0))
        tail_rows[pl.ds(base * 4, chunk * 4), :] = stack_tiles(tiles)
        for acc in tail_acc:
            acc[pl.ds(base * 4, chunk * 4), :] = jnp.zeros((chunk * 4, LANES), F32)
        return carry

    lax.fori_loop(0, table_ref.shape[0], widen, 0)

    def clear(n, carry):
        base = pl.multiple_of(n * chunk * 4, chunk * 4)
        for acc in head_acc:
            acc[pl.ds(base, chunk * 4), :] = jnp.zeros((chunk * 4, LANES), F32)
        return carry

    lax.fori_loop(0, head_out.shape[0], clear, 0)
    neg_grad[...] = jnp.zeros_like(neg_grad)
    gh_last[...] = jnp.zeros_like(gh_last)
    gt_last[...] = jnp.zeros_like(gt_last)
    rel_acc[...] = jnp.zeros_like(rel_acc)
    loss_acc[...] = jnp.zeros_like(loss_acc)
    for n, piece in enumerate(in_three(rel_ref[...])):
        rel_three[band(n, REL_PAD), :] = piece
    for load in loads:
        load.wait()

    def take_negs(n, carry):
        base = pl.multiple_of(n * UNROLL, UNROLL)

        def take(u):
            head_buf[row_at(row_address(u)), :] = tail_rows[row_at(neg_ref[base + u]), :]

        each_row(UNROLL, take)
        for t, tile in enumerate(tiles_at(head_buf, 0, UNROLL)):
            neg_rows[pl.ds(base, UNROLL), band(t, LANES)] = tile.astype(BF16)
        return carry

    lax.fori_loop(0, negs // UNROLL, take_negs, 0)

    def take_edges(base):
        def take(u):
            e = edge_ref[base + u]
            head_next[row_at(row_address(u)), :] = ent_ref[head_of(e), :]
            tail_next[row_at(row_address(u)), :] = tail_rows[tail_of(e), :]

        return take

    def put_edges(base):
        def put(pair):
            for lane in range(2):
                u = 2 * pair + lane
                e = edge_ref[base + u]
                row = row_at(row_address(u))
                head_acc[lane][head_of(e), :] += gh_last[row, :]
                tail_acc[lane][tail_of(e), :] += gt_last[row, :]

        return put

    each_row(BLOCK, take_edges(BLOCK))
    spans = [slice(r, r + STRIP) for r in range(0, BLOCK, STRIP)]

    def block(n, carry):
        base = pl.multiple_of(n * BLOCK, BLOCK)
        hot = lax.broadcasted_iota(jnp.int32, (REL_PAD, BLOCK), 0) == rel_id_ref[pl.ds(n, 1), :]
        hot = jnp.where(hot, 1.0, 0.0).astype(BF16)
        rel_buf[...] = dot(jnp.concatenate([hot] * 3, axis=0), rel_three[...], COL_COL)
        for span in spans:
            head, tail, rel = tiles_at(head_next, span.start, STRIP), tiles_at(tail_next, span.start, STRIP), tiles_of(rel_buf[span, :])
            wide = slice(4 * span.start, 4 * span.stop)
            head_buf[wide, :], tail_buf[wide, :] = stack_tiles(head), stack_tiles(tail)
            total = None
            for t, q in enumerate(times(head, rel)):
                q = q.astype(BF16)
                query_buf[span, band(t, LANES)] = q
                product = q.astype(F32) * tail[t]
                total = product if total is None else total + product
            pos_buf[span, :] = jnp.sum(total, axis=1, keepdims=True)
        each_row(BLOCK, take_edges(base + 2 * BLOCK))
        each_row(BLOCK // 2, put_edges(base))
        score_buf[...] = dot(query_buf[...], neg_rows[...], ROW_ROW)
        for span in spans:
            weight = jnp.where(lax.broadcasted_iota(jnp.int32, (STRIP, 1), 0) + (base + span.start) < count, 1.0, 0.0)
            score, pos = score_buf[span, :], pos_buf[span, :]
            top = jnp.maximum(jnp.max(score, axis=1, keepdims=True), pos)
            pos_exp = jnp.exp(pos - top)
            neg_exp = jnp.exp(score - top)
            total = pos_exp + jnp.sum(neg_exp, axis=1, keepdims=True)
            loss_acc[...] += jnp.sum(weight * (top + jnp.log(total) - pos), axis=0, keepdims=True)
            pos_buf[span, :] = weight * (pos_exp / total - 1.0)
            d_neg_buf[span, :] = ((weight / total) * neg_exp).astype(BF16)
        grad_buf[...] = dot(d_neg_buf[...], neg_rows[...], ROW_COL)
        neg_grad[...] += dot(d_neg_buf[...], query_buf[...], COL_COL)
        for span in spans:
            wide = slice(4 * span.start, 4 * span.stop)
            d_pos = pos_buf[span, :]
            tail, rel = tiles_at(tail_buf, span.start, STRIP), tiles_of(rel_buf[span, :])
            grad_q = [d_pos * x + y for x, y in zip(tail, tiles_of(grad_buf[span, :]))]
            gt_last[wide, :] = stack_tiles([d_pos * q.astype(F32) for q in tiles_of(query_buf[span, :])])
            gh_last[wide, :] = stack_tiles(times_conj(grad_q, rel))
            for t, grad in enumerate(times_conj(grad_q, tiles_at(head_buf, span.start, STRIP))):
                for k, piece in enumerate(in_three(grad)):
                    piece_buf[k * BLOCK + span.start:k * BLOCK + span.stop, band(t, LANES)] = piece
        rel_acc[...] += dot(jnp.concatenate([hot] * 3, axis=1), piece_buf[...], ROW_COL)
        return carry

    blocks = pl.cdiv(count, BLOCK)
    lax.fori_loop(0, blocks, block, 0)
    each_row(BLOCK // 2, put_edges(pl.multiple_of(blocks * BLOCK, BLOCK)))

    def put_negs(n, carry):
        base = pl.multiple_of(n * UNROLL, UNROLL)
        gt_last[:4 * UNROLL, :] = stack_tiles(tiles_of(neg_grad[pl.ds(base, UNROLL), :]))

        def put(pair):
            for lane in range(2):
                u = 2 * pair + lane
                tail_acc[lane][row_at(neg_ref[base + u]), :] += gt_last[row_at(row_address(u)), :]

        each_row(UNROLL // 2, put)
        return carry

    lax.fori_loop(0, negs // UNROLL, put_negs, 0)

    def emit(out_ref, acc):
        def one(n, carry):
            base = pl.multiple_of(n * chunk, chunk)
            tiles = [a + b for a, b in zip(tiles_at(acc[0], base, chunk), tiles_at(acc[1], base, chunk))]
            for t in TILES[:-1]:
                out_ref[n, band(t, chunk), :] = tiles[t]
            out_ref[n, 3 * chunk:, :] = fold_last(tiles[3])
            return carry

        lax.fori_loop(0, out_ref.shape[0], one, 0)

    emit(tail_out, tail_acc)
    emit(head_out, head_acc)
    _, x, _, top, _ = where_here()
    group = 2 * x + top
    row = lax.broadcasted_iota(jnp.int32, (REL_PAD, LANES), 0)
    lane = lax.broadcasted_iota(jnp.int32, (REL_PAD, LANES), 1)
    loss = jnp.where(lane == group, loss_acc[...], 0.0)
    for t in TILES[:-1]:
        rows = rel_acc[:, band(t, LANES)]
        rel_out[band(t, REL_PAD), :] = jnp.where(row == REL_PAD - 1, loss, rows) if t == 0 else rows
    rel_out[3 * REL_PAD:, :] = fold_last(rel_acc[:, 3 * LANES:])


def bucket_call(step, tail_bits, edges, counts, negs, rel_ids, ent, rel, table):
    smem, vmem, hbm = (pl.BlockSpec(memory_space=m) for m in (pltpu.SMEM, pltpu.VMEM, pl.ANY))
    rows, neg_count, chunks = ent.shape[0] // 4, negs.shape[-1], table.shape[0]
    width = 4 * LANES
    wire = wire_rows(CHUNK)
    block = pltpu.VMEM((BLOCK * 4, LANES), F32)
    table_rows = pltpu.VMEM((chunks * CHUNK * 4, LANES), F32)
    head_rows = pltpu.VMEM((rows * 4, LANES), F32)
    return pl.pallas_call(
        functools.partial(bucket_kernel, (step, tail_bits)),
        out_shape=(
            jax.ShapeDtypeStruct((chunks, wire, LANES), F32),
            jax.ShapeDtypeStruct((rows // CHUNK, wire, LANES), F32),
            jax.ShapeDtypeStruct((wire_rows(REL_PAD), LANES), F32),
        ),
        in_specs=[hbm, smem, hbm, hbm, vmem, vmem, vmem],
        out_specs=(vmem, vmem, vmem),
        scratch_shapes=[
            table_rows, *[block] * 6, pltpu.VMEM((BLOCK, width), F32), pltpu.VMEM((BLOCK, width), BF16), pltpu.VMEM((BLOCK, 1), F32),
            pltpu.VMEM((BLOCK, neg_count), F32), pltpu.VMEM((BLOCK, neg_count), BF16), pltpu.VMEM((BLOCK, width), F32), pltpu.VMEM((3 * BLOCK, width), BF16),
            pltpu.VMEM((neg_count, width), BF16), pltpu.VMEM((neg_count, width), F32), pltpu.VMEM((3 * REL_PAD, width), BF16),
            table_rows, table_rows, head_rows, head_rows,
            pltpu.VMEM((REL_PAD, width), F32), pltpu.VMEM((1, 1), F32),
            pltpu.SMEM((edges.shape[-1],), jnp.int32), pltpu.SMEM((neg_count,), jnp.int32), pltpu.VMEM(rel_ids.shape[1:], jnp.int32), pltpu.SemaphoreType.DMA((3,)),
        ],
        compiler_params=pltpu.CompilerParams(vmem_limit_bytes=VMEM_LIMIT),
        name='bucket',
    )(edges, counts, negs, rel_ids, ent, rel, table)


def entry(peers):
    barrier = pltpu.get_barrier_semaphore()
    for peer in peers:
        pl.semaphore_signal(barrier, inc=1, device_id=peer, device_id_type=pl.DeviceIdType.MESH)
    pl.semaphore_wait(barrier, len(peers))


def remote(src, dst, send, recv, peer):
    return pltpu.make_async_remote_copy(src_ref=src, dst_ref=dst, send_sem=send, recv_sem=recv, device_id=peer, device_id_type=pl.DeviceIdType.MESH)


def adagrad(rows, state, grad, mean_of, learn_rate):
    square = grad[0] * grad[0] + grad[1] * grad[1] + grad[2] * grad[2] + grad[3] * grad[3]
    state = state + jnp.sum(square, axis=1, keepdims=True) / mean_of
    root = jnp.sqrt(state + EPSILON)
    return [r - learn_rate * (g / root) for r, g in zip(rows, grad)], state


def exchange_kernel(cfg, tail_ref, head_ref, rel_grad_ref, ent_ref, state_ref, rel_ref, rel_state_ref, *refs):
    step, groups, chunks, emb_width, last = cfg
    if last:
        ent_wire, rel_out, loss_out, *refs = refs
    else:
        ent_out, state_out, rel_out, rel_state_out, loss_out, table, *refs = refs
    (own, from_core, from_y, from_group, rel_sum, rel_from, send_buf,
     own_sem, core_send, core_recv, y_send, y_recv, group_send, group_recv, rel_send, rel_recv, out_send, out_recv) = refs
    learn_rate = LR_SCALE * emb_width ** -0.25
    chunk = CHUNK
    y, x, core, top, bot = where_here()
    mine = 2 * x + top
    x_size = groups // 2

    def place(group, low, c):
        return {'data': 2 * (group % 2) + low, 'ent': 2 * (group // 2) + c}

    def at(dy, dx, c):
        return {'data': dy, 'ent': 2 * dx + c}

    def turned(shift):
        return (bot + shift) % 2

    other_core = at(y, x, 1 - core)
    other_y = at(2 * top + 1 - bot, x, core)
    rel_peers = (other_core, other_y, at(3 - y, x, core), at(y, x + 1 - 2 * (x % 2), core), at(y, x_size - 1 - x, core), other_core)
    grad_to = place((mine + step) % groups, turned(step), core)
    grad_from = place((mine + groups - step) % groups, turned(step), core)
    nxt = step + 1
    table_to = place((mine + groups - nxt) % groups, turned(nxt), core)
    table_from = place((mine + nxt) % groups, turned(nxt), core)
    peers = list(rel_peers)
    if step:
        peers += [grad_to, grad_from]
    if last:
        for turn in range(4):
            peers.append(at((y + turn) % 4, x, top))
        senders = [at((2 * core + d), x, c) for d in range(2) for c in range(2)]
        peers += senders
    else:
        peers += [table_to, table_from]
    entry(peers)
    keep = turned(step)
    pending = []

    def start(copy):
        copy.start()
        pending.append(copy)
        return copy

    shards = [(1 - keep, k) for k in range(chunks)] + [(keep, k) for k in range(chunks)]
    loads, cores = [], []
    rel_copies = [start(remote(rel_grad_ref.at[1 - core], rel_from.at[0], rel_send.at[0], rel_recv.at[0], rel_peers[0]))]
    for n, (low, k) in enumerate(shards):
        cores.append(start(remote(tail_ref.at[(low * 2 + 1 - core) * chunks + k], from_core.at[n], core_send.at[n], core_recv.at[n], other_core)))
        load = pltpu.make_async_copy(tail_ref.at[(low * 2 + core) * chunks + k], own.at[n], own_sem.at[n])
        load.start()
        loads.append(load)

    def rel_step(n):
        rel_copies[n].wait_recv()
        rel_sum[n] = (rel_grad_ref[core] if n == 0 else rel_sum[n - 1]) + rel_from[n]
        rel_copies.append(start(remote(rel_sum.at[n], rel_from.at[n + 1], rel_send.at[n + 1], rel_recv.at[n + 1], rel_peers[n + 1])))

    ys = []
    for k in range(chunks):
        loads[k].wait()
        cores[k].wait_recv()
        own[k] = own[k] + from_core[k]
        ys.append(start(remote(own.at[k], from_y.at[k], y_send.at[k], y_recv.at[k], other_y)))
        if k == 1:
            rel_step(0)
    for k in range(chunks, 2 * chunks):
        loads[k].wait()
        cores[k].wait_recv()
        own[k] = own[k] + from_core[k]
    gs, outs, forwards, crosses = [], [], [], []

    def stage_group(k):
        ys[k].wait_recv()
        own[chunks + k] = own[chunks + k] + from_y[k]
        if step:
            gs.append(start(remote(own.at[chunks + k], from_group.at[k], group_send.at[k], group_recv.at[k], grad_to)))

    def cross_copy(k):
        return remote(send_buf.at[k], ent_wire.at[(bot * 2 + core) * chunks + k], out_send.at[2 * chunks + k], out_recv.at[(bot * 2 + core) * chunks + k], other_core)

    turn = (y + 4 - 2 * core) % 4
    near = 1 - turn % 2
    back = jnp.where((turn == 1) | (turn == 2), 0, 1)
    onward = at((y + 1 + 2 * back) % 4, x, core)

    def landed(low, c, k):
        slot = (low * 2 + c) * chunks + k
        remote(ent_wire.at[slot], ent_wire.at[slot], out_send.at[0], out_recv.at[slot], other_core).wait_recv()

    def stage_relay(k):
        if k % 2 == 0:
            return
        for c in CORES:
            landed(near, c, k - 1)
            landed(near, c, k)
            slot = (near * 2 + c) * chunks + k - 1 + back
            start(remote(ent_wire.at[slot], ent_wire.at[slot], out_send.at[(3 + c) * chunks + k], out_recv.at[slot], onward))

    def stage_update(k):
        if step:
            gs[k].wait_recv()
        total = from_group if step else own
        base = k if step else chunks + k
        grad = [total[base, band(t, chunk), :] + head_ref[k, band(t, chunk), :] for t in TILES[:-1]]
        grad.append(jnp.concatenate(unfold_last(total[base, 3 * chunk:, :] + head_ref[k, 3 * chunk:, :]), axis=0))
        span = band(k, chunk)
        rows, state = adagrad(tiles_at(ent_ref, k * chunk, chunk), state_ref[span, :], grad, emb_width, learn_rate)
        wire = rows[:3] + [fold_last(rows[3])]
        if last:
            lane = lax.broadcasted_iota(jnp.int32, (chunk, LANES), 1)
            wire.append(fold_last(jnp.where(lane < 1, state, 0.0)))
        else:
            ent_out[band(k, 4 * chunk), :] = stack_tiles(rows)
            state_out[span, :] = state
        offset = 0
        for piece in wire:
            send_buf[k, offset:offset + piece.shape[0], :] = piece.astype(send_buf.dtype)
            offset += piece.shape[0]
        slot = (bot * 2 + core) * chunks + k
        if last:
            for n, turn in enumerate((1, 3)):
                start(remote(send_buf.at[k], ent_wire.at[slot], out_send.at[n * chunks + k], out_recv.at[slot], at((y + turn) % 4, x, top)))

            @pl.when(core == top)
            def _():
                pltpu.make_async_copy(send_buf.at[k], ent_wire.at[slot], out_recv.at[slot]).start()

            @pl.when(core != top)
            def _():
                cross_copy(k).start()
        else:
            outs.append(start(remote(send_buf.at[k], table.at[slot], out_send.at[k], out_recv.at[k], table_to)))

    def forward(n, low, k, peer):
        slot = (low * 2 + core) * chunks + k
        return start(remote(table.at[slot], table.at[slot], out_send.at[n * chunks + k], out_recv.at[n * chunks + k], peer))

    def stage_forward(k):
        outs[k].wait_recv()
        forwards.append(forward(1, turned(nxt), k, other_y))
        crosses.append(forward(2, turned(nxt), k, other_core))

    def stage_cross(k):
        forwards[k].wait_recv()
        crosses.append(forward(3, 1 - turned(nxt), k, other_core))

    stages = (stage_group, stage_update, stage_relay) if last else (stage_group, stage_update, stage_forward, stage_cross)
    rel_steps = len(rel_peers) - 1
    for tick in range(chunks + LAG * (len(stages) - 1)):
        for n, stage in enumerate(stages):
            if 0 <= tick - LAG * n < chunks:
                stage(tick - LAG * n)
        if tick % 2 == 1 and tick < 2 * rel_steps - 1:
            rel_step(tick // 2 + 1)

    rel_copies[rel_steps].wait_recv()
    halves = rel_sum[rel_steps - 1], rel_from[rel_steps]
    summed = jnp.concatenate([jnp.where(core == n, halves[0], halves[1]) for n in CORES], axis=0)
    rel_grad = [summed[band(t, REL_PAD)] for t in TILES[:-1]] + [jnp.concatenate(unfold_last(summed[3 * REL_PAD:]), axis=0)]
    loss_out[...] = rel_grad[0][REL_PAD - 1:, :]
    row = lax.broadcasted_iota(jnp.int32, (REL_PAD, LANES), 0)
    rel_grad[0] = jnp.where(row < REL_PAD - 1, rel_grad[0], 0.0)
    rel_rows, rel_state = adagrad(tiles_of(rel_ref[...]), rel_state_ref[...], rel_grad, emb_width, learn_rate)
    for t in TILES:
        rel_out[:, band(t, LANES)] = rel_rows[t]
    if not last:
        rel_state_out[...] = rel_state

    if last:
        for c in CORES:
            for k in range(chunks):
                landed(1 - near, c, k)

        @pl.when(core != top)
        def _():
            for k in range(chunks):
                cross_copy(k).wait_send()
    else:
        for copy in crosses:
            copy.wait_recv()
    for copy in pending:
        copy.wait_send()


def exchange_call(step, groups, emb_width, tail, head, rel_grad, ent, state, rel, rel_state):
    vmem, hbm = pl.BlockSpec(memory_space=pltpu.VMEM), pl.BlockSpec(memory_space=pl.ANY)
    chunks = head.shape[0]
    rel_grad = rel_grad.reshape(2, -1, LANES)
    wire = wire_rows(CHUNK)
    last = step == groups - 1
    like = lambda x: jax.ShapeDtypeStruct(x.shape, x.dtype)
    loss = jax.ShapeDtypeStruct((1, LANES), F32)
    out_wire = wire + (CHUNK // LEFT if last else 0)
    out_type = F32 if last else BF16
    gathered = jax.ShapeDtypeStruct((4 * chunks, out_wire, LANES), out_type)
    out_shape = (gathered, like(rel), loss) if last else (like(ent), like(state), like(rel), like(rel_state), loss, gathered)
    sems = lambda n: pltpu.SemaphoreType.DMA((n,))
    return pl.pallas_call(
        functools.partial(exchange_kernel, (step, groups, chunks, emb_width, last)),
        out_shape=out_shape,
        in_specs=[hbm] + [vmem] * 6,
        out_specs=tuple(vmem for _ in out_shape),
        scratch_shapes=[
            pltpu.VMEM((2 * chunks, wire, LANES), F32), pltpu.VMEM((2 * chunks, wire, LANES), F32),
            pltpu.VMEM((chunks, wire, LANES), F32), pltpu.VMEM((chunks, wire, LANES), F32),
            pltpu.VMEM((REL_HOPS - 1, *rel_grad.shape[1:]), F32), pltpu.VMEM((REL_HOPS, *rel_grad.shape[1:]), F32),
            pltpu.VMEM((chunks, out_wire, LANES), out_type),
            sems(2 * chunks), sems(2 * chunks), sems(2 * chunks), sems(chunks), sems(chunks), sems(chunks), sems(chunks),
            sems(REL_HOPS), sems(REL_HOPS), sems(5 * chunks), sems(4 * chunks),
        ],
        compiler_params=pltpu.CompilerParams(vmem_limit_bytes=VMEM_LIMIT, collective_id=step, has_side_effects=True),
        name='exchange',
    )(tail, head, rel_grad, ent, state, rel, rel_state)


def index_kernel(cfg, head_ref, tail_ref, rel_ref, mask_ref, neg_ref, key_out, count_out, neg_out, packed, shares, neg_buf, send_sem, recv_sem, neg_send, neg_recv):
    head_bits, tail_bits, spare = cfg
    y, x, core, top, bot = where_here()
    own = 2 * x + core
    other_core = {'data': y, 'ent': 2 * x + 1 - core}
    users = [(c, 2 * core + d) for c in range(2) for d in range(2)]
    users = [({'data': row, 'ent': 2 * x + c}, (core == c) & (y == row)) for c, row in users]
    entry([peer for peer, _ in users] + [{'data': row, 'ent': 2 * x + top} for row in range(4)] + [other_core])
    edges = head_ref[...] | (tail_ref[...] << tail_bits) | (rel_ref[...] << (2 * tail_bits))
    packed[...] = jnp.where(mask_ref[...] > 0, edges, spare << (2 * tail_bits))
    neg_buf[...] = row_address(neg_ref[...])
    to_users = [remote(packed, shares.at[y], send_sem.at[n], recv_sem.at[y], peer) for n, (peer, _) in enumerate(users)]
    for copy, (_, here) in zip(to_users, users):
        @pl.when(jnp.logical_not(here))
        def _():
            copy.start()

    @pl.when(core == top)
    def _():
        pltpu.make_async_copy(packed, shares.at[y], recv_sem.at[y]).start()
        remote(neg_buf, neg_out, neg_send, neg_recv, other_core).start()
        neg_out[...] = neg_buf[...]

    count = jnp.zeros((packed.shape[0], 1), jnp.int32)
    width = packed.shape[1]
    for row in range(4):
        remote(packed, shares.at[row], send_sem.at[0], recv_sem.at[row], other_core).wait_recv()
        share = shares[row]
        mine = ((share >> head_bits) & 3 == 2 * bot + core) & (share >> (2 * tail_bits) != spare)
        local = (share & (2**head_bits - 1)) | (share >> tail_bits << head_bits)
        key_out[:, band(row, width)] = jnp.where(mine, local, spare << (head_bits + tail_bits))
        count = count + jnp.sum(jnp.where(mine, 1, 0), axis=1, keepdims=True)
    count_out[...] = jnp.broadcast_to(count, count_out.shape)
    for copy, (_, here) in zip(to_users, users):
        @pl.when(jnp.logical_not(here))
        def _():
            copy.wait_send()

    @pl.when(core == top)
    def _():
        remote(neg_buf, neg_out, neg_send, neg_recv, other_core).wait_send()

    @pl.when(core != top)
    def _():
        remote(neg_buf, neg_out, neg_send, neg_recv, other_core).wait_recv()


def index_call(cfg, head, tail, rel, mask, neg, reps):
    vmem = pl.BlockSpec(memory_space=pltpu.VMEM)
    groups, share = head.shape
    return pl.pallas_call(
        functools.partial(index_kernel, cfg),
        out_shape=(jax.ShapeDtypeStruct((groups, reps * share), jnp.int32), jax.ShapeDtypeStruct((groups, LANES), jnp.int32), jax.ShapeDtypeStruct(neg.shape, jnp.int32)),
        in_specs=[vmem] * 5,
        out_specs=(vmem,) * 3,
        scratch_shapes=[pltpu.VMEM(head.shape, jnp.int32), pltpu.VMEM((reps, *head.shape), jnp.int32), pltpu.VMEM(neg.shape, jnp.int32),
                        pltpu.SemaphoreType.DMA((4,)), pltpu.SemaphoreType.DMA((4,)), pltpu.SemaphoreType.DMA, pltpu.SemaphoreType.DMA],
        compiler_params=pltpu.CompilerParams(collective_id=20, has_side_effects=True),
        name='setup_index',
    )(head, tail, rel, mask, neg)


def rows_kernel(ent_hbm, rel_ref, table, ent_out, rel_out, rows_buf, away, load_sem, table_send, table_recv, ent_send, ent_recv):
    y, x, core, top, bot = where_here()
    other_core = {'data': y, 'ent': 2 * x + 1 - core}
    chunks, chunk = table.shape[0], CHUNK
    shard = chunks // 4
    entry([other_core])
    for t, tile in enumerate(columns_to_tiles(rel_ref[...])):
        rel_out[:, band(t, LANES)] = tile

    def load(n):
        return pltpu.make_async_copy(ent_hbm.at[:, pl.ds(pl.multiple_of(n * chunk, chunk), chunk)], rows_buf.at[n % 4], load_sem.at[n % 4])

    def table_copy(q):
        part = table.at[pl.ds(q * shard, shard)]
        return remote(part, part, table_send.at[q], table_recv.at[q], other_core)

    ent_copy = remote(away, ent_out, ent_send, ent_recv, other_core)

    @pl.when(core == top)
    def _():
        for n in range(3):
            load(n).start()
        for q in range(4):
            def one(k, carry):
                n = q * shard + k

                @pl.when(n + 3 < chunks)
                def _():
                    load(n + 3).start()

                load(n).wait()
                tiles = columns_to_tiles(rows_buf[n % 4])
                for t in TILES[:-1]:
                    table[n, band(t, chunk), :] = tiles[t].astype(BF16)
                table[n, 3 * chunk:, :] = fold_last(tiles[3]).astype(BF16)
                place = pl.ds(pl.multiple_of(k * chunk * 4, chunk * 4), chunk * 4)

                @pl.when(2 * bot + core == q)
                def _():
                    ent_out[place, :] = stack_tiles(tiles)

                @pl.when(2 * bot + 1 - core == q)
                def _():
                    away[place, :] = stack_tiles(tiles)

                return carry

            lax.fori_loop(0, shard, one, 0)
            table_copy(q).start()

            @pl.when(2 * bot + 1 - core == q)
            def _():
                ent_copy.start()

        for q in range(4):
            table_copy(q).wait_send()
        ent_copy.wait_send()

    @pl.when(core != top)
    def _():
        for q in range(4):
            table_copy(q).wait_recv()
        ent_copy.wait_recv()


def rows_call(ent, rel):
    vmem, hbm = pl.BlockSpec(memory_space=pltpu.VMEM), pl.BlockSpec(memory_space=pl.ANY)
    width, rows = ent.shape
    chunks = rows // CHUNK
    dma = pltpu.SemaphoreType.DMA
    return pl.pallas_call(
        rows_kernel,
        out_shape=(jax.ShapeDtypeStruct((chunks, wire_rows(CHUNK), LANES), BF16), jax.ShapeDtypeStruct((rows, LANES), F32), jax.ShapeDtypeStruct((REL_PAD, 4 * LANES), F32)),
        in_specs=[hbm, vmem],
        out_specs=(vmem,) * 3,
        scratch_shapes=[pltpu.VMEM((4, width, CHUNK), F32), pltpu.VMEM((rows, LANES), F32), dma((4,)), dma((4,)), dma((4,)), dma, dma],
        compiler_params=pltpu.CompilerParams(collective_id=21, has_side_effects=True),
        cost_estimate=pl.CostEstimate(flops=10**9, bytes_accessed=2 * 10**7, transcendentals=0),
        name='setup_rows',
    )(ent, rel)


def finish_kernel(wire_ref, rel_ref, ent_out, rel_out):
    chunk = CHUNK
    for n in range(wire_ref.shape[0]):
        tiles = [wire_ref[n, band(t, chunk), :] for t in TILES[:-1]]
        tiles.append(jnp.concatenate(unfold_last(wire_ref[n, 3 * chunk:wire_rows(chunk), :]), axis=0))
        ent_out[:, band(n, chunk)] = tiles_to_columns(tiles)

    @pl.when(pl.program_id(0) == 0)
    def _():
        rel_out[...] = tiles_to_columns(tiles_of(rel_ref[...]))


def finish_call(wire, rel, width):
    chunks = wire.shape[0]
    size = chunks // 8
    whole = lambda n: (0, 0)
    return pl.pallas_call(
        finish_kernel,
        out_shape=(jax.ShapeDtypeStruct((width, chunks * CHUNK), F32), jax.ShapeDtypeStruct((width, REL_PAD), F32)),
        grid=(chunks // size,),
        in_specs=[pl.BlockSpec((size, *wire.shape[1:]), lambda n: (n, 0, 0)), pl.BlockSpec(rel.shape, whole)],
        out_specs=(pl.BlockSpec((width, size * CHUNK), lambda n: (0, n)), pl.BlockSpec((width, REL_PAD), whole)),
        name='finish',
    )(wire, rel)


def solution(mesh):
    groups = mesh.shape['ent']
    data_reps = mesh.shape['data']
    row_spec = P(('sweep', 'ent'), None)
    edge_spec = P(('sweep', 'ent'), None, 'data')

    def device_fn(ent_table, ent_state, rel_table, head_idx, tail_idx, rel_idx, edge_mask, neg_idx):
        part_rows, emb_width = ent_table.shape
        rel_rows = rel_table.shape[0]
        bucket_edges = head_idx.shape[2] * data_reps
        shard = part_rows // 4
        tail_bits = (part_rows - 1).bit_length()
        head_bits = (shard - 1).bit_length()
        spare = 2**(REL_PAD - 1).bit_length() - 1
        ent = lax.axis_index('ent')
        _, _, core, top, bot = where_here()

        keys, counts, neg = index_call((head_bits, tail_bits, spare), head_idx[0], tail_idx[0], rel_idx[0], edge_mask[0], neg_idx[0], data_reps)
        keys = lax.sort(keys, dimension=1)
        counts = counts[:, 0]
        neg = neg[:, None]
        rel_ids = (keys >> (head_bits + tail_bits)).reshape(groups, -1, BLOCK)
        words = (row_address(keys & (shard - 1)) << (tail_bits + 2)) | row_address((keys >> head_bits) & (part_rows - 1))
        words = jnp.pad(words, ((0, 0), (BLOCK, BLOCK)))[:, None]

        table, ent_now, rel_now = rows_call(ent_table.T, jnp.pad(rel_table.T, ((0, 0), (0, REL_PAD - rel_rows))))
        to_core = lambda c: lax.dynamic_slice_in_dim(ent_state, (2 * bot + c) * shard, shard)
        away = [(d * groups + 2 * (n // 2) + d // 2, d * groups + 2 * (n // 2) + 1 - d // 2) for d in range(data_reps) for n in range(0, groups, 2)]
        state_now = jnp.where(core == top, to_core(core), lax.ppermute(to_core(1 - core), ('data', 'ent'), away))[:, None]
        rel_state = jnp.zeros((REL_PAD, 1), F32)
        losses = []
        for step in range(groups):
            tail, head, rel_grad = bucket_call(step, tail_bits + 2, words, counts, neg, rel_ids, ent_now, rel_now, table)
            out = exchange_call(step, groups, emb_width, tail, head, rel_grad, ent_now, state_now, rel_now, rel_state)
            if step + 1 < groups:
                ent_now, state_now, rel_now, rel_state, loss, table = out
            else:
                wire, rel_now, loss = out
            losses.append(loss)
        ent_out, rel_out = finish_call(wire, rel_now, emb_width)
        state_out = wire[:, wire_rows(CHUNK):, :HALF:LEFT].transpose(0, 2, 1).reshape(part_rows)
        loss_rows = jnp.concatenate(losses, axis=0) / bucket_edges
        bucket_loss = lax.dynamic_slice_in_dim(loss_rows, ent, 1, axis=1).reshape(1, groups)
        return ent_out.T, state_out, rel_out[:, :rel_rows].T, bucket_loss

    return jax.shard_map(device_fn, mesh=mesh, in_specs=(row_spec, P(('sweep', 'ent')), P('sweep', None), edge_spec, edge_spec, edge_spec, edge_spec, P(('sweep', 'ent'), None, None)), out_specs=(row_spec, P(('sweep', 'ent')), P('sweep', None), row_spec), check_vma=False)
```

```python
import functools

import jax
import jax.numpy as jnp
from jax import lax
from jax.experimental import pallas as pl
from jax.experimental.pallas import tpu as pltpu
from jax.sharding import PartitionSpec as P

LR_SCALE = 0.2
EPSILON = 1e-8
LANES = 128
HALF = 64
LEFT = 8
BLOCK = 256
CHUNK = 128
UNROLL = 128
LAG = 2
PARTS = 4
REL_HOPS = 6
STRIP = 32
REL_PAD = 128
TILES = range(4)
CORES = range(2)
ROW_COL, ROW_ROW, COL_COL = (((1,), (0,)), ((1,), (1,)), ((0,), (0,)))
F32 = jnp.float32
BF16 = jnp.bfloat16
VMEM_LIMIT = 60 * 2**20


def roll(x, by):
    return pltpu.roll(x, by, 1)


def beside(parts):
    return jnp.concatenate(parts, axis=1)


def below(parts):
    return jnp.concatenate(parts, axis=0)


def lanes(shape):
    return lax.broadcasted_iota(jnp.int32, shape, 1)


def sublanes(shape):
    return lax.broadcasted_iota(jnp.int32, shape, 0)


def row_sum(x):
    return jnp.sum(x, axis=1, keepdims=True)


def wire_rows(rows):
    return 3 * rows + rows // LEFT


def columns_to_tiles(x):
    half = x.shape[0] // 2
    a, c, d = slice(0, LANES), slice(LANES, LANES + HALF), slice(LANES + HALF, half)
    re, im = x[:half], x[half:]
    zero = jnp.zeros((HALF - LEFT, x.shape[1]), x.dtype)
    return [t.T for t in (re[a], im[a], below([re[c], im[c]]), below([re[d], zero, im[d], zero]))]


def tiles_to_columns(tiles):
    a, b, c, d = (t.T for t in tiles)
    high = slice(HALF, HALF + LEFT)
    return below([a, c[:HALF], d[:LEFT], b, c[HALF:], d[high]])


def each_row(count, body):
    for u in range(count):
        body(u)


def band(n, size):
    return slice(n * size, (n + 1) * size)


def where_here():
    y, ent = lax.axis_index('data'), lax.axis_index('ent')
    return y, ent // 2, ent % 2, y // 2, y % 2


def fold_last(tile):
    n = tile.shape[0] // LEFT
    out = tile[:n]
    for k in range(1, LEFT):
        out = out + roll(tile[band(k, n)], LEFT * k)
    return out


def unfold_last(packed):
    keep = lanes(packed.shape) % HALF < LEFT
    return [jnp.where(keep, packed if k == 0 else roll(packed, LANES - LEFT * k), 0.0) for k in range(LEFT)]


def tiles_of(x):
    return [x[:, band(t, LANES)] for t in TILES]


def times(x, y):
    out = [x[0] * y[0] - x[1] * y[1], x[0] * y[1] + x[1] * y[0]]
    for a, b in zip(x[2:], y[2:]):
        low = lanes(a.shape) < HALF
        a_swap, b_swap = roll(a, HALF), roll(b, HALF)
        out.append(jnp.where(low, a * b - a_swap * b_swap, a_swap * b + a * b_swap))
    return out


def times_conj(x, y):
    out = [x[0] * y[0] + x[1] * y[1], x[1] * y[0] - x[0] * y[1]]
    for a, b in zip(x[2:], y[2:]):
        low = lanes(a.shape) < HALF
        a_swap, b_swap = roll(a, HALF), roll(b, HALF)
        out.append(jnp.where(low, a * b + a_swap * b_swap, a * b_swap - a_swap * b))
    return out


def tiles_at(ref, row, rows):
    block = ref[pl.ds(row * 4, rows * 4), :].reshape(rows // 8, 32, LANES)
    return [block[:, 8 * t:8 * t + 8].reshape(rows, LANES) for t in TILES]


def stack_tiles(tiles):
    rows = tiles[0].shape[0]
    return beside([t.reshape(rows // 8, 8, LANES) for t in tiles]).reshape(rows * 4, LANES)


def row_at(address):
    return pl.ds(address, 4, stride=8)


def row_address(row):
    return (row >> 3 << 5) | (row & 7)


def in_three(x):
    pieces = []
    for _ in range(3):
        piece = x.astype(BF16)
        pieces.append(piece)
        x = x - piece.astype(F32)
    return pieces


def dot(x, y, dims):
    return lax.dot_general(x, y, (dims, ((), ())), preferred_element_type=F32)


def bucket_kernel(cfg, edges_hbm, count_ref, negs_hbm, rel_ids_hbm, ent_hbm, rel_ref, table_hbm, tail_hbm, head_hbm, rel_out,
                  tail_rows, head_next, tail_next, head_buf, tail_buf, gh_last, gt_last, rel_buf, query_buf, pos_buf, score_buf, d_neg_buf, grad_buf, piece_buf,
                  neg_rows, neg_grad, rel_three, tail_acc0, tail_acc1, head_acc0, head_acc1, rel_acc, loss_acc,
                  edge_ref, neg_ref, rel_id_ref, ent_ref, table_ref, tail_out, head_out, sems, table_sems, tail_sems):
    step, tail_bits = cfg
    chunk = CHUNK
    part = chunk // LEFT
    tail_acc, head_acc = (tail_acc0, tail_acc1), (head_acc0, head_acc1)
    count = count_ref[step]
    negs = neg_ref.shape[0]
    loads = [
        pltpu.make_async_copy(negs_hbm.at[step, 0], neg_ref, sems.at[0]),
        pltpu.make_async_copy(edges_hbm.at[step, 0], edge_ref, sems.at[1]),
        pltpu.make_async_copy(rel_ids_hbm.at[step], rel_id_ref, sems.at[2]),
        pltpu.make_async_copy(ent_hbm, ent_ref, sems.at[3]),
    ]
    parts = table_sems.shape[0]
    size = table_ref.shape[0] // parts
    tables = [pltpu.make_async_copy(table_hbm.at[band(n, size)], table_ref.at[band(n, size)], table_sems.at[n]) for n in range(parts)]
    for load in tables + loads:
        load.start()

    def head_of(e):
        return row_at(e >> tail_bits)

    def tail_of(e):
        return row_at(e & (2**tail_bits - 1))

    def clear(accs, n, carry):
        for acc in accs:
            acc[pl.ds(pl.multiple_of(n * chunk * 4, chunk * 4), chunk * 4), :] = jnp.zeros((chunk * 4, LANES), F32)
        return carry

    lax.fori_loop(0, table_ref.shape[0], functools.partial(clear, tail_acc), 0)
    lax.fori_loop(0, head_out.shape[0], functools.partial(clear, head_acc), 0)
    neg_grad[...] = jnp.zeros_like(neg_grad)
    gh_last[...] = jnp.zeros_like(gh_last)
    gt_last[...] = jnp.zeros_like(gt_last)
    rel_acc[...] = jnp.zeros_like(rel_acc)
    loss_acc[...] = jnp.zeros_like(loss_acc)
    for n, piece in enumerate(in_three(rel_ref[...])):
        rel_three[band(n, REL_PAD), :] = piece
    for load in loads:
        load.wait()

    def widen(n, carry):
        base = pl.multiple_of(n * chunk, chunk)
        tiles = [table_ref[n, band(t, chunk), :].astype(F32) for t in TILES[:-1]]
        tiles.append(below(unfold_last(table_ref[n, 3 * chunk:, :].astype(F32))))
        tail_rows[pl.ds(base * 4, chunk * 4), :] = stack_tiles(tiles)
        return carry

    for n, load in enumerate(tables):
        load.wait()
        lax.fori_loop(n * size, (n + 1) * size, widen, 0)

    def take_negs(n, carry):
        base = pl.multiple_of(n * UNROLL, UNROLL)

        def take(u):
            head_buf[row_at(row_address(u)), :] = tail_rows[row_at(neg_ref[base + u]), :]

        each_row(UNROLL, take)
        for t, tile in enumerate(tiles_at(head_buf, 0, UNROLL)):
            neg_rows[pl.ds(base, UNROLL), band(t, LANES)] = tile.astype(BF16)
        return carry

    lax.fori_loop(0, negs // UNROLL, take_negs, 0)

    def take_edges(base):
        def take(u):
            e = edge_ref[base + u]
            head_next[row_at(row_address(u)), :] = ent_ref[head_of(e), :]
            tail_next[row_at(row_address(u)), :] = tail_rows[tail_of(e), :]

        return take

    def put_edges(base):
        def put(pair):
            for lane in range(2):
                u = 2 * pair + lane
                e = edge_ref[base + u]
                row = row_at(row_address(u))
                head_acc[lane][head_of(e), :] += gh_last[row, :]
                tail_acc[lane][tail_of(e), :] += gt_last[row, :]

        return put

    each_row(BLOCK, take_edges(BLOCK))
    spans = [slice(r, r + STRIP) for r in range(0, BLOCK, STRIP)]

    def block(n, carry):
        base = pl.multiple_of(n * BLOCK, BLOCK)
        hot = sublanes((REL_PAD, BLOCK)) == rel_id_ref[pl.ds(n, 1), :]
        hot = jnp.where(hot, 1.0, 0.0).astype(BF16)
        rel_buf[...] = dot(below([hot] * 3), rel_three[...], COL_COL)
        for span in spans:
            head, tail, rel = tiles_at(head_next, span.start, STRIP), tiles_at(tail_next, span.start, STRIP), tiles_of(rel_buf[span, :])
            wide = slice(4 * span.start, 4 * span.stop)
            head_buf[wide, :], tail_buf[wide, :] = stack_tiles(head), stack_tiles(tail)
            total = None
            for t, q in enumerate(times(head, rel)):
                q = q.astype(BF16)
                query_buf[span, band(t, LANES)] = q
                product = q.astype(F32) * tail[t]
                total = product if total is None else total + product
            pos_buf[span, :] = row_sum(total)
        each_row(BLOCK, take_edges(base + 2 * BLOCK))
        each_row(BLOCK // 2, put_edges(base))
        score_buf[...] = dot(query_buf[...], neg_rows[...], ROW_ROW)
        for span in spans:
            weight = jnp.where(sublanes((STRIP, 1)) + (base + span.start) < count, 1.0, 0.0)
            score, pos = score_buf[span, :], pos_buf[span, :]
            top = jnp.maximum(jnp.max(score, axis=1, keepdims=True), pos)
            pos_exp = jnp.exp(pos - top)
            neg_exp = jnp.exp(score - top)
            total = pos_exp + row_sum(neg_exp)
            loss_acc[...] += jnp.sum(weight * (top + jnp.log(total) - pos), axis=0, keepdims=True)
            pos_buf[span, :] = weight * (pos_exp / total - 1.0)
            d_neg_buf[span, :] = ((weight / total) * neg_exp).astype(BF16)
        grad_buf[...] = dot(d_neg_buf[...], neg_rows[...], ROW_COL)
        neg_grad[...] += dot(d_neg_buf[...], query_buf[...], COL_COL)
        for span in spans:
            wide = slice(4 * span.start, 4 * span.stop)
            d_pos = pos_buf[span, :]
            tail, rel = tiles_at(tail_buf, span.start, STRIP), tiles_of(rel_buf[span, :])
            grad_q = [d_pos * x + y for x, y in zip(tail, tiles_of(grad_buf[span, :]))]
            gt_last[wide, :] = stack_tiles([d_pos * q.astype(F32) for q in tiles_of(query_buf[span, :])])
            gh_last[wide, :] = stack_tiles(times_conj(grad_q, rel))
            for t, grad in enumerate(times_conj(grad_q, tiles_at(head_buf, span.start, STRIP))):
                for k, piece in enumerate(in_three(grad)):
                    piece_buf[k * BLOCK + span.start:k * BLOCK + span.stop, band(t, LANES)] = piece
        rel_acc[...] += dot(beside([hot] * 3), piece_buf[...], ROW_COL)
        return carry

    blocks = pl.cdiv(count, BLOCK)
    lax.fori_loop(0, blocks, block, 0)
    each_row(BLOCK // 2, put_edges(pl.multiple_of(blocks * BLOCK, BLOCK)))

    def put_negs(n, carry):
        base = pl.multiple_of(n * UNROLL, UNROLL)
        gt_last[:4 * UNROLL, :] = stack_tiles(tiles_of(neg_grad[pl.ds(base, UNROLL), :]))

        def put(pair):
            for lane in range(2):
                u = 2 * pair + lane
                tail_acc[lane][row_at(neg_ref[base + u]), :] += gt_last[row_at(row_address(u)), :]

        each_row(UNROLL // 2, put)
        return carry

    lax.fori_loop(0, negs // UNROLL, put_negs, 0)

    def emit(out_ref, acc, n, carry):
        base = pl.multiple_of(n * chunk, chunk)
        tiles = [a + b for a, b in zip(tiles_at(acc[0], base, chunk), tiles_at(acc[1], base, chunk))]
        for t in TILES[:-1]:
            out_ref[n, band(t, chunk), :] = tiles[t]
        out_ref[n, 3 * chunk:, :] = fold_last(tiles[3])
        return carry

    stores = []
    for n in range(tail_sems.shape[0]):
        out, dst, acc, span = (head_out, head_hbm, head_acc, range(head_out.shape[0])) if n == parts else (tail_out, tail_hbm, tail_acc, range(n * size, (n + 1) * size))
        lax.fori_loop(span.start, span.stop, functools.partial(emit, out, acc), 0)
        part_of = pl.ds(span.start, len(span))
        stores.append(pltpu.make_async_copy(out.at[part_of], dst.at[part_of], tail_sems.at[n]))
        stores[-1].start()
    _, x, _, top, _ = where_here()
    group = 2 * x + top
    row = sublanes((REL_PAD, LANES))
    lane = lanes((REL_PAD, LANES))
    loss = jnp.where(lane == group, loss_acc[...], 0.0)
    for t in TILES[:-1]:
        rows = rel_acc[:, band(t, LANES)]
        rel_out[band(t, REL_PAD), :] = jnp.where(row == REL_PAD - 1, loss, rows) if t == 0 else rows
    rel_out[3 * REL_PAD:, :] = fold_last(rel_acc[:, 3 * LANES:])
    for store in stores:
        store.wait()


def dma_sems(n):
    return pltpu.SemaphoreType.DMA((n,))


def bucket_call(step, tail_bits, edges, counts, negs, rel_ids, ent, rel, table):
    smem, vmem, hbm = (pl.BlockSpec(memory_space=m) for m in (pltpu.SMEM, pltpu.VMEM, pl.ANY))
    rows, neg_count, chunks = ent.shape[0] // 4, negs.shape[-1], table.shape[0]
    width = 4 * LANES
    wire = wire_rows(CHUNK)
    block = pltpu.VMEM((BLOCK * 4, LANES), F32)
    table_rows = pltpu.VMEM((chunks * CHUNK * 4, LANES), F32)
    head_rows = pltpu.VMEM((rows * 4, LANES), F32)
    return pl.pallas_call(
        functools.partial(bucket_kernel, (step, tail_bits)),
        out_shape=(
            jax.ShapeDtypeStruct((chunks, wire, LANES), F32),
            jax.ShapeDtypeStruct((rows // CHUNK, wire, LANES), F32),
            jax.ShapeDtypeStruct((wire_rows(REL_PAD), LANES), F32),
        ),
        in_specs=[hbm, smem, hbm, hbm, hbm, vmem, hbm],
        out_specs=(hbm, hbm, vmem),
        scratch_shapes=[
            table_rows, *[block] * 6, pltpu.VMEM((BLOCK, width), F32), pltpu.VMEM((BLOCK, width), BF16), pltpu.VMEM((BLOCK, 1), F32),
            pltpu.VMEM((BLOCK, neg_count), F32), pltpu.VMEM((BLOCK, neg_count), BF16), pltpu.VMEM((BLOCK, width), F32), pltpu.VMEM((3 * BLOCK, width), BF16),
            pltpu.VMEM((neg_count, width), BF16), pltpu.VMEM((neg_count, width), F32), pltpu.VMEM((3 * REL_PAD, width), BF16),
            table_rows, table_rows, head_rows, head_rows,
            pltpu.VMEM((REL_PAD, width), F32), pltpu.VMEM((1, 1), F32),
            pltpu.SMEM((edges.shape[-1],), jnp.int32), pltpu.SMEM((neg_count,), jnp.int32), pltpu.VMEM(rel_ids.shape[1:], jnp.int32),
            pltpu.VMEM(ent.shape, F32), pltpu.VMEM(table.shape, BF16), pltpu.VMEM((chunks, wire, LANES), F32), pltpu.VMEM((rows // CHUNK, wire, LANES), F32),
            dma_sems(4), dma_sems(PARTS), dma_sems(PARTS + 1),
        ],
        compiler_params=pltpu.CompilerParams(vmem_limit_bytes=VMEM_LIMIT),
        name='bucket',
    )(edges, counts, negs, rel_ids, ent, rel, table)


def entry(peers):
    barrier = pltpu.get_barrier_semaphore()
    for peer in peers:
        pl.semaphore_signal(barrier, inc=1, device_id=peer, device_id_type=pl.DeviceIdType.MESH)
    pl.semaphore_wait(barrier, len(peers))


def remote(src, dst, send, recv, peer):
    return pltpu.make_async_remote_copy(src_ref=src, dst_ref=dst, send_sem=send, recv_sem=recv, device_id=peer, device_id_type=pl.DeviceIdType.MESH)


def adagrad(rows, state, grad, mean_of, learn_rate):
    square = grad[0] * grad[0] + grad[1] * grad[1] + grad[2] * grad[2] + grad[3] * grad[3]
    state = state + row_sum(square) / mean_of
    root = jnp.sqrt(state + EPSILON)
    return [r - learn_rate * (g / root) for r, g in zip(rows, grad)], state


def exchange_kernel(cfg, tail_ref, head_hbm, rel_grad_ref, ent_hbm, state_ref, rel_ref, rel_state_ref, *refs):
    step, groups, chunks, emb_width, last = cfg
    if last:
        ent_wire, rel_out, loss_out, *refs = refs
    else:
        ent_out, state_out, rel_out, rel_state_out, loss_out, table_hbm, *refs, table, store_sem = refs
    (own, from_core, from_y, from_group, rel_sum, rel_from, send_buf,
     own_sem, core_send, core_recv, y_send, y_recv, group_send, group_recv, rel_send, rel_recv, out_send, out_recv, head_ref, ent_ref, row_sem) = refs
    learn_rate = LR_SCALE * emb_width ** -0.25
    chunk = CHUNK
    y, x, core, top, bot = where_here()
    mine = 2 * x + top
    x_size = groups // 2

    def place(group, low, c):
        return {'data': 2 * (group % 2) + low, 'ent': 2 * (group // 2) + c}

    def at(dy, dx, c):
        return {'data': dy, 'ent': 2 * dx + c}

    def slot_of(low, c, k):
        return (low * 2 + c) * chunks + k

    def turned(shift):
        return (bot + shift) % 2

    other_core = at(y, x, 1 - core)
    other_y = at(2 * top + 1 - bot, x, core)
    rel_peers = (other_core, other_y, at(3 - y, x, core), at(y, x + 1 - 2 * (x % 2), core), at(y, x_size - 1 - x, core), other_core)
    grad_to = place((mine + step) % groups, turned(step), core)
    grad_from = place((mine + groups - step) % groups, turned(step), core)
    nxt = step + 1
    table_to = place((mine + groups - nxt) % groups, turned(nxt), core)
    table_from = place((mine + nxt) % groups, turned(nxt), core)
    peers = list(rel_peers)
    if step:
        peers += [grad_to, grad_from]
    if last:
        for turn in range(4):
            peers.append(at((y + turn) % 4, x, top))
        senders = [at((2 * core + d), x, c) for d in range(2) for c in range(2)]
        peers += senders
    else:
        peers += [table_to, table_from]
    entry(peers)
    keep = turned(step)
    pending = []

    def start(copy):
        copy.start()
        pending.append(copy)
        return copy

    shards = [(1 - keep, k) for k in range(chunks)] + [(keep, k) for k in range(chunks)]
    loads, cores = [], []
    row_loads = [pltpu.make_async_copy(src, dst, row_sem.at[n]) for n, (src, dst) in enumerate(((head_hbm, head_ref), (ent_hbm, ent_ref)))]
    for load in row_loads:
        load.start()
    stores = []

    def store(n, src, dst):
        copy = pltpu.make_async_copy(src, dst, store_sem.at[n])
        copy.start()
        stores.append(copy)

    def store_table(low, c, k):
        slot = slot_of(low, c, k)
        store(slot, table.at[slot], table_hbm.at[slot])

    rel_copies = [start(remote(rel_grad_ref.at[1 - core], rel_from.at[0], rel_send.at[0], rel_recv.at[0], rel_peers[0]))]
    for n, (low, k) in enumerate(shards):
        cores.append(start(remote(tail_ref.at[slot_of(low, 1 - core, k)], from_core.at[n], core_send.at[n], core_recv.at[n], other_core)))
        load = pltpu.make_async_copy(tail_ref.at[slot_of(low, core, k)], own.at[n], own_sem.at[n])
        load.start()
        loads.append(load)

    def rel_step(n):
        rel_copies[n].wait_recv()
        rel_sum[n] = (rel_grad_ref[core] if n == 0 else rel_sum[n - 1]) + rel_from[n]
        rel_copies.append(start(remote(rel_sum.at[n], rel_from.at[n + 1], rel_send.at[n + 1], rel_recv.at[n + 1], rel_peers[n + 1])))

    ys = []
    for k in range(chunks):
        loads[k].wait()
        cores[k].wait_recv()
        own[k] = own[k] + from_core[k]
        ys.append(start(remote(own.at[k], from_y.at[k], y_send.at[k], y_recv.at[k], other_y)))
        if k == 1:
            rel_step(0)
    for k in range(chunks, 2 * chunks):
        loads[k].wait()
        cores[k].wait_recv()
        own[k] = own[k] + from_core[k]
    gs, outs, forwards, crosses = [], [], [], []

    def stage_group(k):
        ys[k].wait_recv()
        own[chunks + k] = own[chunks + k] + from_y[k]
        if step:
            gs.append(start(remote(own.at[chunks + k], from_group.at[k], group_send.at[k], group_recv.at[k], grad_to)))

    def cross_copy(k):
        return remote(send_buf.at[k], ent_wire.at[slot_of(bot, core, k)], out_send.at[2 * chunks + k], out_recv.at[slot_of(bot, core, k)], other_core)

    turn = (y + 4 - 2 * core) % 4
    near = 1 - turn % 2
    back = jnp.where((turn == 1) | (turn == 2), 0, 1)
    onward = at((y + 1 + 2 * back) % 4, x, core)

    def landed(low, c, k):
        slot = slot_of(low, c, k)
        remote(ent_wire.at[slot], ent_wire.at[slot], out_send.at[0], out_recv.at[slot], other_core).wait_recv()

    def stage_relay(k):
        if k % 2 == 0:
            return
        for c in CORES:
            landed(near, c, k - 1)
            landed(near, c, k)
            slot = slot_of(near, c, k) - 1 + back
            start(remote(ent_wire.at[slot], ent_wire.at[slot], out_send.at[(3 + c) * chunks + k], out_recv.at[slot], onward))

    def stage_update(k):
        if k == 0:
            for load in row_loads:
                load.wait()
        if step:
            gs[k].wait_recv()
        total = from_group if step else own
        base = k if step else chunks + k
        grad = [total[base, band(t, chunk), :] + head_ref[k, band(t, chunk), :] for t in TILES[:-1]]
        grad.append(below(unfold_last(total[base, 3 * chunk:, :] + head_ref[k, 3 * chunk:, :])))
        span = band(k, chunk)
        rows, state = adagrad(tiles_at(ent_ref, k * chunk, chunk), state_ref[span, :], grad, emb_width, learn_rate)
        wire = rows[:3] + [fold_last(rows[3])]
        if last:
            lane = lanes((chunk, LANES))
            wire.append(fold_last(jnp.where(lane < 1, state, 0.0)))
        else:
            wide = band(k, 4 * chunk)
            ent_ref[wide, :] = stack_tiles(rows)
            store(4 * chunks + k, ent_ref.at[wide], ent_out.at[wide])
            state_out[span, :] = state
        offset = 0
        for piece in wire:
            send_buf[k, offset:offset + piece.shape[0], :] = piece.astype(send_buf.dtype)
            offset += piece.shape[0]
        slot = slot_of(bot, core, k)
        if last:
            for n, turn in enumerate((1, 3)):
                start(remote(send_buf.at[k], ent_wire.at[slot], out_send.at[n * chunks + k], out_recv.at[slot], at((y + turn) % 4, x, top)))

            @pl.when(core == top)
            def _():
                pltpu.make_async_copy(send_buf.at[k], ent_wire.at[slot], out_recv.at[slot]).start()

            @pl.when(core != top)
            def _():
                cross_copy(k).start()
        else:
            outs.append(start(remote(send_buf.at[k], table.at[slot], out_send.at[k], out_recv.at[k], table_to)))

    def forward(n, low, k, peer):
        slot = slot_of(low, core, k)
        return start(remote(table.at[slot], table.at[slot], out_send.at[n * chunks + k], out_recv.at[n * chunks + k], peer))

    def stage_forward(k):
        outs[k].wait_recv()
        store_table(turned(nxt), core, k)
        forwards.append(forward(1, turned(nxt), k, other_y))
        crosses.append(forward(2, turned(nxt), k, other_core))

    def stage_cross(k):
        forwards[k].wait_recv()
        store_table(1 - turned(nxt), core, k)
        crosses.append(forward(3, 1 - turned(nxt), k, other_core))

    stages = (stage_group, stage_update, stage_relay) if last else (stage_group, stage_update, stage_forward, stage_cross)
    rel_steps = len(rel_peers) - 1
    for tick in range(chunks + LAG * (len(stages) - 1)):
        for n, stage in enumerate(stages):
            if 0 <= tick - LAG * n < chunks:
                stage(tick - LAG * n)
        if tick % 2 == 1 and tick < 2 * rel_steps - 1:
            rel_step(tick // 2 + 1)

    rel_copies[rel_steps].wait_recv()
    halves = rel_sum[rel_steps - 1], rel_from[rel_steps]
    summed = below([jnp.where(core == n, halves[0], halves[1]) for n in CORES])
    rel_grad = [summed[band(t, REL_PAD)] for t in TILES[:-1]] + [below(unfold_last(summed[3 * REL_PAD:]))]
    loss_out[...] = rel_grad[0][REL_PAD - 1:, :]
    row = sublanes((REL_PAD, LANES))
    rel_grad[0] = jnp.where(row < REL_PAD - 1, rel_grad[0], 0.0)
    rel_rows, rel_state = adagrad(tiles_of(rel_ref[...]), rel_state_ref[...], rel_grad, emb_width, learn_rate)
    for t in TILES:
        rel_out[:, band(t, LANES)] = rel_rows[t]
    if not last:
        rel_state_out[...] = rel_state

    if last:
        for c in CORES:
            for k in range(chunks):
                landed(1 - near, c, k)

        @pl.when(core != top)
        def _():
            for k in range(chunks):
                cross_copy(k).wait_send()
    else:
        for n, copy in enumerate(crosses):
            copy.wait_recv()
        for low in CORES:
            for k in range(chunks):
                store_table(low, 1 - core, k)
        for copy in stores:
            copy.wait()
    for copy in pending:
        copy.wait_send()


def exchange_call(step, groups, emb_width, tail, head, rel_grad, ent, state, rel, rel_state):
    vmem, hbm = pl.BlockSpec(memory_space=pltpu.VMEM), pl.BlockSpec(memory_space=pl.ANY)
    chunks = head.shape[0]
    rel_grad = rel_grad.reshape(2, -1, LANES)
    wire = wire_rows(CHUNK)
    last = step == groups - 1
    like = lambda x: jax.ShapeDtypeStruct(x.shape, x.dtype)
    loss = jax.ShapeDtypeStruct((1, LANES), F32)
    out_wire = wire + (CHUNK // LEFT if last else 0)
    out_type = F32 if last else BF16
    gathered = jax.ShapeDtypeStruct((4 * chunks, out_wire, LANES), out_type)
    out_shape = (gathered, like(rel), loss) if last else (like(ent), like(state), like(rel), like(rel_state), loss, gathered)
    return pl.pallas_call(
        functools.partial(exchange_kernel, (step, groups, chunks, emb_width, last)),
        out_shape=out_shape,
        in_specs=[hbm, hbm, vmem, hbm, vmem, vmem, vmem],
        out_specs=(vmem,) * 3 if last else (hbm, vmem, vmem, vmem, vmem, hbm),
        scratch_shapes=[
            pltpu.VMEM((2 * chunks, wire, LANES), F32), pltpu.VMEM((2 * chunks, wire, LANES), F32),
            pltpu.VMEM((chunks, wire, LANES), F32), pltpu.VMEM((chunks, wire, LANES), F32),
            pltpu.VMEM((REL_HOPS - 1, *rel_grad.shape[1:]), F32), pltpu.VMEM((REL_HOPS, *rel_grad.shape[1:]), F32),
            pltpu.VMEM((chunks, out_wire, LANES), out_type),
            *[dma_sems(2 * chunks)] * 3, *[dma_sems(chunks)] * 4,
            dma_sems(REL_HOPS), dma_sems(REL_HOPS), dma_sems(5 * chunks), dma_sems(4 * chunks),
            pltpu.VMEM(head.shape, F32), pltpu.VMEM(ent.shape, F32), dma_sems(2),
            *(() if last else (pltpu.VMEM(gathered.shape, BF16), dma_sems(5 * chunks))),
        ],
        compiler_params=pltpu.CompilerParams(vmem_limit_bytes=VMEM_LIMIT, collective_id=step, has_side_effects=True),
        name='exchange',
    )(tail, head, rel_grad, ent, state, rel, rel_state)


def index_kernel(cfg, head_ref, tail_ref, rel_ref, mask_ref, neg_ref, word_out, rel_id_out, count_out, neg_out, packed, shares, neg_buf, send_sem, recv_sem, neg_send, neg_recv):
    head_bits, tail_bits, spare = cfg
    y, x, core, top, bot = where_here()
    own = 2 * x + core
    other_core = {'data': y, 'ent': 2 * x + 1 - core}
    users = [(c, 2 * core + d) for c in range(2) for d in range(2)]
    users = [({'data': row, 'ent': 2 * x + c}, (core == c) & (y == row)) for c, row in users]
    entry([peer for peer, _ in users] + [{'data': row, 'ent': 2 * x + top} for row in range(4)] + [other_core])
    edges = head_ref[...] | (tail_ref[...] << tail_bits) | (rel_ref[...] << (2 * tail_bits))
    packed[...] = jnp.where(mask_ref[...] > 0, edges, spare << (2 * tail_bits))
    neg_buf[...] = row_address(neg_ref[...])
    to_users = [remote(packed, shares.at[y], send_sem.at[n], recv_sem.at[y], peer) for n, (peer, _) in enumerate(users)]
    for copy, (_, here) in zip(to_users, users):
        @pl.when(jnp.logical_not(here))
        def _():
            copy.start()

    @pl.when(core == top)
    def _():
        pltpu.make_async_copy(packed, shares.at[y], recv_sem.at[y]).start()
        remote(neg_buf, neg_out, neg_send, neg_recv, other_core).start()
        neg_out[...] = neg_buf[...]

    for row in TILES:
        remote(packed, shares.at[row], send_sem.at[0], recv_sem.at[row], other_core).wait_recv()
    share = beside([shares[row] for row in TILES])
    mine = ((share >> head_bits) & 3 == 2 * bot + core) & (share >> (2 * tail_bits) != spare)
    lane = lanes(share.shape)
    width = share.shape[1]
    steps = (width - 1).bit_length()
    other = jnp.where(mine, 0, 1)
    before = other
    for bit in range(steps):
        before = before + jnp.where(lane < 2**bit, 0, roll(before, 2**bit))
    count_out[...] = jnp.broadcast_to(width - before[:, width - 1:], count_out.shape)
    none = spare << (head_bits + tail_bits)
    edge = jnp.where(mine, (share & (2**head_bits - 1)) | (share >> tail_bits << head_bits), none)
    shift = jnp.where(mine, before - other, 0)
    for bit in range(steps):
        here = (shift >> bit) & 1 == 1
        edge_in, shift_in = roll(edge, width - 2**bit), roll(shift, width - 2**bit)
        there = (shift_in >> bit) & 1 == 1
        edge = jnp.where(there, edge_in, jnp.where(here, none, edge))
        shift = jnp.where(there, shift_in, jnp.where(here, 0, shift))
    rel_id_out[...] = edge >> (head_bits + tail_bits)
    head, tail = edge & (2**head_bits - 1), (edge >> head_bits) & (2**tail_bits - 1)
    margin = jnp.zeros((share.shape[0], BLOCK), jnp.int32)
    word_out[...] = beside([margin, (row_address(head) << (tail_bits + 2)) | row_address(tail), margin])
    for copy, (_, here) in zip(to_users, users):
        @pl.when(jnp.logical_not(here))
        def _():
            copy.wait_send()

    @pl.when(core == top)
    def _():
        remote(neg_buf, neg_out, neg_send, neg_recv, other_core).wait_send()

    @pl.when(core != top)
    def _():
        remote(neg_buf, neg_out, neg_send, neg_recv, other_core).wait_recv()


def index_call(cfg, head, tail, rel, mask, neg, reps):
    vmem = pl.BlockSpec(memory_space=pltpu.VMEM)
    groups, share = head.shape
    return pl.pallas_call(
        functools.partial(index_kernel, cfg),
        out_shape=tuple(jax.ShapeDtypeStruct((groups, n), jnp.int32) for n in (reps * share + 2 * BLOCK, reps * share, LANES, neg.shape[1])),
        in_specs=[vmem] * 5,
        out_specs=(vmem,) * 4,
        scratch_shapes=[pltpu.VMEM(head.shape, jnp.int32), pltpu.VMEM((reps, *head.shape), jnp.int32), pltpu.VMEM(neg.shape, jnp.int32),
                        pltpu.SemaphoreType.DMA((4,)), pltpu.SemaphoreType.DMA((4,)), pltpu.SemaphoreType.DMA, pltpu.SemaphoreType.DMA],
        compiler_params=pltpu.CompilerParams(collective_id=20, has_side_effects=True),
        name='setup_index',
    )(head, tail, rel, mask, neg)


def rows_kernel(ent_hbm, rel_ref, table, ent_out, rel_out, rows_buf, away, load_sem, table_send, table_recv, ent_send, ent_recv):
    y, x, core, top, bot = where_here()
    other_core = {'data': y, 'ent': 2 * x + 1 - core}
    chunks, chunk = table.shape[0], CHUNK
    shard = chunks // 4
    entry([other_core])
    for t, tile in enumerate(columns_to_tiles(rel_ref[...])):
        rel_out[:, band(t, LANES)] = tile

    def load(n):
        return pltpu.make_async_copy(ent_hbm.at[:, pl.ds(pl.multiple_of(n * chunk, chunk), chunk)], rows_buf.at[n % 4], load_sem.at[n % 4])

    def table_copy(q):
        part = table.at[pl.ds(q * shard, shard)]
        return remote(part, part, table_send.at[q], table_recv.at[q], other_core)

    ent_copy = remote(away, ent_out, ent_send, ent_recv, other_core)

    @pl.when(core == top)
    def _():
        for n in range(3):
            load(n).start()
        for q in range(4):
            def one(k, carry):
                n = q * shard + k

                @pl.when(n + 3 < chunks)
                def _():
                    load(n + 3).start()

                load(n).wait()
                tiles = columns_to_tiles(rows_buf[n % 4])
                for t in TILES[:-1]:
                    table[n, band(t, chunk), :] = tiles[t].astype(BF16)
                table[n, 3 * chunk:, :] = fold_last(tiles[3]).astype(BF16)
                place = pl.ds(pl.multiple_of(k * chunk * 4, chunk * 4), chunk * 4)

                @pl.when(2 * bot + core == q)
                def _():
                    ent_out[place, :] = stack_tiles(tiles)

                @pl.when(2 * bot + 1 - core == q)
                def _():
                    away[place, :] = stack_tiles(tiles)

                return carry

            lax.fori_loop(0, shard, one, 0)
            table_copy(q).start()

            @pl.when(2 * bot + 1 - core == q)
            def _():
                ent_copy.start()

        for q in range(4):
            table_copy(q).wait_send()
        ent_copy.wait_send()

    @pl.when(core != top)
    def _():
        for q in range(4):
            table_copy(q).wait_recv()
        ent_copy.wait_recv()


def rows_call(ent, rel):
    vmem, hbm = pl.BlockSpec(memory_space=pltpu.VMEM), pl.BlockSpec(memory_space=pl.ANY)
    width, rows = ent.shape
    chunks = rows // CHUNK
    dma = pltpu.SemaphoreType.DMA
    return pl.pallas_call(
        rows_kernel,
        out_shape=(jax.ShapeDtypeStruct((chunks, wire_rows(CHUNK), LANES), BF16), jax.ShapeDtypeStruct((rows, LANES), F32), jax.ShapeDtypeStruct((REL_PAD, 4 * LANES), F32)),
        in_specs=[hbm, vmem],
        out_specs=(vmem,) * 3,
        scratch_shapes=[pltpu.VMEM((4, width, CHUNK), F32), pltpu.VMEM((rows, LANES), F32), dma((4,)), dma((4,)), dma((4,)), dma, dma],
        compiler_params=pltpu.CompilerParams(collective_id=21, has_side_effects=True),
        cost_estimate=pl.CostEstimate(flops=10**9, bytes_accessed=2 * 10**7, transcendentals=0),
        name='setup_rows',
    )(ent, rel)


def finish_kernel(wire_ref, rel_ref, ent_out, rel_out):
    chunk = CHUNK
    for n in range(wire_ref.shape[0]):
        tiles = [wire_ref[n, band(t, chunk), :] for t in TILES[:-1]]
        tiles.append(below(unfold_last(wire_ref[n, 3 * chunk:wire_rows(chunk), :])))
        ent_out[:, band(n, chunk)] = tiles_to_columns(tiles)

    @pl.when(pl.program_id(0) == 0)
    def _():
        rel_out[...] = tiles_to_columns(tiles_of(rel_ref[...]))


def finish_call(wire, rel, width):
    chunks = wire.shape[0]
    size = chunks // 8
    whole = lambda n: (0, 0)
    return pl.pallas_call(
        finish_kernel,
        out_shape=(jax.ShapeDtypeStruct((width, chunks * CHUNK), F32), jax.ShapeDtypeStruct((width, REL_PAD), F32)),
        grid=(chunks // size,),
        in_specs=[pl.BlockSpec((size, *wire.shape[1:]), lambda n: (n, 0, 0)), pl.BlockSpec(rel.shape, whole)],
        out_specs=(pl.BlockSpec((width, size * CHUNK), lambda n: (0, n)), pl.BlockSpec((width, REL_PAD), whole)),
        name='finish',
    )(wire, rel)


def solution(mesh):
    groups = mesh.shape['ent']
    data_reps = mesh.shape['data']
    row_spec = P(('sweep', 'ent'), None)
    edge_spec = P(('sweep', 'ent'), None, 'data')

    def device_fn(ent_table, ent_state, rel_table, head_idx, tail_idx, rel_idx, edge_mask, neg_idx):
        part_rows, emb_width = ent_table.shape
        rel_rows = rel_table.shape[0]
        bucket_edges = head_idx.shape[2] * data_reps
        shard = part_rows // 4
        tail_bits = (part_rows - 1).bit_length()
        head_bits = (shard - 1).bit_length()
        spare = 2**(REL_PAD - 1).bit_length() - 1
        ent = lax.axis_index('ent')
        _, _, core, top, bot = where_here()

        words, rel_ids, counts, neg = index_call((head_bits, tail_bits, spare), head_idx[0], tail_idx[0], rel_idx[0], edge_mask[0], neg_idx[0], data_reps)
        words, neg, counts = words[:, None], neg[:, None], counts[:, 0]
        rel_ids = rel_ids.reshape(groups, -1, BLOCK)

        table, ent_now, rel_now = rows_call(ent_table.T, jnp.pad(rel_table.T, ((0, 0), (0, REL_PAD - rel_rows))))
        to_core = lambda c: lax.dynamic_slice_in_dim(ent_state, (2 * bot + c) * shard, shard)
        away = [(d * groups + 2 * (n // 2) + d // 2, d * groups + 2 * (n // 2) + 1 - d // 2) for d in range(data_reps) for n in range(0, groups, 2)]
        state_now = jnp.where(core == top, to_core(core), lax.ppermute(to_core(1 - core), ('data', 'ent'), away))[:, None]
        rel_state = jnp.zeros((REL_PAD, 1), F32)
        losses = []
        for step in range(groups):
            tail, head, rel_grad = bucket_call(step, tail_bits + 2, words, counts, neg, rel_ids, ent_now, rel_now, table)
            out = exchange_call(step, groups, emb_width, tail, head, rel_grad, ent_now, state_now, rel_now, rel_state)
            if step + 1 < groups:
                ent_now, state_now, rel_now, rel_state, loss, table = out
            else:
                wire, rel_now, loss = out
            losses.append(loss)
        ent_out, rel_out = finish_call(wire, rel_now, emb_width)
        state_out = wire[:, wire_rows(CHUNK):, :HALF:LEFT].transpose(0, 2, 1).reshape(part_rows)
        loss_rows = below(losses) / bucket_edges
        bucket_loss = lax.dynamic_slice_in_dim(loss_rows, ent, 1, axis=1).reshape(1, groups)
        return ent_out.T, state_out, rel_out[:, :rel_rows].T, bucket_loss

    return jax.shard_map(device_fn, mesh=mesh, in_specs=(row_spec, P(('sweep', 'ent')), P('sweep', None), edge_spec, edge_spec, edge_spec, edge_spec, P(('sweep', 'ent'), None, None)), out_specs=(row_spec, P(('sweep', 'ent')), P('sweep', None), row_spec), check_vma=False)
```

```python
import functools

import jax
import jax.numpy as jnp
from jax import lax
from jax.experimental import pallas as pl
from jax.experimental.pallas import tpu as pltpu
from jax.sharding import PartitionSpec as P

LR_SCALE = 0.2
EPSILON = 1e-8
LANES = 128
HALF = 64
LEFT = 8
BLOCK = 256
CHUNK = 128
UNROLL = 64
ROLLED = 32
LAG = 3
PARTS = 4
REL_HOPS = 6
STRIP = 32
REL_PAD = 128
TILES = range(4)
CORES = range(2)
ROW_COL, ROW_ROW, COL_COL = (((1,), (0,)), ((1,), (1,)), ((0,), (0,)))
F32 = jnp.float32
BF16 = jnp.bfloat16
VMEM_LIMIT = 60 * 2**20


def roll(x, by):
    return pltpu.roll(x, by, 1)


def beside(parts):
    return jnp.concatenate(parts, axis=1)


def below(parts):
    return jnp.concatenate(parts, axis=0)


def lanes(shape):
    return lax.broadcasted_iota(jnp.int32, shape, 1)


def sublanes(shape):
    return lax.broadcasted_iota(jnp.int32, shape, 0)


def row_sum(x):
    return jnp.sum(x, axis=1, keepdims=True)


def wire_rows(rows):
    return 3 * rows + rows // LEFT


def columns_to_tiles(x):
    half = x.shape[0] // 2
    a, c, d = slice(0, LANES), slice(LANES, LANES + HALF), slice(LANES + HALF, half)
    re, im = x[:half], x[half:]
    zero = jnp.zeros((HALF - LEFT, x.shape[1]), x.dtype)
    return [t.T for t in (re[a], im[a], below([re[c], im[c]]), below([re[d], zero, im[d], zero]))]


def tiles_to_columns(tiles):
    a, b, c, d = (t.T for t in tiles)
    high = slice(HALF, HALF + LEFT)
    return below([a, c[:HALF], d[:LEFT], b, c[HALF:], d[high]])


def each_row(count, body):
    for u in range(count):
        body(u)


def band(n, size):
    return slice(n * size, (n + 1) * size)


def where_here():
    y, ent = lax.axis_index('data'), lax.axis_index('ent')
    return y, ent // 2, ent % 2, y // 2, y % 2


def fold_last(tile):
    n = tile.shape[0] // LEFT
    out = tile[:n]
    for k in range(1, LEFT):
        out = out + roll(tile[band(k, n)], LEFT * k)
    return out


def unfold_last(packed):
    keep = lanes(packed.shape) % HALF < LEFT
    return [jnp.where(keep, packed if k == 0 else roll(packed, LANES - LEFT * k), 0.0) for k in range(LEFT)]


def tiles_of(x):
    return [x[:, band(t, LANES)] for t in TILES]


def times(x, y):
    out = [x[0] * y[0] - x[1] * y[1], x[0] * y[1] + x[1] * y[0]]
    for a, b in zip(x[2:], y[2:]):
        low = lanes(a.shape) < HALF
        a_swap, b_swap = roll(a, HALF), roll(b, HALF)
        out.append(jnp.where(low, a * b - a_swap * b_swap, a_swap * b + a * b_swap))
    return out


def times_conj(x, y):
    out = [x[0] * y[0] + x[1] * y[1], x[1] * y[0] - x[0] * y[1]]
    for a, b in zip(x[2:], y[2:]):
        low = lanes(a.shape) < HALF
        a_swap, b_swap = roll(a, HALF), roll(b, HALF)
        out.append(jnp.where(low, a * b + a_swap * b_swap, a * b_swap - a_swap * b))
    return out


def tiles_at(ref, row, rows):
    block = ref[pl.ds(row * 4, rows * 4), :].reshape(rows // 8, 32, LANES)
    return [block[:, 8 * t:8 * t + 8].reshape(rows, LANES) for t in TILES]


def stack_tiles(tiles):
    rows = tiles[0].shape[0]
    return beside([t.reshape(rows // 8, 8, LANES) for t in tiles]).reshape(rows * 4, LANES)


def row_at(address):
    return pl.ds(address, 4, stride=8)


def row_address(row):
    return (row >> 3 << 5) | (row & 7)


def in_three(x):
    pieces = []
    for _ in range(3):
        piece = x.astype(BF16)
        pieces.append(piece)
        x = x - piece.astype(F32)
    return pieces


def dot(x, y, dims):
    return lax.dot_general(x, y, (dims, ((), ())), preferred_element_type=F32)


def bucket_kernel(cfg, edges_hbm, count_ref, negs_hbm, rel_ids_hbm, ent_hbm, rel_ref, table_hbm, tail_hbm, head_hbm, rel_out,
                  tail_rows, head_next, tail_next, head_buf, tail_buf, gh_last, gt_last, rel_buf, query_buf, pos_buf, score_buf, d_neg_buf, grad_buf, piece_buf,
                  neg_rows, neg_grad, rel_three, tail_acc0, tail_acc1, head_acc0, head_acc1, rel_acc, loss_acc,
                  edge_ref, neg_ref, rel_id_ref, ent_ref, table_ref, tail_out, head_out, sems, table_sems, tail_sems):
    step, tail_bits = cfg
    chunk = CHUNK
    part = chunk // LEFT
    tail_acc, head_acc = (tail_acc0, tail_acc1), (head_acc0, head_acc1)
    count = count_ref[step]
    negs = neg_ref.shape[0]
    loads = [
        pltpu.make_async_copy(negs_hbm.at[step, 0], neg_ref, sems.at[0]),
        pltpu.make_async_copy(rel_ids_hbm.at[step], rel_id_ref, sems.at[2]),
        pltpu.make_async_copy(ent_hbm, ent_ref, sems.at[3]),
    ]
    parts = table_sems.shape[0]
    size = table_ref.shape[0] // parts
    tables = [pltpu.make_async_copy(table_hbm.at[band(n, size)], table_ref.at[band(n, size)], table_sems.at[n]) for n in range(parts)]
    blocks = pl.cdiv(count, BLOCK)

    def edge_pieces(act):
        def one(n, carry):
            span = pl.ds(pl.multiple_of(n * 2 * BLOCK, 2 * BLOCK), 2 * BLOCK)
            act(pltpu.make_async_copy(edges_hbm.at[step, 0, span], edge_ref.at[span], sems.at[1]))
            return carry

        lax.fori_loop(0, (blocks + 3) // 2, one, 0)

    edge_pieces(lambda copy: copy.start())
    for load in loads + tables:
        load.start()

    def head_of(e):
        return row_at(e >> tail_bits)

    def tail_of(e):
        return row_at(e & (2**tail_bits - 1))

    def clear(accs, n, carry):
        for acc in accs:
            acc[pl.ds(pl.multiple_of(n * chunk * 4, chunk * 4), chunk * 4), :] = jnp.zeros((chunk * 4, LANES), F32)
        return carry

    lax.fori_loop(0, table_ref.shape[0], functools.partial(clear, tail_acc), 0)
    lax.fori_loop(0, head_out.shape[0], functools.partial(clear, head_acc), 0)
    neg_grad[...] = jnp.zeros_like(neg_grad)
    gh_last[...] = jnp.zeros_like(gh_last)
    gt_last[...] = jnp.zeros_like(gt_last)
    rel_acc[...] = jnp.zeros_like(rel_acc)
    loss_acc[...] = jnp.zeros_like(loss_acc)
    for n, piece in enumerate(in_three(rel_ref[...])):
        rel_three[band(n, REL_PAD), :] = piece
    for load in loads:
        load.wait()
    edge_pieces(lambda copy: copy.wait())

    def widen(n, carry):
        base = pl.multiple_of(n * chunk, chunk)
        tiles = [table_ref[n, band(t, chunk), :].astype(F32) for t in TILES[:-1]]
        tiles.append(below(unfold_last(table_ref[n, 3 * chunk:, :].astype(F32))))
        tail_rows[pl.ds(base * 4, chunk * 4), :] = stack_tiles(tiles)
        return carry

    for n, load in enumerate(tables):
        load.wait()
        lax.fori_loop(n * size, (n + 1) * size, widen, 0)

    def take_negs(n, carry):
        base = pl.multiple_of(n * UNROLL, UNROLL)

        def take(u):
            head_buf[row_at(row_address(u)), :] = tail_rows[row_at(neg_ref[base + u]), :]

        each_row(UNROLL, take)
        for t, tile in enumerate(tiles_at(head_buf, 0, UNROLL)):
            neg_rows[pl.ds(base, UNROLL), band(t, LANES)] = tile.astype(BF16)
        return carry

    lax.fori_loop(0, negs // UNROLL, take_negs, 0)

    def take_edges(base, row=0):
        def take(u):
            e = edge_ref[base + u]
            place = row_at(row * 4 + row_address(u))
            head_next[place, :] = ent_ref[head_of(e), :]
            tail_next[place, :] = tail_rows[tail_of(e), :]

        return take

    def put_edges(base, row=0):
        def put(pair):
            for lane in range(2):
                u = 2 * pair + lane
                e = edge_ref[base + u]
                place = row_at(row * 4 + row_address(u))
                head_acc[lane][head_of(e), :] += gh_last[place, :]
                tail_acc[lane][tail_of(e), :] += gt_last[place, :]

        return put


    def take_first(n, carry):
        row = pl.multiple_of(n * ROLLED, ROLLED)
        each_row(ROLLED, take_edges(BLOCK + row, row))
        return carry

    lax.fori_loop(0, BLOCK // ROLLED, take_first, 0)
    spans = [slice(r, r + STRIP) for r in range(0, BLOCK, STRIP)]

    def block(n, carry):
        base = pl.multiple_of(n * BLOCK, BLOCK)
        hot = sublanes((REL_PAD, BLOCK)) == rel_id_ref[pl.ds(n, 1), :]
        hot = jnp.where(hot, 1.0, 0.0).astype(BF16)
        rel_buf[...] = dot(below([hot] * 3), rel_three[...], COL_COL)
        for span in spans:
            head, tail, rel = tiles_at(head_next, span.start, STRIP), tiles_at(tail_next, span.start, STRIP), tiles_of(rel_buf[span, :])
            wide = slice(4 * span.start, 4 * span.stop)
            head_buf[wide, :], tail_buf[wide, :] = stack_tiles(head), stack_tiles(tail)
            total = None
            for t, q in enumerate(times(head, rel)):
                q = q.astype(BF16)
                query_buf[span, band(t, LANES)] = q
                product = q.astype(F32) * tail[t]
                total = product if total is None else total + product
            pos_buf[span, :] = row_sum(total)
        each_row(BLOCK, take_edges(base + 2 * BLOCK))
        each_row(BLOCK // 2, put_edges(base))
        score_buf[...] = dot(query_buf[...], neg_rows[...], ROW_ROW)
        for span in spans:
            weight = jnp.where(sublanes((STRIP, 1)) + (base + span.start) < count, 1.0, 0.0)
            score, pos = score_buf[span, :], pos_buf[span, :]
            top = jnp.maximum(jnp.max(score, axis=1, keepdims=True), pos)
            pos_exp = jnp.exp(pos - top)
            neg_exp = jnp.exp(score - top)
            total = pos_exp + row_sum(neg_exp)
            loss_acc[...] += jnp.sum(weight * (top + jnp.log(total) - pos), axis=0, keepdims=True)
            pos_buf[span, :] = weight * (pos_exp / total - 1.0)
            d_neg_buf[span, :] = ((weight / total) * neg_exp).astype(BF16)
        grad_buf[...] = dot(d_neg_buf[...], neg_rows[...], ROW_COL)
        neg_grad[...] += dot(d_neg_buf[...], query_buf[...], COL_COL)
        for span in spans:
            wide = slice(4 * span.start, 4 * span.stop)
            d_pos = pos_buf[span, :]
            tail, rel = tiles_at(tail_buf, span.start, STRIP), tiles_of(rel_buf[span, :])
            grad_q = [d_pos * x + y for x, y in zip(tail, tiles_of(grad_buf[span, :]))]
            gt_last[wide, :] = stack_tiles([d_pos * q.astype(F32) for q in tiles_of(query_buf[span, :])])
            gh_last[wide, :] = stack_tiles(times_conj(grad_q, rel))
            for t, grad in enumerate(times_conj(grad_q, tiles_at(head_buf, span.start, STRIP))):
                for k, piece in enumerate(in_three(grad)):
                    piece_buf[k * BLOCK + span.start:k * BLOCK + span.stop, band(t, LANES)] = piece
        rel_acc[...] += dot(beside([hot] * 3), piece_buf[...], ROW_COL)
        return carry

    lax.fori_loop(0, blocks, block, 0)

    def put_last(n, carry):
        row = pl.multiple_of(n * ROLLED, ROLLED)
        each_row(ROLLED // 2, put_edges(blocks * BLOCK + row, row))
        return carry

    lax.fori_loop(0, BLOCK // ROLLED, put_last, 0)

    def put_negs(n, carry):
        base = pl.multiple_of(n * UNROLL, UNROLL)
        gt_last[:4 * UNROLL, :] = stack_tiles(tiles_of(neg_grad[pl.ds(base, UNROLL), :]))

        def put(pair):
            for lane in range(2):
                u = 2 * pair + lane
                tail_acc[lane][row_at(neg_ref[base + u]), :] += gt_last[row_at(row_address(u)), :]

        each_row(UNROLL // 2, put)
        return carry

    lax.fori_loop(0, negs // UNROLL, put_negs, 0)

    def emit(out_ref, acc, n, carry):
        base = pl.multiple_of(n * chunk, chunk)
        tiles = [a + b for a, b in zip(tiles_at(acc[0], base, chunk), tiles_at(acc[1], base, chunk))]
        for t in TILES[:-1]:
            out_ref[n, band(t, chunk), :] = tiles[t]
        out_ref[n, 3 * chunk:, :] = fold_last(tiles[3])
        return carry

    stores = []
    for n in range(tail_sems.shape[0]):
        out, dst, acc, span = (head_out, head_hbm, head_acc, range(head_out.shape[0])) if n == parts else (tail_out, tail_hbm, tail_acc, range(n * size, (n + 1) * size))
        lax.fori_loop(span.start, span.stop, functools.partial(emit, out, acc), 0)
        part_of = pl.ds(span.start, len(span))
        stores.append(pltpu.make_async_copy(out.at[part_of], dst.at[part_of], tail_sems.at[n]))
        stores[-1].start()
    _, x, _, top, _ = where_here()
    group = 2 * x + top
    row = sublanes((REL_PAD, LANES))
    lane = lanes((REL_PAD, LANES))
    loss = jnp.where(lane == group, loss_acc[...], 0.0)
    for t in TILES[:-1]:
        rows = rel_acc[:, band(t, LANES)]
        rel_out[band(t, REL_PAD), :] = jnp.where(row == REL_PAD - 1, loss, rows) if t == 0 else rows
    rel_out[3 * REL_PAD:, :] = fold_last(rel_acc[:, 3 * LANES:])
    for store in stores:
        store.wait()


def dma_sems(n):
    return pltpu.SemaphoreType.DMA((n,))


def bucket_call(step, tail_bits, edges, counts, negs, rel_ids, ent, rel, table):
    smem, vmem, hbm = (pl.BlockSpec(memory_space=m) for m in (pltpu.SMEM, pltpu.VMEM, pl.ANY))
    rows, neg_count, chunks = ent.shape[0] // 4, negs.shape[-1], table.shape[0]
    width = 4 * LANES
    wire = wire_rows(CHUNK)
    block = pltpu.VMEM((BLOCK * 4, LANES), F32)
    table_rows = pltpu.VMEM((chunks * CHUNK * 4, LANES), F32)
    head_rows = pltpu.VMEM((rows * 4, LANES), F32)
    return pl.pallas_call(
        functools.partial(bucket_kernel, (step, tail_bits)),
        out_shape=(
            jax.ShapeDtypeStruct((chunks, wire, LANES), F32),
            jax.ShapeDtypeStruct((rows // CHUNK, wire, LANES), F32),
            jax.ShapeDtypeStruct((wire_rows(REL_PAD), LANES), F32),
        ),
        in_specs=[hbm, smem, hbm, hbm, hbm, vmem, hbm],
        out_specs=(hbm, hbm, vmem),
        scratch_shapes=[
            table_rows, *[block] * 6, pltpu.VMEM((BLOCK, width), F32), pltpu.VMEM((BLOCK, width), BF16), pltpu.VMEM((BLOCK, 1), F32),
            pltpu.VMEM((BLOCK, neg_count), F32), pltpu.VMEM((BLOCK, neg_count), BF16), pltpu.VMEM((BLOCK, width), F32), pltpu.VMEM((3 * BLOCK, width), BF16),
            pltpu.VMEM((neg_count, width), BF16), pltpu.VMEM((neg_count, width), F32), pltpu.VMEM((3 * REL_PAD, width), BF16),
            table_rows, table_rows, head_rows, head_rows,
            pltpu.VMEM((REL_PAD, width), F32), pltpu.VMEM((1, 1), F32),
            pltpu.SMEM((edges.shape[-1],), jnp.int32), pltpu.SMEM((neg_count,), jnp.int32), pltpu.VMEM(rel_ids.shape[1:], jnp.int32),
            pltpu.VMEM(ent.shape, F32), pltpu.VMEM(table.shape, BF16), pltpu.VMEM((chunks, wire, LANES), F32), pltpu.VMEM((rows // CHUNK, wire, LANES), F32),
            dma_sems(4), dma_sems(PARTS), dma_sems(PARTS + 1),
        ],
        compiler_params=pltpu.CompilerParams(vmem_limit_bytes=VMEM_LIMIT),
        name='bucket',
    )(edges, counts, negs, rel_ids, ent, rel, table)


def entry(peers):
    barrier = pltpu.get_barrier_semaphore()
    for peer in peers:
        pl.semaphore_signal(barrier, inc=1, device_id=peer, device_id_type=pl.DeviceIdType.MESH)
    pl.semaphore_wait(barrier, len(peers))


def remote(src, dst, send, recv, peer):
    return pltpu.make_async_remote_copy(src_ref=src, dst_ref=dst, send_sem=send, recv_sem=recv, device_id=peer, device_id_type=pl.DeviceIdType.MESH)


def adagrad(rows, state, grad, mean_of, learn_rate):
    square = grad[0] * grad[0] + grad[1] * grad[1] + grad[2] * grad[2] + grad[3] * grad[3]
    state = state + row_sum(square) / mean_of
    root = jnp.sqrt(state + EPSILON)
    return [r - learn_rate * (g / root) for r, g in zip(rows, grad)], state


def exchange_kernel(cfg, tail_ref, head_hbm, rel_grad_ref, ent_hbm, state_ref, rel_ref, rel_state_ref, *refs):
    step, groups, chunks, emb_width, last = cfg
    if last:
        ent_wire, rel_out, loss_out, *refs = refs
    else:
        ent_out, state_out, rel_out, rel_state_out, loss_out, table_hbm, *refs, table, store_sem = refs
    (own, from_core, from_y, from_group, rel_sum, rel_from, send_buf,
     own_sem, core_send, core_recv, y_send, y_recv, group_send, group_recv, rel_send, rel_recv, out_send, out_recv, head_ref, ent_ref, row_sem) = refs
    learn_rate = LR_SCALE * emb_width ** -0.25
    chunk = CHUNK
    y, x, core, top, bot = where_here()
    mine = 2 * x + top
    x_size = groups // 2

    def place(group, low, c):
        return {'data': 2 * (group % 2) + low, 'ent': 2 * (group // 2) + c}

    def at(dy, dx, c):
        return {'data': dy, 'ent': 2 * dx + c}

    def slot_of(low, c, k):
        return (low * 2 + c) * chunks + k

    def turned(shift):
        return (bot + shift) % 2

    other_core = at(y, x, 1 - core)
    other_y = at(2 * top + 1 - bot, x, core)
    rel_peers = (other_core, other_y, at(3 - y, x, core), at(y, x + 1 - 2 * (x % 2), core), at(y, x_size - 1 - x, core), other_core)
    grad_to = place((mine + step) % groups, turned(step), core)
    grad_from = place((mine + groups - step) % groups, turned(step), core)
    nxt = step + 1
    table_to = place((mine + groups - nxt) % groups, turned(nxt), core)
    table_from = place((mine + nxt) % groups, turned(nxt), core)
    peers = list(rel_peers)
    if step:
        peers += [grad_to, grad_from]
    if last:
        for turn in range(4):
            peers.append(at((y + turn) % 4, x, top))
        senders = [at((2 * core + d), x, c) for d in range(2) for c in range(2)]
        peers += senders
    else:
        peers += [table_to, table_from]
    entry(peers)
    keep = turned(step)
    pending = []

    def start(copy):
        copy.start()
        pending.append(copy)
        return copy

    shards = [(1 - keep, k) for k in range(chunks)] + [(keep, k) for k in range(chunks)]
    loads, cores = [], []
    row_loads = [pltpu.make_async_copy(src, dst, row_sem.at[n]) for n, (src, dst) in enumerate(((head_hbm, head_ref), (ent_hbm, ent_ref)))]
    for load in row_loads:
        load.start()
    stores = []

    def store(n, src, dst):
        copy = pltpu.make_async_copy(src, dst, store_sem.at[n])
        copy.start()
        stores.append(copy)

    def store_table(low, c, k):
        slot = slot_of(low, c, k)
        store(slot, table.at[slot], table_hbm.at[slot])

    rel_copies = [start(remote(rel_grad_ref.at[1 - core], rel_from.at[0], rel_send.at[0], rel_recv.at[0], rel_peers[0]))]
    for n, (low, k) in enumerate(shards):
        cores.append(start(remote(tail_ref.at[slot_of(low, 1 - core, k)], from_core.at[n], core_send.at[n], core_recv.at[n], other_core)))
        load = pltpu.make_async_copy(tail_ref.at[slot_of(low, core, k)], own.at[n], own_sem.at[n])
        load.start()
        loads.append(load)

    def rel_step(n):
        rel_copies[n].wait_recv()
        rel_sum[n] = (rel_grad_ref[core] if n == 0 else rel_sum[n - 1]) + rel_from[n]
        rel_copies.append(start(remote(rel_sum.at[n], rel_from.at[n + 1], rel_send.at[n + 1], rel_recv.at[n + 1], rel_peers[n + 1])))

    ys = []
    for k in range(chunks):
        loads[k].wait()
        cores[k].wait_recv()
        own[k] = own[k] + from_core[k]
        ys.append(start(remote(own.at[k], from_y.at[k], y_send.at[k], y_recv.at[k], other_y)))
        if k == 1:
            rel_step(0)
    for k in range(chunks, 2 * chunks):
        loads[k].wait()
        cores[k].wait_recv()
        own[k] = own[k] + from_core[k]
    gs, outs, forwards, crosses = [], [], [], []

    def stage_group(k):
        ys[k].wait_recv()
        own[chunks + k] = own[chunks + k] + from_y[k]
        if step:
            gs.append(start(remote(own.at[chunks + k], from_group.at[k], group_send.at[k], group_recv.at[k], grad_to)))

    def cross_copy(k):
        return remote(send_buf.at[k], ent_wire.at[slot_of(bot, core, k)], out_send.at[2 * chunks + k], out_recv.at[slot_of(bot, core, k)], other_core)

    turn = (y + 4 - 2 * core) % 4
    near = 1 - turn % 2
    back = jnp.where((turn == 1) | (turn == 2), 0, 1)
    onward = at((y + 1 + 2 * back) % 4, x, core)

    def landed(low, c, k):
        slot = slot_of(low, c, k)
        remote(ent_wire.at[slot], ent_wire.at[slot], out_send.at[0], out_recv.at[slot], other_core).wait_recv()

    def stage_relay(k):
        if k % 2 == 0:
            return
        for c in CORES:
            landed(near, c, k - 1)
            landed(near, c, k)
            slot = slot_of(near, c, k) - 1 + back
            start(remote(ent_wire.at[slot], ent_wire.at[slot], out_send.at[(3 + c) * chunks + k], out_recv.at[slot], onward))

    def stage_update(k):
        if k == 0:
            for load in row_loads:
                load.wait()
        if step:
            gs[k].wait_recv()
        total = from_group if step else own
        base = k if step else chunks + k
        grad = [total[base, band(t, chunk), :] + head_ref[k, band(t, chunk), :] for t in TILES[:-1]]
        grad.append(below(unfold_last(total[base, 3 * chunk:, :] + head_ref[k, 3 * chunk:, :])))
        span = band(k, chunk)
        rows, state = adagrad(tiles_at(ent_ref, k * chunk, chunk), state_ref[span, :], grad, emb_width, learn_rate)
        wire = rows[:3] + [fold_last(rows[3])]
        if last:
            lane = lanes((chunk, LANES))
            wire.append(fold_last(jnp.where(lane < 1, state, 0.0)))
        else:
            wide = band(k, 4 * chunk)
            ent_ref[wide, :] = stack_tiles(rows)
            store(4 * chunks + k, ent_ref.at[wide], ent_out.at[wide])
            state_out[span, :] = state
        offset = 0
        for piece in wire:
            send_buf[k, offset:offset + piece.shape[0], :] = piece.astype(send_buf.dtype)
            offset += piece.shape[0]
        slot = slot_of(bot, core, k)
        if last:
            for n, turn in enumerate((1, 3)):
                start(remote(send_buf.at[k], ent_wire.at[slot], out_send.at[n * chunks + k], out_recv.at[slot], at((y + turn) % 4, x, top)))

            @pl.when(core == top)
            def _():
                pltpu.make_async_copy(send_buf.at[k], ent_wire.at[slot], out_recv.at[slot]).start()

            @pl.when(core != top)
            def _():
                cross_copy(k).start()
        else:
            outs.append(start(remote(send_buf.at[k], table.at[slot], out_send.at[k], out_recv.at[k], table_to)))

    def forward(n, low, k, peer):
        slot = slot_of(low, core, k)
        return start(remote(table.at[slot], table.at[slot], out_send.at[n * chunks + k], out_recv.at[n * chunks + k], peer))

    def stage_forward(k):
        outs[k].wait_recv()
        store_table(turned(nxt), core, k)
        forwards.append(forward(1, turned(nxt), k, other_y))
        crosses.append(forward(2, turned(nxt), k, other_core))

    def stage_cross(k):
        forwards[k].wait_recv()
        store_table(1 - turned(nxt), core, k)
        crosses.append(forward(3, 1 - turned(nxt), k, other_core))

    stages = (stage_group, stage_update, stage_relay) if last else (stage_group, stage_update, stage_forward, stage_cross)
    rel_steps = len(rel_peers) - 1
    for tick in range(chunks + LAG * (len(stages) - 1)):
        for n, stage in enumerate(stages):
            if 0 <= tick - LAG * n < chunks:
                stage(tick - LAG * n)
        if tick % 2 == 1 and tick < 2 * rel_steps - 1:
            rel_step(tick // 2 + 1)

    rel_copies[rel_steps].wait_recv()
    halves = rel_sum[rel_steps - 1], rel_from[rel_steps]
    summed = below([jnp.where(core == n, halves[0], halves[1]) for n in CORES])
    rel_grad = [summed[band(t, REL_PAD)] for t in TILES[:-1]] + [below(unfold_last(summed[3 * REL_PAD:]))]
    loss_out[...] = rel_grad[0][REL_PAD - 1:, :]
    row = sublanes((REL_PAD, LANES))
    rel_grad[0] = jnp.where(row < REL_PAD - 1, rel_grad[0], 0.0)
    rel_rows, rel_state = adagrad(tiles_of(rel_ref[...]), rel_state_ref[...], rel_grad, emb_width, learn_rate)
    for t in TILES:
        rel_out[:, band(t, LANES)] = rel_rows[t]
    if not last:
        rel_state_out[...] = rel_state

    if last:
        for c in CORES:
            for k in range(chunks):
                landed(1 - near, c, k)

        @pl.when(core != top)
        def _():
            for k in range(chunks):
                cross_copy(k).wait_send()
    else:
        for n, copy in enumerate(crosses):
            copy.wait_recv()
        for low in CORES:
            for k in range(chunks):
                store_table(low, 1 - core, k)
        for copy in stores:
            copy.wait()
    for copy in pending:
        copy.wait_send()


def exchange_call(step, groups, emb_width, tail, head, rel_grad, ent, state, rel, rel_state):
    vmem, hbm = pl.BlockSpec(memory_space=pltpu.VMEM), pl.BlockSpec(memory_space=pl.ANY)
    chunks = head.shape[0]
    rel_grad = rel_grad.reshape(2, -1, LANES)
    wire = wire_rows(CHUNK)
    last = step == groups - 1
    like = lambda x: jax.ShapeDtypeStruct(x.shape, x.dtype)
    loss = jax.ShapeDtypeStruct((1, LANES), F32)
    out_wire = wire + (CHUNK // LEFT if last else 0)
    out_type = F32 if last else BF16
    gathered = jax.ShapeDtypeStruct((4 * chunks, out_wire, LANES), out_type)
    out_shape = (gathered, like(rel), loss) if last else (like(ent), like(state), like(rel), like(rel_state), loss, gathered)
    return pl.pallas_call(
        functools.partial(exchange_kernel, (step, groups, chunks, emb_width, last)),
        out_shape=out_shape,
        in_specs=[hbm, hbm, vmem, hbm, vmem, vmem, vmem],
        out_specs=(vmem,) * 3 if last else (hbm, vmem, vmem, vmem, vmem, hbm),
        scratch_shapes=[
            pltpu.VMEM((2 * chunks, wire, LANES), F32), pltpu.VMEM((2 * chunks, wire, LANES), F32),
            pltpu.VMEM((chunks, wire, LANES), F32), pltpu.VMEM((chunks, wire, LANES), F32),
            pltpu.VMEM((REL_HOPS - 1, *rel_grad.shape[1:]), F32), pltpu.VMEM((REL_HOPS, *rel_grad.shape[1:]), F32),
            pltpu.VMEM((chunks, out_wire, LANES), out_type),
            *[dma_sems(2 * chunks)] * 3, *[dma_sems(chunks)] * 4,
            dma_sems(REL_HOPS), dma_sems(REL_HOPS), dma_sems(5 * chunks), dma_sems(4 * chunks),
            pltpu.VMEM(head.shape, F32), pltpu.VMEM(ent.shape, F32), dma_sems(2),
            *(() if last else (pltpu.VMEM(gathered.shape, BF16), dma_sems(5 * chunks))),
        ],
        compiler_params=pltpu.CompilerParams(vmem_limit_bytes=VMEM_LIMIT, collective_id=step, has_side_effects=True),
        name='exchange',
    )(tail, head, rel_grad, ent, state, rel, rel_state)


def setup_kernel(cfg, head_ref, tail_ref, rel_id_ref, mask_ref, neg_ref, ent_hbm, rel_ref, word_out, rel_id_out, count_out, neg_out, table, ent_out, rel_out,
                 packed, shares, neg_buf, rows_buf, away, send_sem, recv_sem, core_send, core_recv, load_sem, table_send, table_recv):
    head_bits, tail_bits, spare = cfg
    y, x, core, top, bot = where_here()
    home = core == top
    other_core = {'data': y, 'ent': 2 * x + 1 - core}
    users = [(c, 2 * core + d) for c in CORES for d in CORES]
    users = [({'data': row, 'ent': 2 * x + c}, (core == c) & (y == row)) for c, row in users]
    entry([peer for peer, _ in users] + [{'data': row, 'ent': 2 * x + top} for row in TILES] + [other_core])
    edges = head_ref[...] | (tail_ref[...] << tail_bits) | (rel_id_ref[...] << (2 * tail_bits))
    packed[...] = jnp.where(mask_ref[...] > 0, edges, spare << (2 * tail_bits))
    neg_buf[...] = row_address(neg_ref[...])
    to_users = [remote(packed, shares.at[y], send_sem.at[n], recv_sem.at[y], peer) for n, (peer, _) in enumerate(users)]
    for copy, (_, here) in zip(to_users, users):
        @pl.when(jnp.logical_not(here))
        def _():
            copy.start()

    chunks, chunk = table.shape[0], CHUNK
    shard = chunks // 4

    def load(n):
        return pltpu.make_async_copy(ent_hbm.at[:, pl.ds(pl.multiple_of(n * chunk, chunk), chunk)], rows_buf.at[n % 4], load_sem.at[n % 4])

    def table_copy(q):
        part = table.at[pl.ds(q * shard, shard)]
        return remote(part, part, table_send.at[q], table_recv.at[q], other_core)

    neg_copy = remote(neg_buf, neg_out, core_send.at[0], core_recv.at[0], other_core)
    ent_copy = remote(away, ent_out, core_send.at[1], core_recv.at[1], other_core)

    @pl.when(home)
    def _():
        pltpu.make_async_copy(packed, shares.at[y], recv_sem.at[y]).start()
        neg_copy.start()
        neg_out[...] = neg_buf[...]
        for n in range(3):
            load(n).start()
        for q in TILES:
            def one(k, carry):
                n = q * shard + k

                @pl.when(n + 3 < chunks)
                def _():
                    load(n + 3).start()

                load(n).wait()
                tiles = columns_to_tiles(rows_buf[n % 4])
                for t in TILES[:-1]:
                    table[n, band(t, chunk), :] = tiles[t].astype(BF16)
                table[n, 3 * chunk:, :] = fold_last(tiles[3]).astype(BF16)
                place = pl.ds(pl.multiple_of(k * chunk * 4, chunk * 4), chunk * 4)

                @pl.when(2 * bot + core == q)
                def _():
                    ent_out[place, :] = stack_tiles(tiles)

                @pl.when(2 * bot + 1 - core == q)
                def _():
                    away[place, :] = stack_tiles(tiles)

                return carry

            lax.fori_loop(0, shard, one, 0)
            table_copy(q).start()

            @pl.when(2 * bot + 1 - core == q)
            def _():
                ent_copy.start()

    for t, tile in enumerate(columns_to_tiles(rel_ref[...])):
        rel_out[:, band(t, LANES)] = tile
    for row in TILES:
        remote(packed, shares.at[row], send_sem.at[0], recv_sem.at[row], other_core).wait_recv()
    share = beside([shares[row] for row in TILES])
    mine = ((share >> head_bits) & 3 == 2 * bot + core) & (share >> (2 * tail_bits) != spare)
    lane = lanes(share.shape)
    width = share.shape[1]
    steps = (width - 1).bit_length()
    other = jnp.where(mine, 0, 1)
    before = other
    for bit in range(steps):
        before = before + jnp.where(lane < 2**bit, 0, roll(before, 2**bit))
    count_out[...] = jnp.broadcast_to(width - before[:, width - 1:], count_out.shape)
    none = spare << (head_bits + tail_bits)
    edge = jnp.where(mine, (share & (2**head_bits - 1)) | (share >> tail_bits << head_bits), none)
    shift = jnp.where(mine, before - other, 0)
    for bit in range(steps):
        here = (shift >> bit) & 1 == 1
        edge_in, shift_in = roll(edge, width - 2**bit), roll(shift, width - 2**bit)
        there = (shift_in >> bit) & 1 == 1
        edge = jnp.where(there, edge_in, jnp.where(here, none, edge))
        shift = jnp.where(there, shift_in, jnp.where(here, 0, shift))
    rel_id_out[...] = edge >> (head_bits + tail_bits)
    head, tail = edge & (2**head_bits - 1), (edge >> head_bits) & (2**tail_bits - 1)
    margin = jnp.zeros((share.shape[0], BLOCK), jnp.int32)
    word_out[...] = beside([margin, (row_address(head) << (tail_bits + 2)) | row_address(tail), margin])
    for copy, (_, here) in zip(to_users, users):
        @pl.when(jnp.logical_not(here))
        def _():
            copy.wait_send()

    between = [neg_copy, ent_copy, *(table_copy(q) for q in TILES)]

    @pl.when(home)
    def _():
        for copy in between:
            copy.wait_send()

    @pl.when(jnp.logical_not(home))
    def _():
        for copy in between:
            copy.wait_recv()


def setup_call(cfg, head, tail, rel_ids, mask, neg, reps, ent, rel):
    vmem, hbm = pl.BlockSpec(memory_space=pltpu.VMEM), pl.BlockSpec(memory_space=pl.ANY)
    groups, share = head.shape
    width, rows = ent.shape
    chunks = rows // CHUNK
    return pl.pallas_call(
        functools.partial(setup_kernel, cfg),
        out_shape=(*(jax.ShapeDtypeStruct((groups, n), jnp.int32) for n in (reps * share + 2 * BLOCK, reps * share, LANES, neg.shape[1])),
                   jax.ShapeDtypeStruct((chunks, wire_rows(CHUNK), LANES), BF16), jax.ShapeDtypeStruct((rows, LANES), F32), jax.ShapeDtypeStruct((REL_PAD, 4 * LANES), F32)),
        in_specs=[*[vmem] * 5, hbm, vmem],
        out_specs=(vmem,) * 7,
        scratch_shapes=[pltpu.VMEM(head.shape, jnp.int32), pltpu.VMEM((reps, *head.shape), jnp.int32), pltpu.VMEM(neg.shape, jnp.int32),
                        pltpu.VMEM((4, width, CHUNK), F32), pltpu.VMEM((rows, LANES), F32), *[dma_sems(4)] * 2, *[dma_sems(2)] * 2, *[dma_sems(4)] * 3],
        compiler_params=pltpu.CompilerParams(collective_id=20, has_side_effects=True),
        name='setup',
    )(head, tail, rel_ids, mask, neg, ent, rel)


def finish_kernel(wire_ref, rel_ref, ent_out, rel_out):
    chunk = CHUNK
    for n in range(wire_ref.shape[0]):
        tiles = [wire_ref[n, band(t, chunk), :] for t in TILES[:-1]]
        tiles.append(below(unfold_last(wire_ref[n, 3 * chunk:wire_rows(chunk), :])))
        ent_out[:, band(n, chunk)] = tiles_to_columns(tiles)

    @pl.when(pl.program_id(0) == 0)
    def _():
        rel_out[...] = tiles_to_columns(tiles_of(rel_ref[...]))


def finish_call(wire, rel, width):
    chunks = wire.shape[0]
    size = chunks // 8
    whole = lambda n: (0, 0)
    return pl.pallas_call(
        finish_kernel,
        out_shape=(jax.ShapeDtypeStruct((width, chunks * CHUNK), F32), jax.ShapeDtypeStruct((width, REL_PAD), F32)),
        grid=(chunks // size,),
        in_specs=[pl.BlockSpec((size, *wire.shape[1:]), lambda n: (n, 0, 0)), pl.BlockSpec(rel.shape, whole)],
        out_specs=(pl.BlockSpec((width, size * CHUNK), lambda n: (0, n)), pl.BlockSpec((width, REL_PAD), whole)),
        name='finish',
    )(wire, rel)


def solution(mesh):
    groups = mesh.shape['ent']
    data_reps = mesh.shape['data']
    row_spec = P(('sweep', 'ent'), None)
    edge_spec = P(('sweep', 'ent'), None, 'data')

    def device_fn(ent_table, ent_state, rel_table, head_idx, tail_idx, rel_idx, edge_mask, neg_idx):
        part_rows, emb_width = ent_table.shape
        rel_rows = rel_table.shape[0]
        bucket_edges = head_idx.shape[2] * data_reps
        shard = part_rows // 4
        tail_bits = (part_rows - 1).bit_length()
        head_bits = (shard - 1).bit_length()
        spare = 2**(REL_PAD - 1).bit_length() - 1
        ent = lax.axis_index('ent')
        _, _, core, top, bot = where_here()

        words, rel_ids, counts, neg, table, ent_now, rel_now = setup_call(
            (head_bits, tail_bits, spare), head_idx[0], tail_idx[0], rel_idx[0], edge_mask[0], neg_idx[0], data_reps,
            ent_table.T, jnp.pad(rel_table.T, ((0, 0), (0, REL_PAD - rel_rows))))
        words, neg, counts = words[:, None], neg[:, None], counts[:, 0]
        rel_ids = rel_ids.reshape(groups, -1, BLOCK)

        to_core = lambda c: lax.dynamic_slice_in_dim(ent_state, (2 * bot + c) * shard, shard)
        away = [(d * groups + 2 * (n // 2) + d // 2, d * groups + 2 * (n // 2) + 1 - d // 2) for d in range(data_reps) for n in range(0, groups, 2)]
        state_now = jnp.where(core == top, to_core(core), lax.ppermute(to_core(1 - core), ('data', 'ent'), away))[:, None]
        rel_state = jnp.zeros((REL_PAD, 1), F32)
        losses = []
        for step in range(groups):
            tail, head, rel_grad = bucket_call(step, tail_bits + 2, words, counts, neg, rel_ids, ent_now, rel_now, table)
            out = exchange_call(step, groups, emb_width, tail, head, rel_grad, ent_now, state_now, rel_now, rel_state)
            if step + 1 < groups:
                ent_now, state_now, rel_now, rel_state, loss, table = out
            else:
                wire, rel_now, loss = out
            losses.append(loss)
        ent_out, rel_out = finish_call(wire, rel_now, emb_width)
        state_out = wire[:, wire_rows(CHUNK):, :HALF:LEFT].transpose(0, 2, 1).reshape(part_rows)
        loss_rows = below(losses) / bucket_edges
        bucket_loss = lax.dynamic_slice_in_dim(loss_rows, ent, 1, axis=1).reshape(1, groups)
        return ent_out.T, state_out, rel_out[:, :rel_rows].T, bucket_loss

    return jax.shard_map(device_fn, mesh=mesh, in_specs=(row_spec, P(('sweep', 'ent')), P('sweep', None), edge_spec, edge_spec, edge_spec, edge_spec, P(('sweep', 'ent'), None, None)), out_specs=(row_spec, P(('sweep', 'ent')), P('sweep', None), row_spec), check_vma=False)
```

```python
import functools

import jax
import jax.numpy as jnp
from jax import lax
from jax.experimental import pallas as pl
from jax.experimental.pallas import tpu as pltpu
from jax.sharding import PartitionSpec as P

LR_SCALE = 0.2
EPSILON = 1e-8
LANES = 128
HALF = 64
LEFT = 8
BLOCK = 256
CHUNK = 128
UNROLL = 64
ROLLED = 32
TOGETHER = 4
LAG = 3
PARTS = 4
REL_HOPS = 6
STRIP = 32
REL_PAD = 128
TILES = range(4)
CORES = range(2)
ROW_COL, ROW_ROW, COL_COL = (((1,), (0,)), ((1,), (1,)), ((0,), (0,)))
F32 = jnp.float32
BF16 = jnp.bfloat16
VMEM_LIMIT = 60 * 2**20


def roll(x, by):
    return pltpu.roll(x, by, 1)


def beside(parts):
    return jnp.concatenate(parts, axis=1)


def below(parts):
    return jnp.concatenate(parts, axis=0)


def lanes(shape):
    return lax.broadcasted_iota(jnp.int32, shape, 1)


def sublanes(shape):
    return lax.broadcasted_iota(jnp.int32, shape, 0)


def row_sum(x):
    return jnp.sum(x, axis=1, keepdims=True)


def wire_rows(rows):
    return 3 * rows + rows // LEFT


def columns_to_tiles(x):
    half = x.shape[0] // 2
    a, c, d = slice(0, LANES), slice(LANES, LANES + HALF), slice(LANES + HALF, half)
    re, im = x[:half], x[half:]
    zero = jnp.zeros((HALF - LEFT, x.shape[1]), x.dtype)
    return [t.T for t in (re[a], im[a], below([re[c], im[c]]), below([re[d], zero, im[d], zero]))]


def tiles_to_columns(tiles):
    a, b, c, d = (t.T for t in tiles)
    high = slice(HALF, HALF + LEFT)
    return below([a, c[:HALF], d[:LEFT], b, c[HALF:], d[high]])


def each_row(count, body):
    for u in range(count):
        body(u)


def band(n, size):
    return slice(n * size, (n + 1) * size)


def where_here():
    y, ent = lax.axis_index('data'), lax.axis_index('ent')
    return y, ent // 2, ent % 2, y // 2, y % 2


def fold_last(tile):
    n = tile.shape[0] // LEFT
    out = tile[:n]
    for k in range(1, LEFT):
        out = out + roll(tile[band(k, n)], LEFT * k)
    return out


def unfold_last(packed):
    keep = lanes(packed.shape) % HALF < LEFT
    return [jnp.where(keep, packed if k == 0 else roll(packed, LANES - LEFT * k), 0.0) for k in range(LEFT)]


def tiles_of(x):
    return [x[:, band(t, LANES)] for t in TILES]


def times(x, y):
    out = [x[0] * y[0] - x[1] * y[1], x[0] * y[1] + x[1] * y[0]]
    for a, b in zip(x[2:], y[2:]):
        low = lanes(a.shape) < HALF
        a_swap, b_swap = roll(a, HALF), roll(b, HALF)
        out.append(jnp.where(low, a * b - a_swap * b_swap, a_swap * b + a * b_swap))
    return out


def times_conj(x, y):
    out = [x[0] * y[0] + x[1] * y[1], x[1] * y[0] - x[0] * y[1]]
    for a, b in zip(x[2:], y[2:]):
        low = lanes(a.shape) < HALF
        a_swap, b_swap = roll(a, HALF), roll(b, HALF)
        out.append(jnp.where(low, a * b + a_swap * b_swap, a * b_swap - a_swap * b))
    return out


def tiles_at(ref, row, rows):
    block = ref[pl.ds(row * 4, rows * 4), :].reshape(rows // 8, 32, LANES)
    return [block[:, 8 * t:8 * t + 8].reshape(rows, LANES) for t in TILES]


def stack_tiles(tiles):
    rows = tiles[0].shape[0]
    return beside([t.reshape(rows // 8, 8, LANES) for t in tiles]).reshape(rows * 4, LANES)


def row_at(address):
    return pl.ds(address, 4, stride=8)


def row_address(row):
    return (row >> 3 << 5) | (row & 7)


def in_three(x):
    pieces = []
    for _ in range(3):
        piece = x.astype(BF16)
        pieces.append(piece)
        x = x - piece.astype(F32)
    return pieces


def dot(x, y, dims):
    return lax.dot_general(x, y, (dims, ((), ())), preferred_element_type=F32)


def bucket_kernel(cfg, edges_hbm, count_ref, negs_hbm, rel_ids_hbm, ent_hbm, rel_ref, table_hbm, tail_hbm, head_hbm, rel_out,
                  tail_rows, head_next, tail_next, head_buf, tail_buf, gh_last, gt_last, rel_buf, query_buf, pos_buf, score_buf, d_neg_buf, grad_buf, piece_buf,
                  neg_rows, neg_grad, rel_three, tail_acc0, tail_acc1, head_acc0, head_acc1, rel_acc, loss_acc,
                  edge_ref, neg_ref, rel_id_ref, ent_ref, table_ref, tail_out, head_out, sems, table_sems, tail_sems):
    step, tail_bits = cfg
    chunk = CHUNK
    part = chunk // LEFT
    tail_acc, head_acc = (tail_acc0, tail_acc1), (head_acc0, head_acc1)
    count = count_ref[step, 0]
    negs = neg_ref.shape[0]
    loads = [
        pltpu.make_async_copy(negs_hbm.at[step, 0], neg_ref, sems.at[0]),
        pltpu.make_async_copy(rel_ids_hbm.at[step], rel_id_ref, sems.at[2]),
        pltpu.make_async_copy(ent_hbm, ent_ref, sems.at[3]),
    ]
    parts = table_sems.shape[0]
    size = table_ref.shape[0] // parts
    tables = [pltpu.make_async_copy(table_hbm.at[band(n, size)], table_ref.at[band(n, size)], table_sems.at[n]) for n in range(parts)]
    blocks = pl.cdiv(count, BLOCK)

    def edge_pieces(act):
        def one(n, carry):
            span = pl.ds(pl.multiple_of(n * 2 * BLOCK, 2 * BLOCK), 2 * BLOCK)
            act(pltpu.make_async_copy(edges_hbm.at[step, 0, span], edge_ref.at[span], sems.at[1]))
            return carry

        lax.fori_loop(0, (blocks + 3) // 2, one, 0)

    edge_pieces(lambda copy: copy.start())
    for load in loads + tables:
        load.start()

    def head_of(e):
        return row_at(e >> tail_bits)

    def tail_of(e):
        return row_at(e & (2**tail_bits - 1))

    def clear(accs, n, carry):
        for acc in accs:
            acc[pl.ds(pl.multiple_of(n * chunk * 4, chunk * 4), chunk * 4), :] = jnp.zeros((chunk * 4, LANES), F32)
        return carry

    lax.fori_loop(0, table_ref.shape[0], functools.partial(clear, tail_acc), 0)
    lax.fori_loop(0, head_out.shape[0], functools.partial(clear, head_acc), 0)
    neg_grad[...] = jnp.zeros_like(neg_grad)
    gh_last[...] = jnp.zeros_like(gh_last)
    gt_last[...] = jnp.zeros_like(gt_last)
    rel_acc[...] = jnp.zeros_like(rel_acc)
    loss_acc[...] = jnp.zeros_like(loss_acc)
    for n, piece in enumerate(in_three(rel_ref[...])):
        rel_three[band(n, REL_PAD), :] = piece
    for load in loads:
        load.wait()
    edge_pieces(lambda copy: copy.wait())

    def widen(i, carry):
        for n in (i * TOGETHER + k for k in range(TOGETHER)):
            tiles = [table_ref[n, band(t, chunk), :].astype(F32) for t in TILES[:-1]]
            tiles.append(below(unfold_last(table_ref[n, 3 * chunk:, :].astype(F32))))
            tail_rows[pl.ds(pl.multiple_of(n * chunk * 4, chunk * 4), chunk * 4), :] = stack_tiles(tiles)
        return carry

    for n, load in enumerate(tables):
        load.wait()
        lax.fori_loop(n * size // TOGETHER, (n + 1) * size // TOGETHER, widen, 0)

    def take_negs(n, carry):
        base = pl.multiple_of(n * UNROLL, UNROLL)

        def take(u):
            head_buf[row_at(row_address(u)), :] = tail_rows[row_at(neg_ref[base + u]), :]

        each_row(UNROLL, take)
        for t, tile in enumerate(tiles_at(head_buf, 0, UNROLL)):
            neg_rows[pl.ds(base, UNROLL), band(t, LANES)] = tile.astype(BF16)
        return carry

    lax.fori_loop(0, negs // UNROLL, take_negs, 0)

    def take_edges(base, row=0):
        def take(u):
            e = edge_ref[base + u]
            place = row_at(row * 4 + row_address(u))
            head_next[place, :] = ent_ref[head_of(e), :]
            tail_next[place, :] = tail_rows[tail_of(e), :]

        return take

    def put_edges(base, row=0):
        def put(pair):
            for lane in range(2):
                u = 2 * pair + lane
                e = edge_ref[base + u]
                place = row_at(row * 4 + row_address(u))
                head_acc[lane][head_of(e), :] += gh_last[place, :]
                tail_acc[lane][tail_of(e), :] += gt_last[place, :]

        return put


    def take_first(n, carry):
        row = pl.multiple_of(n * ROLLED, ROLLED)
        each_row(ROLLED, take_edges(BLOCK + row, row))
        return carry

    lax.fori_loop(0, BLOCK // ROLLED, take_first, 0)
    spans = [slice(r, r + STRIP) for r in range(0, BLOCK, STRIP)]

    def block(n, carry):
        base = pl.multiple_of(n * BLOCK, BLOCK)
        hot = sublanes((REL_PAD, BLOCK)) == rel_id_ref[:, pl.ds(base, BLOCK)]
        hot = jnp.where(hot, 1.0, 0.0).astype(BF16)
        rel_buf[...] = dot(below([hot] * 3), rel_three[...], COL_COL)
        for span in spans:
            head, tail, rel = tiles_at(head_next, span.start, STRIP), tiles_at(tail_next, span.start, STRIP), tiles_of(rel_buf[span, :])
            wide = slice(4 * span.start, 4 * span.stop)
            head_buf[wide, :], tail_buf[wide, :] = stack_tiles(head), stack_tiles(tail)
            total = None
            for t, q in enumerate(times(head, rel)):
                q = q.astype(BF16)
                query_buf[span, band(t, LANES)] = q
                product = q.astype(F32) * tail[t]
                total = product if total is None else total + product
            pos_buf[span, :] = row_sum(total)
        each_row(BLOCK, take_edges(base + 2 * BLOCK))
        each_row(BLOCK // 2, put_edges(base))
        score_buf[...] = dot(query_buf[...], neg_rows[...], ROW_ROW)
        for span in spans:
            weight = jnp.where(sublanes((STRIP, 1)) + (base + span.start) < count, 1.0, 0.0)
            score, pos = score_buf[span, :], pos_buf[span, :]
            top = jnp.maximum(jnp.max(score, axis=1, keepdims=True), pos)
            pos_exp = jnp.exp(pos - top)
            neg_exp = jnp.exp(score - top)
            total = pos_exp + row_sum(neg_exp)
            loss_acc[...] += jnp.sum(weight * (top + jnp.log(total) - pos), axis=0, keepdims=True)
            pos_buf[span, :] = weight * (pos_exp / total - 1.0)
            d_neg_buf[span, :] = ((weight / total) * neg_exp).astype(BF16)
        grad_buf[...] = dot(d_neg_buf[...], neg_rows[...], ROW_COL)
        neg_grad[...] += dot(d_neg_buf[...], query_buf[...], COL_COL)
        for span in spans:
            wide = slice(4 * span.start, 4 * span.stop)
            d_pos = pos_buf[span, :]
            tail, rel = tiles_at(tail_buf, span.start, STRIP), tiles_of(rel_buf[span, :])
            grad_q = [d_pos * x + y for x, y in zip(tail, tiles_of(grad_buf[span, :]))]
            gt_last[wide, :] = stack_tiles([d_pos * q.astype(F32) for q in tiles_of(query_buf[span, :])])
            gh_last[wide, :] = stack_tiles(times_conj(grad_q, rel))
            for t, grad in enumerate(times_conj(grad_q, tiles_at(head_buf, span.start, STRIP))):
                for k, piece in enumerate(in_three(grad)):
                    piece_buf[k * BLOCK + span.start:k * BLOCK + span.stop, band(t, LANES)] = piece
        rel_acc[...] += dot(beside([hot] * 3), piece_buf[...], ROW_COL)
        return carry

    lax.fori_loop(0, blocks, block, 0)

    def put_last(n, carry):
        row = pl.multiple_of(n * ROLLED, ROLLED)
        each_row(ROLLED // 2, put_edges(blocks * BLOCK + row, row))
        return carry

    lax.fori_loop(0, BLOCK // ROLLED, put_last, 0)

    def put_negs(n, carry):
        base = pl.multiple_of(n * UNROLL, UNROLL)
        gt_last[:4 * UNROLL, :] = stack_tiles(tiles_of(neg_grad[pl.ds(base, UNROLL), :]))

        def put(pair):
            for lane in range(2):
                u = 2 * pair + lane
                tail_acc[lane][row_at(neg_ref[base + u]), :] += gt_last[row_at(row_address(u)), :]

        each_row(UNROLL // 2, put)
        return carry

    lax.fori_loop(0, negs // UNROLL, put_negs, 0)

    def emit(out_ref, acc, i, carry):
        for n in (i * TOGETHER + k for k in range(TOGETHER)):
            base = pl.multiple_of(n * chunk, chunk)
            tiles = [a + b for a, b in zip(tiles_at(acc[0], base, chunk), tiles_at(acc[1], base, chunk))]
            for t in TILES[:-1]:
                out_ref[n, band(t, chunk), :] = tiles[t]
            out_ref[n, 3 * chunk:, :] = fold_last(tiles[3])
        return carry

    stores = []
    for n in range(tail_sems.shape[0]):
        out, dst, acc, span = (head_out, head_hbm, head_acc, range(head_out.shape[0])) if n == parts else (tail_out, tail_hbm, tail_acc, range(n * size, (n + 1) * size))
        lax.fori_loop(span.start // TOGETHER, span.stop // TOGETHER, functools.partial(emit, out, acc), 0)
        part_of = pl.ds(span.start, len(span))
        stores.append(pltpu.make_async_copy(out.at[part_of], dst.at[part_of], tail_sems.at[n]))
        stores[-1].start()
    _, x, _, top, _ = where_here()
    group = 2 * x + top
    row = sublanes((REL_PAD, LANES))
    lane = lanes((REL_PAD, LANES))
    loss = jnp.where(lane == group, loss_acc[...], 0.0)
    for t in TILES[:-1]:
        rows = rel_acc[:, band(t, LANES)]
        rel_out[band(t, REL_PAD), :] = jnp.where(row == REL_PAD - 1, loss, rows) if t == 0 else rows
    rel_out[3 * REL_PAD:, :] = fold_last(rel_acc[:, 3 * LANES:])
    for store in stores:
        store.wait()


def dma_sems(n):
    return pltpu.SemaphoreType.DMA((n,))


def bucket_call(step, tail_bits, edges, counts, negs, rel_ids, ent, rel, table):
    smem, vmem, hbm = (pl.BlockSpec(memory_space=m) for m in (pltpu.SMEM, pltpu.VMEM, pl.ANY))
    rows, neg_count, chunks = ent.shape[0] // 4, negs.shape[-1], table.shape[0]
    width = 4 * LANES
    wire = wire_rows(CHUNK)
    block = pltpu.VMEM((BLOCK * 4, LANES), F32)
    table_rows = pltpu.VMEM((chunks * CHUNK * 4, LANES), F32)
    head_rows = pltpu.VMEM((rows * 4, LANES), F32)
    return pl.pallas_call(
        functools.partial(bucket_kernel, (step, tail_bits)),
        out_shape=(
            jax.ShapeDtypeStruct((chunks, wire, LANES), F32),
            jax.ShapeDtypeStruct((rows // CHUNK, wire, LANES), F32),
            jax.ShapeDtypeStruct((wire_rows(REL_PAD), LANES), F32),
        ),
        in_specs=[hbm, smem, hbm, hbm, hbm, vmem, hbm],
        out_specs=(hbm, hbm, vmem),
        scratch_shapes=[
            table_rows, *[block] * 6, pltpu.VMEM((BLOCK, width), F32), pltpu.VMEM((BLOCK, width), BF16), pltpu.VMEM((BLOCK, 1), F32),
            pltpu.VMEM((BLOCK, neg_count), F32), pltpu.VMEM((BLOCK, neg_count), BF16), pltpu.VMEM((BLOCK, width), F32), pltpu.VMEM((3 * BLOCK, width), BF16),
            pltpu.VMEM((neg_count, width), BF16), pltpu.VMEM((neg_count, width), F32), pltpu.VMEM((3 * REL_PAD, width), BF16),
            table_rows, table_rows, head_rows, head_rows,
            pltpu.VMEM((REL_PAD, width), F32), pltpu.VMEM((1, 1), F32),
            pltpu.SMEM((edges.shape[-1],), jnp.int32), pltpu.SMEM((neg_count,), jnp.int32), pltpu.VMEM(rel_ids.shape[1:], jnp.int32),
            pltpu.VMEM(ent.shape, F32), pltpu.VMEM(table.shape, BF16), pltpu.VMEM((chunks, wire, LANES), F32), pltpu.VMEM((rows // CHUNK, wire, LANES), F32),
            dma_sems(4), dma_sems(PARTS), dma_sems(PARTS + 1),
        ],
        compiler_params=pltpu.CompilerParams(vmem_limit_bytes=VMEM_LIMIT),
        name='bucket',
    )(edges, counts, negs, rel_ids, ent, rel, table)


def entry(peers):
    barrier = pltpu.get_barrier_semaphore()
    for peer in peers:
        pl.semaphore_signal(barrier, inc=1, device_id=peer, device_id_type=pl.DeviceIdType.MESH)
    pl.semaphore_wait(barrier, len(peers))


def remote(src, dst, send, recv, peer):
    return pltpu.make_async_remote_copy(src_ref=src, dst_ref=dst, send_sem=send, recv_sem=recv, device_id=peer, device_id_type=pl.DeviceIdType.MESH)


def adagrad(rows, state, grad, mean_of, learn_rate):
    square = grad[0] * grad[0] + grad[1] * grad[1] + grad[2] * grad[2] + grad[3] * grad[3]
    state = state + row_sum(square) / mean_of
    root = jnp.sqrt(state + EPSILON)
    return [r - learn_rate * (g / root) for r, g in zip(rows, grad)], state


def exchange_kernel(cfg, tail_ref, head_hbm, rel_grad_ref, ent_hbm, state_ref, rel_ref, rel_state_ref, *refs):
    step, groups, chunks, emb_width, last = cfg
    if last:
        ent_wire, rel_out, loss_out, *refs = refs
    else:
        ent_out, state_out, rel_out, rel_state_out, loss_out, table_hbm, *refs, table, store_sem = refs
    (own, from_core, from_y, from_group, rel_sum, rel_from, send_buf,
     own_sem, core_send, core_recv, y_send, y_recv, group_send, group_recv, rel_send, rel_recv, out_send, out_recv, head_ref, ent_ref, row_sem) = refs
    learn_rate = LR_SCALE * emb_width ** -0.25
    chunk = CHUNK
    y, x, core, top, bot = where_here()
    mine = 2 * x + top
    x_size = groups // 2

    def place(group, low, c):
        return {'data': 2 * (group % 2) + low, 'ent': 2 * (group // 2) + c}

    def at(dy, dx, c):
        return {'data': dy, 'ent': 2 * dx + c}

    def slot_of(low, c, k):
        return (low * 2 + c) * chunks + k

    def turned(shift):
        return (bot + shift) % 2

    other_core = at(y, x, 1 - core)
    other_y = at(2 * top + 1 - bot, x, core)
    rel_peers = (other_core, other_y, at(3 - y, x, core), at(y, x + 1 - 2 * (x % 2), core), at(y, x_size - 1 - x, core), other_core)
    grad_to = place((mine + step) % groups, turned(step), core)
    grad_from = place((mine + groups - step) % groups, turned(step), core)
    nxt = step + 1
    table_to = place((mine + groups - nxt) % groups, turned(nxt), core)
    table_from = place((mine + nxt) % groups, turned(nxt), core)
    peers = list(rel_peers)
    if step:
        peers += [grad_to, grad_from]
    if last:
        for turn in range(4):
            peers.append(at((y + turn) % 4, x, top))
        senders = [at((2 * core + d), x, c) for d in range(2) for c in range(2)]
        peers += senders
    else:
        peers += [table_to, table_from]
    entry(peers)
    keep = turned(step)
    pending = []

    def start(copy):
        copy.start()
        pending.append(copy)
        return copy

    shards = [(1 - keep, k) for k in range(chunks)] + [(keep, k) for k in range(chunks)]
    loads, cores = [], []
    row_loads = [pltpu.make_async_copy(src, dst, row_sem.at[n]) for n, (src, dst) in enumerate(((head_hbm, head_ref), (ent_hbm, ent_ref)))]
    for load in row_loads:
        load.start()
    stores = []

    def store(n, src, dst):
        copy = pltpu.make_async_copy(src, dst, store_sem.at[n])
        copy.start()
        stores.append(copy)

    def store_table(low, c, k):
        slot = slot_of(low, c, k)
        store(slot, table.at[slot], table_hbm.at[slot])

    rel_copies = [start(remote(rel_grad_ref.at[1 - core], rel_from.at[0], rel_send.at[0], rel_recv.at[0], rel_peers[0]))]
    for n, (low, k) in enumerate(shards):
        cores.append(start(remote(tail_ref.at[slot_of(low, 1 - core, k)], from_core.at[n], core_send.at[n], core_recv.at[n], other_core)))
        load = pltpu.make_async_copy(tail_ref.at[slot_of(low, core, k)], own.at[n], own_sem.at[n])
        load.start()
        loads.append(load)

    def rel_step(n):
        rel_copies[n].wait_recv()
        rel_sum[n] = (rel_grad_ref[core] if n == 0 else rel_sum[n - 1]) + rel_from[n]
        rel_copies.append(start(remote(rel_sum.at[n], rel_from.at[n + 1], rel_send.at[n + 1], rel_recv.at[n + 1], rel_peers[n + 1])))

    ys = []
    for k in range(chunks):
        loads[k].wait()
        cores[k].wait_recv()
        own[k] = own[k] + from_core[k]
        ys.append(start(remote(own.at[k], from_y.at[k], y_send.at[k], y_recv.at[k], other_y)))
        if k == 1:
            rel_step(0)
    for k in range(chunks, 2 * chunks):
        loads[k].wait()
        cores[k].wait_recv()
        own[k] = own[k] + from_core[k]
    gs, outs, forwards, crosses = [], [], [], []

    def stage_group(k):
        ys[k].wait_recv()
        own[chunks + k] = own[chunks + k] + from_y[k]
        if step:
            gs.append(start(remote(own.at[chunks + k], from_group.at[k], group_send.at[k], group_recv.at[k], grad_to)))

    def cross_copy(k):
        return remote(send_buf.at[k], ent_wire.at[slot_of(bot, core, k)], out_send.at[2 * chunks + k], out_recv.at[slot_of(bot, core, k)], other_core)

    turn = (y + 4 - 2 * core) % 4
    near = 1 - turn % 2
    back = jnp.where((turn == 1) | (turn == 2), 0, 1)
    onward = at((y + 1 + 2 * back) % 4, x, core)

    def landed(low, c, k):
        slot = slot_of(low, c, k)
        remote(ent_wire.at[slot], ent_wire.at[slot], out_send.at[0], out_recv.at[slot], other_core).wait_recv()

    def stage_relay(k):
        if k % 2 == 0:
            return
        for c in CORES:
            landed(near, c, k - 1)
            landed(near, c, k)
            slot = slot_of(near, c, k) - 1 + back
            start(remote(ent_wire.at[slot], ent_wire.at[slot], out_send.at[(3 + c) * chunks + k], out_recv.at[slot], onward))

    def stage_update(k):
        if k == 0:
            for load in row_loads:
                load.wait()
        if step:
            gs[k].wait_recv()
        total = from_group if step else own
        base = k if step else chunks + k
        grad = [total[base, band(t, chunk), :] + head_ref[k, band(t, chunk), :] for t in TILES[:-1]]
        grad.append(below(unfold_last(total[base, 3 * chunk:, :] + head_ref[k, 3 * chunk:, :])))
        span = band(k, chunk)
        rows, state = adagrad(tiles_at(ent_ref, k * chunk, chunk), state_ref[span, :], grad, emb_width, learn_rate)
        wire = rows[:3] + [fold_last(rows[3])]
        if last:
            lane = lanes((chunk, LANES))
            wire.append(fold_last(jnp.where(lane < 1, state, 0.0)))
        else:
            wide = band(k, 4 * chunk)
            ent_ref[wide, :] = stack_tiles(rows)
            store(4 * chunks + k, ent_ref.at[wide], ent_out.at[wide])
            state_out[span, :] = state
        offset = 0
        for piece in wire:
            send_buf[k, offset:offset + piece.shape[0], :] = piece.astype(send_buf.dtype)
            offset += piece.shape[0]
        slot = slot_of(bot, core, k)
        if last:
            for n, turn in enumerate((1, 3)):
                start(remote(send_buf.at[k], ent_wire.at[slot], out_send.at[n * chunks + k], out_recv.at[slot], at((y + turn) % 4, x, top)))

            @pl.when(core == top)
            def _():
                pltpu.make_async_copy(send_buf.at[k], ent_wire.at[slot], out_recv.at[slot]).start()

            @pl.when(core != top)
            def _():
                cross_copy(k).start()
        else:
            outs.append(start(remote(send_buf.at[k], table.at[slot], out_send.at[k], out_recv.at[k], table_to)))

    def forward(n, low, k, peer):
        slot = slot_of(low, core, k)
        return start(remote(table.at[slot], table.at[slot], out_send.at[n * chunks + k], out_recv.at[n * chunks + k], peer))

    def stage_forward(k):
        outs[k].wait_recv()
        store_table(turned(nxt), core, k)
        forwards.append(forward(1, turned(nxt), k, other_y))
        crosses.append(forward(2, turned(nxt), k, other_core))

    def stage_cross(k):
        forwards[k].wait_recv()
        store_table(1 - turned(nxt), core, k)
        crosses.append(forward(3, 1 - turned(nxt), k, other_core))

    stages = (stage_group, stage_update, stage_relay) if last else (stage_group, stage_update, stage_forward, stage_cross)
    rel_steps = len(rel_peers) - 1
    for tick in range(chunks + LAG * (len(stages) - 1)):
        for n, stage in enumerate(stages):
            if 0 <= tick - LAG * n < chunks:
                stage(tick - LAG * n)
        if tick % 2 == 1 and tick < 2 * rel_steps - 1:
            rel_step(tick // 2 + 1)

    rel_copies[rel_steps].wait_recv()
    halves = rel_sum[rel_steps - 1], rel_from[rel_steps]
    summed = below([jnp.where(core == n, halves[0], halves[1]) for n in CORES])
    rel_grad = [summed[band(t, REL_PAD)] for t in TILES[:-1]] + [below(unfold_last(summed[3 * REL_PAD:]))]
    loss_out[...] = rel_grad[0][REL_PAD - 1:, :]
    row = sublanes((REL_PAD, LANES))
    rel_grad[0] = jnp.where(row < REL_PAD - 1, rel_grad[0], 0.0)
    rel_rows, rel_state = adagrad(tiles_of(rel_ref[...]), rel_state_ref[...], rel_grad, emb_width, learn_rate)
    for t in TILES:
        rel_out[:, band(t, LANES)] = rel_rows[t]
    if not last:
        rel_state_out[...] = rel_state

    if last:
        for c in CORES:
            for k in range(chunks):
                landed(1 - near, c, k)

        @pl.when(core != top)
        def _():
            for k in range(chunks):
                cross_copy(k).wait_send()
    else:
        for n, copy in enumerate(crosses):
            copy.wait_recv()
        for low in CORES:
            for k in range(chunks):
                store_table(low, 1 - core, k)
        for copy in stores:
            copy.wait()
    for copy in pending:
        copy.wait_send()


def exchange_call(step, groups, emb_width, tail, head, rel_grad, ent, state, rel, rel_state):
    vmem, hbm = pl.BlockSpec(memory_space=pltpu.VMEM), pl.BlockSpec(memory_space=pl.ANY)
    chunks = head.shape[0]
    rel_grad = rel_grad.reshape(2, -1, LANES)
    wire = wire_rows(CHUNK)
    last = step == groups - 1
    like = lambda x: jax.ShapeDtypeStruct(x.shape, x.dtype)
    loss = jax.ShapeDtypeStruct((1, LANES), F32)
    out_wire = wire + (CHUNK // LEFT if last else 0)
    out_type = F32 if last else BF16
    gathered = jax.ShapeDtypeStruct((4 * chunks, out_wire, LANES), out_type)
    out_shape = (gathered, like(rel), loss) if last else (like(ent), like(state), like(rel), like(rel_state), loss, gathered)
    return pl.pallas_call(
        functools.partial(exchange_kernel, (step, groups, chunks, emb_width, last)),
        out_shape=out_shape,
        in_specs=[hbm, hbm, vmem, hbm, vmem, vmem, vmem],
        out_specs=(vmem,) * 3 if last else (hbm, vmem, vmem, vmem, vmem, hbm),
        scratch_shapes=[
            pltpu.VMEM((2 * chunks, wire, LANES), F32), pltpu.VMEM((2 * chunks, wire, LANES), F32),
            pltpu.VMEM((chunks, wire, LANES), F32), pltpu.VMEM((chunks, wire, LANES), F32),
            pltpu.VMEM((REL_HOPS - 1, *rel_grad.shape[1:]), F32), pltpu.VMEM((REL_HOPS, *rel_grad.shape[1:]), F32),
            pltpu.VMEM((chunks, out_wire, LANES), out_type),
            *[dma_sems(2 * chunks)] * 3, *[dma_sems(chunks)] * 4,
            dma_sems(REL_HOPS), dma_sems(REL_HOPS), dma_sems(5 * chunks), dma_sems(4 * chunks),
            pltpu.VMEM(head.shape, F32), pltpu.VMEM(ent.shape, F32), dma_sems(2),
            *(() if last else (pltpu.VMEM(gathered.shape, BF16), dma_sems(5 * chunks))),
        ],
        compiler_params=pltpu.CompilerParams(vmem_limit_bytes=VMEM_LIMIT, collective_id=step, has_side_effects=True),
        name='exchange',
    )(tail, head, rel_grad, ent, state, rel, rel_state)


def setup_kernel(cfg, head_ref, tail_ref, rel_id_ref, mask_ref, neg_ref, ent_hbm, rel_ref, word_out, rel_id_out, count_out, neg_out, table, ent_out, rel_out,
                 packed, shares, neg_buf, rows_buf, away, send_sem, recv_sem, core_send, core_recv, load_sem, table_send, table_recv):
    head_bits, tail_bits, spare = cfg
    y, x, core, top, bot = where_here()
    home = core == top
    other_core = {'data': y, 'ent': 2 * x + 1 - core}
    users = [(c, 2 * core + d) for c in CORES for d in CORES]
    users = [({'data': row, 'ent': 2 * x + c}, (core == c) & (y == row)) for c, row in users]
    entry([peer for peer, _ in users] + [{'data': row, 'ent': 2 * x + top} for row in TILES] + [other_core])
    edges = head_ref[...] | (tail_ref[...] << tail_bits) | (rel_id_ref[...] << (2 * tail_bits))
    packed[...] = jnp.where(mask_ref[...] > 0, edges, spare << (2 * tail_bits))
    neg_buf[:, 0, :] = row_address(neg_ref[...])
    to_users = [remote(packed, shares.at[y], send_sem.at[n], recv_sem.at[y], peer) for n, (peer, _) in enumerate(users)]
    for copy, (_, here) in zip(to_users, users):
        @pl.when(jnp.logical_not(here))
        def _():
            copy.start()

    chunks, chunk = table.shape[0], CHUNK
    shard = chunks // 4

    def load(n):
        return pltpu.make_async_copy(ent_hbm.at[:, pl.ds(pl.multiple_of(n * chunk, chunk), chunk)], rows_buf.at[n % 4], load_sem.at[n % 4])

    def table_copy(q):
        part = table.at[pl.ds(q * shard, shard)]
        return remote(part, part, table_send.at[q], table_recv.at[q], other_core)

    neg_copy = remote(neg_buf, neg_out, core_send.at[0], core_recv.at[0], other_core)
    ent_copy = remote(away, ent_out, core_send.at[1], core_recv.at[1], other_core)

    @pl.when(home)
    def _():
        pltpu.make_async_copy(packed, shares.at[y], recv_sem.at[y]).start()
        neg_copy.start()
        neg_out[...] = neg_buf[...]
        for n in range(3):
            load(n).start()
        for q in TILES:
            def one(k, carry):
                n = q * shard + k

                @pl.when(n + 3 < chunks)
                def _():
                    load(n + 3).start()

                load(n).wait()
                tiles = columns_to_tiles(rows_buf[n % 4])
                for t in TILES[:-1]:
                    table[n, band(t, chunk), :] = tiles[t].astype(BF16)
                table[n, 3 * chunk:, :] = fold_last(tiles[3]).astype(BF16)
                place = pl.ds(pl.multiple_of(k * chunk * 4, chunk * 4), chunk * 4)

                @pl.when(2 * bot + core == q)
                def _():
                    ent_out[place, :] = stack_tiles(tiles)

                @pl.when(2 * bot + 1 - core == q)
                def _():
                    away[place, :] = stack_tiles(tiles)

                return carry

            lax.fori_loop(0, shard, one, 0)
            table_copy(q).start()

            @pl.when(2 * bot + 1 - core == q)
            def _():
                ent_copy.start()

    for t, tile in enumerate(columns_to_tiles(rel_ref[...])):
        rel_out[:, band(t, LANES)] = tile
    for row in TILES:
        remote(packed, shares.at[row], send_sem.at[0], recv_sem.at[row], other_core).wait_recv()
    share = beside([shares[row] for row in TILES])
    mine = ((share >> head_bits) & 3 == 2 * bot + core) & (share >> (2 * tail_bits) != spare)
    lane = lanes(share.shape)
    width = share.shape[1]
    steps = (width - 1).bit_length()
    other = jnp.where(mine, 0, 1)
    before = other
    for bit in range(steps):
        before = before + jnp.where(lane < 2**bit, 0, roll(before, 2**bit))
    count_out[...] = jnp.broadcast_to(width - before[:, width - 1:], count_out.shape)
    none = spare << (head_bits + tail_bits)
    edge = jnp.where(mine, (share & (2**head_bits - 1)) | (share >> tail_bits << head_bits), none)
    shift = jnp.where(mine, before - other, 0)
    for bit in range(steps):
        here = (shift >> bit) & 1 == 1
        edge_in, shift_in = roll(edge, width - 2**bit), roll(shift, width - 2**bit)
        there = (shift_in >> bit) & 1 == 1
        edge = jnp.where(there, edge_in, jnp.where(here, none, edge))
        shift = jnp.where(there, shift_in, jnp.where(here, 0, shift))
    rel_id_out[:, 0, :] = edge >> (head_bits + tail_bits)
    head, tail = edge & (2**head_bits - 1), (edge >> head_bits) & (2**tail_bits - 1)
    margin = jnp.zeros((share.shape[0], BLOCK), jnp.int32)
    word_out[:, 0, :] = beside([margin, (row_address(head) << (tail_bits + 2)) | row_address(tail), margin])
    for copy, (_, here) in zip(to_users, users):
        @pl.when(jnp.logical_not(here))
        def _():
            copy.wait_send()

    between = [neg_copy, ent_copy, *(table_copy(q) for q in TILES)]

    @pl.when(home)
    def _():
        for copy in between:
            copy.wait_send()

    @pl.when(jnp.logical_not(home))
    def _():
        for copy in between:
            copy.wait_recv()


def setup_call(cfg, head, tail, rel_ids, mask, neg, reps, ent, rel):
    vmem, hbm = pl.BlockSpec(memory_space=pltpu.VMEM), pl.BlockSpec(memory_space=pl.ANY)
    groups, share = head.shape
    width, rows = ent.shape
    chunks = rows // CHUNK
    return pl.pallas_call(
        functools.partial(setup_kernel, cfg),
        out_shape=(*(jax.ShapeDtypeStruct(shape, jnp.int32) for shape in ((groups, 1, reps * share + 2 * BLOCK), (groups, 1, reps * share), (groups, LANES), (groups, 1, neg.shape[1]))),
                   jax.ShapeDtypeStruct((chunks, wire_rows(CHUNK), LANES), BF16), jax.ShapeDtypeStruct((rows, LANES), F32), jax.ShapeDtypeStruct((REL_PAD, 4 * LANES), F32)),
        in_specs=[*[vmem] * 5, hbm, vmem],
        out_specs=(vmem,) * 7,
        scratch_shapes=[pltpu.VMEM(head.shape, jnp.int32), pltpu.VMEM((reps, *head.shape), jnp.int32), pltpu.VMEM((groups, 1, neg.shape[1]), jnp.int32),
                        pltpu.VMEM((4, width, CHUNK), F32), pltpu.VMEM((rows, LANES), F32), *[dma_sems(4)] * 2, *[dma_sems(2)] * 2, *[dma_sems(4)] * 3],
        compiler_params=pltpu.CompilerParams(collective_id=20, has_side_effects=True),
        name='setup',
    )(head, tail, rel_ids, mask, neg, ent, rel)


def finish_kernel(wire_ref, rel_ref, ent_out, state_out, rel_out):
    chunk = CHUNK
    for n in range(wire_ref.shape[0]):
        tiles = [wire_ref[n, band(t, chunk), :] for t in TILES[:-1]]
        tiles.append(below(unfold_last(wire_ref[n, 3 * chunk:wire_rows(chunk), :])))
        ent_out[:, band(n, chunk)] = tiles_to_columns(tiles)
        state = below([part[:, :1] for part in unfold_last(wire_ref[n, wire_rows(chunk):, :])])
        state_out[:, band(n, chunk)] = jnp.broadcast_to(state, (chunk, LANES)).T[:1]

    @pl.when(pl.program_id(0) == 0)
    def _():
        rel_out[...] = tiles_to_columns(tiles_of(rel_ref[...]))


def finish_call(wire, rel, width):
    chunks = wire.shape[0]
    size = chunks // 8
    whole = lambda n: (0, 0)
    return pl.pallas_call(
        finish_kernel,
        out_shape=tuple(jax.ShapeDtypeStruct(shape, F32) for shape in ((width, chunks * CHUNK), (1, chunks * CHUNK), (width, REL_PAD))),
        grid=(chunks // size,),
        in_specs=[pl.BlockSpec((size, *wire.shape[1:]), lambda n: (n, 0, 0)), pl.BlockSpec(rel.shape, whole)],
        out_specs=(pl.BlockSpec((width, size * CHUNK), lambda n: (0, n)), pl.BlockSpec((1, size * CHUNK), lambda n: (0, n)), pl.BlockSpec((width, REL_PAD), whole)),
        name='finish',
    )(wire, rel)


def solution(mesh):
    groups = mesh.shape['ent']
    data_reps = mesh.shape['data']
    row_spec = P(('sweep', 'ent'), None)
    edge_spec = P(('sweep', 'ent'), None, 'data')

    def device_fn(ent_table, ent_state, rel_table, head_idx, tail_idx, rel_idx, edge_mask, neg_idx):
        part_rows, emb_width = ent_table.shape
        rel_rows = rel_table.shape[0]
        bucket_edges = head_idx.shape[2] * data_reps
        shard = part_rows // 4
        tail_bits = (part_rows - 1).bit_length()
        head_bits = (shard - 1).bit_length()
        spare = 2**(REL_PAD - 1).bit_length() - 1
        ent = lax.axis_index('ent')
        _, _, core, top, bot = where_here()

        words, rel_ids, counts, neg, table, ent_now, rel_now = setup_call(
            (head_bits, tail_bits, spare), head_idx[0], tail_idx[0], rel_idx[0], edge_mask[0], neg_idx[0], data_reps,
            ent_table.T, jnp.pad(rel_table.T, ((0, 0), (0, REL_PAD - rel_rows))))
        to_core = lambda c: lax.dynamic_slice_in_dim(ent_state, (2 * bot + c) * shard, shard)
        away = [(d * groups + 2 * (n // 2) + d // 2, d * groups + 2 * (n // 2) + 1 - d // 2) for d in range(data_reps) for n in range(0, groups, 2)]
        state_now = jnp.where(core == top, to_core(core), lax.ppermute(to_core(1 - core), ('data', 'ent'), away))[:, None]
        rel_state = jnp.zeros((REL_PAD, 1), F32)
        losses = []
        for step in range(groups):
            tail, head, rel_grad = bucket_call(step, tail_bits + 2, words, counts, neg, rel_ids, ent_now, rel_now, table)
            out = exchange_call(step, groups, emb_width, tail, head, rel_grad, ent_now, state_now, rel_now, rel_state)
            if step + 1 < groups:
                ent_now, state_now, rel_now, rel_state, loss, table = out
            else:
                wire, rel_now, loss = out
            losses.append(loss)
        ent_out, state_out, rel_out = finish_call(wire, rel_now, emb_width)
        loss_rows = below(losses) / bucket_edges
        bucket_loss = lax.dynamic_slice_in_dim(loss_rows, ent, 1, axis=1).reshape(1, groups)
        return ent_out.T, state_out[0], rel_out[:, :rel_rows].T, bucket_loss

    return jax.shard_map(device_fn, mesh=mesh, in_specs=(row_spec, P(('sweep', 'ent')), P('sweep', None), edge_spec, edge_spec, edge_spec, edge_spec, P(('sweep', 'ent'), None, None)), out_specs=(row_spec, P(('sweep', 'ent')), P('sweep', None), row_spec), check_vma=False)
```

```python
import functools

import jax
import jax.numpy as jnp
from jax import lax
from jax.experimental import pallas as pl
from jax.experimental.pallas import tpu as pltpu
from jax.sharding import PartitionSpec as P

LR_SCALE = 0.2
EPSILON = 1e-8
LANES = 128
HALF = 64
LEFT = 8
BLOCK = 256
CHUNK = 128
UNROLL = 64
ROLLED = 32
TOGETHER = 8
AHEAD = 6
LAG = 3
PARTS = 4
REL_HOPS = 6
STRIP = 32
REL_PAD = 128
TILES = range(4)
CORES = range(2)
ROW_COL, ROW_ROW, COL_COL = (((1,), (0,)), ((1,), (1,)), ((0,), (0,)))
F32 = jnp.float32
BF16 = jnp.bfloat16
VMEM_LIMIT = 60 * 2**20


def roll(x, by):
    return pltpu.roll(x, by, 1)


def beside(parts):
    return jnp.concatenate(parts, axis=1)


def below(parts):
    return jnp.concatenate(parts, axis=0)


def lanes(shape):
    return lax.broadcasted_iota(jnp.int32, shape, 1)


def sublanes(shape):
    return lax.broadcasted_iota(jnp.int32, shape, 0)


def one_where(mask):
    return jnp.where(mask, 1.0, 0.0)


def on_diagonal(size):
    return sublanes((size, size)) == lanes((size, size))


def row_sum(x):
    return jnp.sum(x, axis=1, keepdims=True)


def column_sum(x):
    return jnp.sum(x, axis=0, keepdims=True)


def wire_rows(rows):
    return 3 * rows + rows // LEFT


def flipped(tiles):
    rows, columns = tiles[0].shape
    unit = one_where(on_diagonal(columns)).astype(BF16)
    high, mid, low = (dot(unit, piece, ROW_ROW) for piece in in_three(below(tiles)))
    both = high + mid + low
    return [both[:, band(t, rows)] for t in TILES]


def columns_to_tiles(x):
    half = x.shape[0] // 2
    a, c, d = slice(0, LANES), slice(LANES, LANES + HALF), slice(LANES + HALF, half)
    re, im = x[:half], x[half:]
    zero = jnp.zeros((HALF - LEFT, x.shape[1]), x.dtype)
    return flipped([re[a], im[a], below([re[c], im[c]]), below([re[d], zero, im[d], zero])])


def tiles_to_columns(tiles):
    a, b, c, d = flipped(tiles)
    high = slice(HALF, HALF + LEFT)
    return below([a, c[:HALF], d[:LEFT], b, c[HALF:], d[high]])


def each_row(count, body):
    for u in range(count):
        body(u)


def band(n, size):
    return slice(n * size, (n + 1) * size)


def where_here():
    y, ent = lax.axis_index('data'), lax.axis_index('ent')
    return y, ent // 2, ent % 2, y // 2, y % 2


def fold_last(tile):
    n = tile.shape[0] // LEFT
    out = tile[:n]
    for k in range(1, LEFT):
        out = out + roll(tile[band(k, n)], LEFT * k)
    return out


def unfold_last(packed):
    keep = lanes(packed.shape) % HALF < LEFT
    return [jnp.where(keep, packed if k == 0 else roll(packed, LANES - LEFT * k), 0.0) for k in range(LEFT)]


def tiles_of(x):
    return [x[:, band(t, LANES)] for t in TILES]


def times(x, y):
    out = [x[0] * y[0] - x[1] * y[1], x[0] * y[1] + x[1] * y[0]]
    for a, b in zip(x[2:], y[2:]):
        low = lanes(a.shape) < HALF
        a_swap, b_swap = roll(a, HALF), roll(b, HALF)
        out.append(jnp.where(low, a * b - a_swap * b_swap, a_swap * b + a * b_swap))
    return out


def times_conj(x, y):
    out = [x[0] * y[0] + x[1] * y[1], x[1] * y[0] - x[0] * y[1]]
    for a, b in zip(x[2:], y[2:]):
        low = lanes(a.shape) < HALF
        a_swap, b_swap = roll(a, HALF), roll(b, HALF)
        out.append(jnp.where(low, a * b + a_swap * b_swap, a * b_swap - a_swap * b))
    return out


def tiles_at(ref, row, rows):
    block = ref[pl.ds(row * 4, rows * 4), :].reshape(rows // 8, 32, LANES)
    return [block[:, 8 * t:8 * t + 8].reshape(rows, LANES) for t in TILES]


def stack_tiles(tiles):
    rows = tiles[0].shape[0]
    return beside([t.reshape(rows // 8, 8, LANES) for t in tiles]).reshape(rows * 4, LANES)


def row_at(address):
    return pl.ds(address, 4, stride=8)


def row_address(row):
    return (row >> 3 << 5) | (row & 7)


def in_three(x):
    pieces = []
    for _ in range(3):
        piece = x.astype(BF16)
        pieces.append(piece)
        x = x - piece.astype(F32)
    return pieces


def dot(x, y, dims):
    return lax.dot_general(x, y, (dims, ((), ())), preferred_element_type=F32)


def bucket_kernel(cfg, edges_hbm, count_ref, negs_hbm, rel_ids_hbm, ent_hbm, rel_ref, table_hbm, tail_hbm, head_hbm, rel_out,
                  tail_rows, head_next, tail_next, head_buf, tail_buf, gh_last, gt_last, rel_buf, query_buf, pos_buf, score_buf, d_neg_buf, grad_buf, piece_buf,
                  neg_rows, neg_grad, rel_three, tail_acc0, tail_acc1, head_acc0, head_acc1, rel_acc, loss_acc,
                  edge_ref, neg_ref, rel_id_ref, ent_ref, table_ref, tail_out, head_out, sems, table_sems, tail_sems):
    step, tail_bits = cfg
    chunk = CHUNK
    part = chunk // LEFT
    tail_acc, head_acc = (tail_acc0, tail_acc1), (head_acc0, head_acc1)
    count = count_ref[step, 0]
    negs = neg_ref.shape[0]
    loads = [
        pltpu.make_async_copy(negs_hbm.at[step, 0], neg_ref, sems.at[0]),
        pltpu.make_async_copy(rel_ids_hbm.at[step], rel_id_ref, sems.at[2]),
        pltpu.make_async_copy(ent_hbm, ent_ref, sems.at[3]),
    ]
    parts = table_sems.shape[0]
    size = table_ref.shape[0] // parts
    tables = [pltpu.make_async_copy(table_hbm.at[band(n, size)], table_ref.at[band(n, size)], table_sems.at[n]) for n in range(parts)]
    blocks = pl.cdiv(count, BLOCK)

    def edge_pieces(act):
        def one(n, carry):
            span = pl.ds(pl.multiple_of(n * 2 * BLOCK, 2 * BLOCK), 2 * BLOCK)
            act(pltpu.make_async_copy(edges_hbm.at[step, 0, span], edge_ref.at[span], sems.at[1]))
            return carry

        lax.fori_loop(0, (blocks + 3) // 2, one, 0)

    edge_pieces(lambda copy: copy.start())
    for load in loads + tables:
        load.start()

    def head_of(e):
        return row_at(e >> tail_bits)

    def tail_of(e):
        return row_at(e & (2**tail_bits - 1))

    def clear(accs, n, carry):
        for acc in accs:
            acc[pl.ds(pl.multiple_of(n * chunk * 4, chunk * 4), chunk * 4), :] = jnp.zeros((chunk * 4, LANES), F32)
        return carry

    lax.fori_loop(0, table_ref.shape[0], functools.partial(clear, tail_acc), 0)
    lax.fori_loop(0, head_out.shape[0], functools.partial(clear, head_acc), 0)
    neg_grad[...] = jnp.zeros_like(neg_grad)
    gh_last[...] = jnp.zeros_like(gh_last)
    gt_last[...] = jnp.zeros_like(gt_last)
    rel_acc[...] = jnp.zeros_like(rel_acc)
    loss_acc[...] = jnp.zeros_like(loss_acc)
    for n, piece in enumerate(in_three(rel_ref[...])):
        rel_three[band(n, REL_PAD), :] = piece
    for load in loads:
        load.wait()
    edge_pieces(lambda copy: copy.wait())

    def widen(i, carry):
        for n in (i * TOGETHER + k for k in range(TOGETHER)):
            tiles = [table_ref[n, band(t, chunk), :].astype(F32) for t in TILES[:-1]]
            tiles.append(below(unfold_last(table_ref[n, 3 * chunk:, :].astype(F32))))
            tail_rows[pl.ds(pl.multiple_of(n * chunk * 4, chunk * 4), chunk * 4), :] = stack_tiles(tiles)
        return carry

    for n, load in enumerate(tables):
        load.wait()
        lax.fori_loop(n * size // TOGETHER, (n + 1) * size // TOGETHER, widen, 0)

    def take_negs(n, carry):
        base = pl.multiple_of(n * UNROLL, UNROLL)

        def take(u):
            head_buf[row_at(row_address(u)), :] = tail_rows[row_at(neg_ref[base + u]), :]

        each_row(UNROLL, take)
        for t, tile in enumerate(tiles_at(head_buf, 0, UNROLL)):
            neg_rows[pl.ds(base, UNROLL), band(t, LANES)] = tile.astype(BF16)
        return carry

    lax.fori_loop(0, negs // UNROLL, take_negs, 0)

    def take_edges(base, row=0):
        def take(u):
            e = edge_ref[base + u]
            place = row_at(row * 4 + row_address(u))
            head_next[place, :] = ent_ref[head_of(e), :]
            tail_next[place, :] = tail_rows[tail_of(e), :]

        return take

    def put_edges(base, row=0):
        def put(pair):
            for lane in range(2):
                u = 2 * pair + lane
                e = edge_ref[base + u]
                place = row_at(row * 4 + row_address(u))
                head_acc[lane][head_of(e), :] += gh_last[place, :]
                tail_acc[lane][tail_of(e), :] += gt_last[place, :]

        return put


    def take_first(n, carry):
        row = pl.multiple_of(n * ROLLED, ROLLED)
        each_row(ROLLED, take_edges(BLOCK + row, row))
        return carry

    lax.fori_loop(0, BLOCK // ROLLED, take_first, 0)
    spans = [slice(r, r + STRIP) for r in range(0, BLOCK, STRIP)]

    def block(n, carry):
        base = pl.multiple_of(n * BLOCK, BLOCK)
        hot = sublanes((REL_PAD, BLOCK)) == rel_id_ref[:, pl.ds(base, BLOCK)]
        hot = one_where(hot).astype(BF16)
        rel_buf[...] = dot(below([hot] * 3), rel_three[...], COL_COL)
        for span in spans:
            head, tail, rel = tiles_at(head_next, span.start, STRIP), tiles_at(tail_next, span.start, STRIP), tiles_of(rel_buf[span, :])
            wide = slice(4 * span.start, 4 * span.stop)
            head_buf[wide, :], tail_buf[wide, :] = stack_tiles(head), stack_tiles(tail)
            total = None
            for t, q in enumerate(times(head, rel)):
                q = q.astype(BF16)
                query_buf[span, band(t, LANES)] = q
                product = q.astype(F32) * tail[t]
                total = product if total is None else total + product
            pos_buf[span, :] = row_sum(total)
        each_row(BLOCK, take_edges(base + 2 * BLOCK))
        each_row(BLOCK // 2, put_edges(base))
        score_buf[...] = dot(query_buf[...], neg_rows[...], ROW_ROW)
        for span in spans:
            weight = one_where(sublanes((STRIP, 1)) + (base + span.start) < count)
            score, pos = score_buf[span, :], pos_buf[span, :]
            top = jnp.maximum(jnp.max(score, axis=1, keepdims=True), pos)
            pos_exp = jnp.exp(pos - top)
            neg_exp = jnp.exp(score - top)
            total = pos_exp + row_sum(neg_exp)
            loss_acc[...] += column_sum(weight * (top + jnp.log(total) - pos))
            pos_buf[span, :] = weight * (pos_exp / total - 1.0)
            d_neg_buf[span, :] = ((weight / total) * neg_exp).astype(BF16)
        grad_buf[...] = dot(d_neg_buf[...], neg_rows[...], ROW_COL)
        neg_grad[...] += dot(d_neg_buf[...], query_buf[...], COL_COL)
        for span in spans:
            wide = slice(4 * span.start, 4 * span.stop)
            d_pos = pos_buf[span, :]
            tail, rel = tiles_at(tail_buf, span.start, STRIP), tiles_of(rel_buf[span, :])
            grad_q = [d_pos * x + y for x, y in zip(tail, tiles_of(grad_buf[span, :]))]
            gt_last[wide, :] = stack_tiles([d_pos * q.astype(F32) for q in tiles_of(query_buf[span, :])])
            gh_last[wide, :] = stack_tiles(times_conj(grad_q, rel))
            for t, grad in enumerate(times_conj(grad_q, tiles_at(head_buf, span.start, STRIP))):
                for k, piece in enumerate(in_three(grad)):
                    piece_buf[k * BLOCK + span.start:k * BLOCK + span.stop, band(t, LANES)] = piece
        rel_acc[...] += dot(beside([hot] * 3), piece_buf[...], ROW_COL)
        return carry

    lax.fori_loop(0, blocks, block, 0)

    def put_last(n, carry):
        row = pl.multiple_of(n * ROLLED, ROLLED)
        each_row(ROLLED // 2, put_edges(blocks * BLOCK + row, row))
        return carry

    lax.fori_loop(0, BLOCK // ROLLED, put_last, 0)

    def put_negs(n, carry):
        base = pl.multiple_of(n * UNROLL, UNROLL)
        gt_last[:4 * UNROLL, :] = stack_tiles(tiles_of(neg_grad[pl.ds(base, UNROLL), :]))

        def put(pair):
            for lane in range(2):
                u = 2 * pair + lane
                tail_acc[lane][row_at(neg_ref[base + u]), :] += gt_last[row_at(row_address(u)), :]

        each_row(UNROLL // 2, put)
        return carry

    lax.fori_loop(0, negs // UNROLL, put_negs, 0)

    def emit(out_ref, acc, i, carry):
        for n in (i * TOGETHER + k for k in range(TOGETHER)):
            base = pl.multiple_of(n * chunk, chunk)
            tiles = [a + b for a, b in zip(tiles_at(acc[0], base, chunk), tiles_at(acc[1], base, chunk))]
            for t in TILES[:-1]:
                out_ref[n, band(t, chunk), :] = tiles[t]
            out_ref[n, 3 * chunk:, :] = fold_last(tiles[3])
        return carry

    stores = []
    for n in range(tail_sems.shape[0]):
        out, dst, acc, span = (head_out, head_hbm, head_acc, range(head_out.shape[0])) if n == parts else (tail_out, tail_hbm, tail_acc, range(n * size, (n + 1) * size))
        lax.fori_loop(span.start // TOGETHER, span.stop // TOGETHER, functools.partial(emit, out, acc), 0)
        part_of = pl.ds(span.start, len(span))
        stores.append(pltpu.make_async_copy(out.at[part_of], dst.at[part_of], tail_sems.at[n]))
        stores[-1].start()
    _, x, _, top, _ = where_here()
    group = 2 * x + top
    row = sublanes((REL_PAD, LANES))
    lane = lanes((REL_PAD, LANES))
    loss = jnp.where(lane == group, loss_acc[...], 0.0)
    for t in TILES[:-1]:
        rows = rel_acc[:, band(t, LANES)]
        rel_out[band(t, REL_PAD), :] = jnp.where(row == REL_PAD - 1, loss, rows) if t == 0 else rows
    rel_out[3 * REL_PAD:, :] = fold_last(rel_acc[:, 3 * LANES:])
    for store in stores:
        store.wait()


def dma_sems(n):
    return pltpu.SemaphoreType.DMA((n,))


def bucket_call(step, tail_bits, edges, counts, negs, rel_ids, ent, rel, table):
    smem, vmem, hbm = (pl.BlockSpec(memory_space=m) for m in (pltpu.SMEM, pltpu.VMEM, pl.ANY))
    rows, neg_count, chunks = ent.shape[0] // 4, negs.shape[-1], table.shape[0]
    width = 4 * LANES
    wire = wire_rows(CHUNK)
    block = pltpu.VMEM((BLOCK * 4, LANES), F32)
    table_rows = pltpu.VMEM((chunks * CHUNK * 4, LANES), F32)
    head_rows = pltpu.VMEM((rows * 4, LANES), F32)
    return pl.pallas_call(
        functools.partial(bucket_kernel, (step, tail_bits)),
        out_shape=(
            jax.ShapeDtypeStruct((chunks, wire, LANES), F32),
            jax.ShapeDtypeStruct((rows // CHUNK, wire, LANES), F32),
            jax.ShapeDtypeStruct((wire_rows(REL_PAD), LANES), F32),
        ),
        in_specs=[hbm, smem, hbm, hbm, hbm, vmem, hbm],
        out_specs=(hbm, hbm, vmem),
        scratch_shapes=[
            table_rows, *[block] * 6, pltpu.VMEM((BLOCK, width), F32), pltpu.VMEM((BLOCK, width), BF16), pltpu.VMEM((BLOCK, 1), F32),
            pltpu.VMEM((BLOCK, neg_count), F32), pltpu.VMEM((BLOCK, neg_count), BF16), pltpu.VMEM((BLOCK, width), F32), pltpu.VMEM((3 * BLOCK, width), BF16),
            pltpu.VMEM((neg_count, width), BF16), pltpu.VMEM((neg_count, width), F32), pltpu.VMEM((3 * REL_PAD, width), BF16),
            table_rows, table_rows, head_rows, head_rows,
            pltpu.VMEM((REL_PAD, width), F32), pltpu.VMEM((1, 1), F32),
            pltpu.SMEM((edges.shape[-1],), jnp.int32), pltpu.SMEM((neg_count,), jnp.int32), pltpu.VMEM(rel_ids.shape[1:], jnp.int32),
            pltpu.VMEM(ent.shape, F32), pltpu.VMEM(table.shape, BF16), pltpu.VMEM((chunks, wire, LANES), F32), pltpu.VMEM((rows // CHUNK, wire, LANES), F32),
            dma_sems(4), dma_sems(PARTS), dma_sems(PARTS + 1),
        ],
        compiler_params=pltpu.CompilerParams(vmem_limit_bytes=VMEM_LIMIT),
        name='bucket',
    )(edges, counts, negs, rel_ids, ent, rel, table)


def entry(peers):
    barrier = pltpu.get_barrier_semaphore()
    for peer in peers:
        pl.semaphore_signal(barrier, inc=1, device_id=peer, device_id_type=pl.DeviceIdType.MESH)
    pl.semaphore_wait(barrier, len(peers))


def remote(src, dst, send, recv, peer):
    return pltpu.make_async_remote_copy(src_ref=src, dst_ref=dst, send_sem=send, recv_sem=recv, device_id=peer, device_id_type=pl.DeviceIdType.MESH)


def adagrad(rows, state, grad, mean_of, learn_rate):
    square = sum(g * g for g in grad)
    state = state + row_sum(square) / mean_of
    root = jnp.sqrt(state + EPSILON)
    return [r - learn_rate * (g / root) for r, g in zip(rows, grad)], state


def exchange_kernel(cfg, tail_ref, head_hbm, rel_grad_ref, ent_hbm, state_ref, rel_ref, rel_state_ref, *refs):
    step, groups, chunks, emb_width, last = cfg
    if last:
        ent_wire, rel_out, loss_out, *refs = refs
    else:
        ent_out, state_out, rel_out, rel_state_out, loss_out, table_hbm, *refs, table, store_sem = refs
    (own, from_core, from_y, from_group, rel_sum, rel_from, send_buf,
     own_sem, core_send, core_recv, y_send, y_recv, group_send, group_recv, rel_send, rel_recv, out_send, out_recv, head_ref, ent_ref, row_sem) = refs
    learn_rate = LR_SCALE * emb_width ** -0.25
    chunk = CHUNK
    y, x, core, top, bot = where_here()
    mine = 2 * x + top
    x_size = groups // 2

    def place(group, low, c):
        return {'data': 2 * (group % 2) + low, 'ent': 2 * (group // 2) + c}

    def at(dy, dx, c):
        return {'data': dy, 'ent': 2 * dx + c}

    def slot_of(low, c, k):
        return (low * 2 + c) * chunks + k

    def turned(shift):
        return (bot + shift) % 2

    other_core = at(y, x, 1 - core)
    other_y = at(2 * top + 1 - bot, x, core)
    rel_peers = (other_core, other_y, at(3 - y, x, core), at(y, x + 1 - 2 * (x % 2), core), at(y, x_size - 1 - x, core), other_core)
    grad_to = place((mine + step) % groups, turned(step), core)
    grad_from = place((mine + groups - step) % groups, turned(step), core)
    nxt = step + 1
    table_to = place((mine + groups - nxt) % groups, turned(nxt), core)
    table_from = place((mine + nxt) % groups, turned(nxt), core)
    peers = list(rel_peers)
    if step:
        peers += [grad_to, grad_from]
    if last:
        for turn in range(4):
            peers.append(at((y + turn) % 4, x, top))
        senders = [at((2 * core + d), x, c) for d in range(2) for c in range(2)]
        peers += senders
    else:
        peers += [table_to, table_from]
    entry(peers)
    keep = turned(step)
    pending = []

    def start(copy):
        copy.start()
        pending.append(copy)
        return copy

    shards = [(1 - keep, k) for k in range(chunks)] + [(keep, k) for k in range(chunks)]
    loads, cores = [], []
    row_loads = [pltpu.make_async_copy(src, dst, row_sem.at[n]) for n, (src, dst) in enumerate(((head_hbm, head_ref), (ent_hbm, ent_ref)))]
    for load in row_loads:
        load.start()
    stores = []

    def store(n, src, dst):
        copy = pltpu.make_async_copy(src, dst, store_sem.at[n])
        copy.start()
        stores.append(copy)

    def store_table(low, c, k):
        slot = slot_of(low, c, k)
        store(slot, table.at[slot], table_hbm.at[slot])

    rel_copies = [start(remote(rel_grad_ref.at[1 - core], rel_from.at[0], rel_send.at[0], rel_recv.at[0], rel_peers[0]))]
    for n, (low, k) in enumerate(shards):
        cores.append(start(remote(tail_ref.at[slot_of(low, 1 - core, k)], from_core.at[n], core_send.at[n], core_recv.at[n], other_core)))
        load = pltpu.make_async_copy(tail_ref.at[slot_of(low, core, k)], own.at[n], own_sem.at[n])
        load.start()
        loads.append(load)

    def rel_step(n):
        rel_copies[n].wait_recv()
        rel_sum[n] = (rel_grad_ref[core] if n == 0 else rel_sum[n - 1]) + rel_from[n]
        rel_copies.append(start(remote(rel_sum.at[n], rel_from.at[n + 1], rel_send.at[n + 1], rel_recv.at[n + 1], rel_peers[n + 1])))

    ys = []
    for k in range(chunks):
        loads[k].wait()
        cores[k].wait_recv()
        own[k] = own[k] + from_core[k]
        ys.append(start(remote(own.at[k], from_y.at[k], y_send.at[k], y_recv.at[k], other_y)))
        if k == 1:
            rel_step(0)
    for k in range(chunks, 2 * chunks):
        loads[k].wait()
        cores[k].wait_recv()
        own[k] = own[k] + from_core[k]
    gs, outs, forwards, crosses = [], [], [], []

    def stage_group(k):
        ys[k].wait_recv()
        own[chunks + k] = own[chunks + k] + from_y[k]
        if step:
            gs.append(start(remote(own.at[chunks + k], from_group.at[k], group_send.at[k], group_recv.at[k], grad_to)))

    def cross_copy(k):
        slot = slot_of(bot, core, k)
        return remote(send_buf.at[k], ent_wire.at[slot], out_send.at[2 * chunks + k], out_recv.at[slot], other_core)

    turn = (y + 4 - 2 * core) % 4
    near = 1 - turn % 2
    back = jnp.where((turn == 1) | (turn == 2), 0, 1)
    onward = at((y + 1 + 2 * back) % 4, x, core)

    def landed(low, c, k):
        slot = slot_of(low, c, k)
        remote(ent_wire.at[slot], ent_wire.at[slot], out_send.at[0], out_recv.at[slot], other_core).wait_recv()

    def stage_relay(k):
        if k % 2 == 0:
            return
        for c in CORES:
            landed(near, c, k - 1)
            landed(near, c, k)
            slot = slot_of(near, c, k) - 1 + back
            start(remote(ent_wire.at[slot], ent_wire.at[slot], out_send.at[(3 + c) * chunks + k], out_recv.at[slot], onward))

    def stage_update(k):
        if k == 0:
            for load in row_loads:
                load.wait()
        if step:
            gs[k].wait_recv()
        total = from_group if step else own
        base = k if step else chunks + k
        grad = [total[base, band(t, chunk), :] + head_ref[k, band(t, chunk), :] for t in TILES[:-1]]
        grad.append(below(unfold_last(total[base, 3 * chunk:, :] + head_ref[k, 3 * chunk:, :])))
        span = band(k, chunk)
        rows, state = adagrad(tiles_at(ent_ref, k * chunk, chunk), state_ref[span, :], grad, emb_width, learn_rate)
        wire = rows[:3] + [fold_last(rows[3])]
        if last:
            lane = lanes((chunk, LANES))
            wire.append(fold_last(jnp.where(lane < 1, state, 0.0)))
        else:
            wide = band(k, 4 * chunk)
            ent_ref[wide, :] = stack_tiles(rows)
            store(4 * chunks + k, ent_ref.at[wide], ent_out.at[wide])
            state_out[span, :] = state
        offset = 0
        for piece in wire:
            send_buf[k, offset:offset + piece.shape[0], :] = piece.astype(send_buf.dtype)
            offset += piece.shape[0]
        slot = slot_of(bot, core, k)
        if last:
            for n, turn in enumerate((1, 3)):
                start(remote(send_buf.at[k], ent_wire.at[slot], out_send.at[n * chunks + k], out_recv.at[slot], at((y + turn) % 4, x, top)))

            @pl.when(core == top)
            def _():
                pltpu.make_async_copy(send_buf.at[k], ent_wire.at[slot], out_recv.at[slot]).start()

            @pl.when(core != top)
            def _():
                cross_copy(k).start()
        else:
            outs.append(start(remote(send_buf.at[k], table.at[slot], out_send.at[k], out_recv.at[k], table_to)))

    def forward(n, low, k, peer):
        slot = slot_of(low, core, k)
        return start(remote(table.at[slot], table.at[slot], out_send.at[n * chunks + k], out_recv.at[n * chunks + k], peer))

    def stage_forward(k):
        outs[k].wait_recv()
        store_table(turned(nxt), core, k)
        forwards.append(forward(1, turned(nxt), k, other_y))
        crosses.append((forward(2, turned(nxt), k, other_core), turned(nxt), k))

    def stage_cross(k):
        forwards[k].wait_recv()
        store_table(1 - turned(nxt), core, k)
        crosses.append((forward(3, 1 - turned(nxt), k, other_core), 1 - turned(nxt), k))

    stages = (stage_group, stage_update, stage_relay) if last else (stage_group, stage_update, stage_forward, stage_cross)
    rel_steps = len(rel_peers) - 1
    for tick in range(chunks + LAG * (len(stages) - 1)):
        for n, stage in enumerate(stages):
            if 0 <= tick - LAG * n < chunks:
                stage(tick - LAG * n)
        if tick % 2 == 1 and tick < 2 * rel_steps - 1:
            rel_step(tick // 2 + 1)

    rel_copies[rel_steps].wait_recv()
    halves = rel_sum[rel_steps - 1], rel_from[rel_steps]
    summed = below([jnp.where(core == n, halves[0], halves[1]) for n in CORES])
    rel_grad = [summed[band(t, REL_PAD)] for t in TILES[:-1]] + [below(unfold_last(summed[3 * REL_PAD:]))]
    loss_out[...] = rel_grad[0][REL_PAD - 1:, :]
    row = sublanes((REL_PAD, LANES))
    rel_grad[0] = jnp.where(row < REL_PAD - 1, rel_grad[0], 0.0)
    rel_rows, rel_state = adagrad(tiles_of(rel_ref[...]), rel_state_ref[...], rel_grad, emb_width, learn_rate)
    for t in TILES:
        rel_out[:, band(t, LANES)] = rel_rows[t]
    if not last:
        rel_state_out[...] = rel_state

    if last:
        for c in CORES:
            for k in range(chunks):
                landed(1 - near, c, k)

        @pl.when(core != top)
        def _():
            for k in range(chunks):
                cross_copy(k).wait_send()
    else:
        for copy, low, k in crosses:
            copy.wait_recv()
            store_table(low, 1 - core, k)
        for copy in stores:
            copy.wait()
    for copy in pending:
        copy.wait_send()


def exchange_call(step, groups, emb_width, tail, head, rel_grad, ent, state, rel, rel_state):
    vmem, hbm = pl.BlockSpec(memory_space=pltpu.VMEM), pl.BlockSpec(memory_space=pl.ANY)
    chunks = head.shape[0]
    rel_grad = rel_grad.reshape(2, -1, LANES)
    wire = wire_rows(CHUNK)
    last = step == groups - 1
    like = lambda x: jax.ShapeDtypeStruct(x.shape, x.dtype)
    loss = jax.ShapeDtypeStruct((1, LANES), F32)
    out_wire = wire + (CHUNK // LEFT if last else 0)
    out_type = F32 if last else BF16
    gathered = jax.ShapeDtypeStruct((4 * chunks, out_wire, LANES), out_type)
    out_shape = (gathered, like(rel), loss) if last else (like(ent), like(state), like(rel), like(rel_state), loss, gathered)
    return pl.pallas_call(
        functools.partial(exchange_kernel, (step, groups, chunks, emb_width, last)),
        out_shape=out_shape,
        in_specs=[hbm, hbm, vmem, hbm, vmem, vmem, vmem],
        out_specs=(vmem,) * 3 if last else (hbm, vmem, vmem, vmem, vmem, hbm),
        scratch_shapes=[
            pltpu.VMEM((2 * chunks, wire, LANES), F32), pltpu.VMEM((2 * chunks, wire, LANES), F32),
            pltpu.VMEM((chunks, wire, LANES), F32), pltpu.VMEM((chunks, wire, LANES), F32),
            pltpu.VMEM((REL_HOPS - 1, *rel_grad.shape[1:]), F32), pltpu.VMEM((REL_HOPS, *rel_grad.shape[1:]), F32),
            pltpu.VMEM((chunks, out_wire, LANES), out_type),
            *[dma_sems(2 * chunks)] * 3, *[dma_sems(chunks)] * 4,
            dma_sems(REL_HOPS), dma_sems(REL_HOPS), dma_sems(5 * chunks), dma_sems(4 * chunks),
            pltpu.VMEM(head.shape, F32), pltpu.VMEM(ent.shape, F32), dma_sems(2),
            *(() if last else (pltpu.VMEM(gathered.shape, BF16), dma_sems(5 * chunks))),
        ],
        compiler_params=pltpu.CompilerParams(vmem_limit_bytes=VMEM_LIMIT, collective_id=step, has_side_effects=True),
        name='exchange',
    )(tail, head, rel_grad, ent, state, rel, rel_state)


def setup_kernel(cfg, head_ref, tail_ref, rel_id_ref, mask_ref, neg_ref, ent_hbm, rel_ref, word_out, rel_id_out, count_out, neg_out, table, ent_out, rel_out,
                 packed, shares, neg_buf, rows_buf, away, send_sem, recv_sem, core_send, core_recv, load_sem, table_send, table_recv):
    head_bits, tail_bits, spare = cfg
    y, x, core, top, bot = where_here()
    home = core == top
    other_core = {'data': y, 'ent': 2 * x + 1 - core}
    users = [(c, 2 * core + d) for c in CORES for d in CORES]
    users = [({'data': row, 'ent': 2 * x + c}, (core == c) & (y == row)) for c, row in users]
    entry([peer for peer, _ in users] + [{'data': row, 'ent': 2 * x + top} for row in TILES] + [other_core])
    edges = head_ref[...] | (tail_ref[...] << tail_bits) | (rel_id_ref[...] << (2 * tail_bits))
    packed[...] = jnp.where(mask_ref[...] > 0, edges, spare << (2 * tail_bits))
    neg_buf[:, 0, :] = row_address(neg_ref[...])
    to_users = [remote(packed, shares.at[y], send_sem.at[n], recv_sem.at[y], peer) for n, (peer, _) in enumerate(users)]
    for copy, (_, here) in zip(to_users, users):
        @pl.when(jnp.logical_not(here))
        def _():
            copy.start()

    chunks, chunk = table.shape[0], CHUNK
    shard = chunks // 4

    def load(n):
        return pltpu.make_async_copy(ent_hbm.at[:, pl.ds(pl.multiple_of(n * chunk, chunk), chunk)], rows_buf.at[n % rows_buf.shape[0]], load_sem.at[n % rows_buf.shape[0]])

    def table_copy(q):
        part = table.at[pl.ds(q * shard, shard)]
        return remote(part, part, table_send.at[q], table_recv.at[q], other_core)

    neg_copy = remote(neg_buf, neg_out, core_send.at[0], core_recv.at[0], other_core)
    ent_copy = remote(away, ent_out, core_send.at[1], core_recv.at[1], other_core)

    @pl.when(home)
    def _():
        pltpu.make_async_copy(packed, shares.at[y], recv_sem.at[y]).start()
        neg_copy.start()
        neg_out[...] = neg_buf[...]
        for n in range(AHEAD):
            load(n).start()
        for q in TILES:
            def one(pair, carry):
                first = 2 * pair
                for c in CORES:
                    n = q * shard + first + c

                    @pl.when(n + AHEAD < chunks)
                    def _():
                        load(n + AHEAD).start()

                    load(n).wait()
                both = [(first + c, columns_to_tiles(rows_buf[(q * shard + first + c) % rows_buf.shape[0]])) for c in CORES]
                for k, tiles in both:
                    n = q * shard + k
                    for t in TILES[:-1]:
                        table[n, band(t, chunk), :] = tiles[t].astype(BF16)
                    table[n, 3 * chunk:, :] = fold_last(tiles[3]).astype(BF16)
                    rows = stack_tiles(tiles)
                    place = pl.ds(pl.multiple_of(k * chunk * 4, chunk * 4), chunk * 4)

                    @pl.when(2 * bot + core == q)
                    def _():
                        ent_out[place, :] = rows

                    @pl.when(2 * bot + 1 - core == q)
                    def _():
                        away[place, :] = rows

                return carry

            lax.fori_loop(0, shard // 2, one, 0)
            table_copy(q).start()

            @pl.when(2 * bot + 1 - core == q)
            def _():
                ent_copy.start()

    for t, tile in enumerate(columns_to_tiles(rel_ref[...])):
        rel_out[:, band(t, LANES)] = tile
    for row in TILES:
        remote(packed, shares.at[row], send_sem.at[0], recv_sem.at[row], other_core).wait_recv()
    share = beside([shares[row] for row in TILES])
    mine = ((share >> head_bits) & 3 == 2 * bot + core) & (share >> (2 * tail_bits) != spare)
    lane = lanes(share.shape)
    width = share.shape[1]
    steps = (width - 1).bit_length()
    other = jnp.where(mine, 0, 1)
    before = other
    for bit in range(steps):
        before = before + jnp.where(lane < 2**bit, 0, roll(before, 2**bit))
    count_out[...] = jnp.broadcast_to(width - before[:, width - 1:], count_out.shape)
    none = spare << (head_bits + tail_bits)
    edge = jnp.where(mine, (share & (2**head_bits - 1)) | (share >> tail_bits << head_bits), none)
    shift = jnp.where(mine, before - other, 0)
    for bit in range(steps):
        here = (shift >> bit) & 1 == 1
        edge_in, shift_in = roll(edge, width - 2**bit), roll(shift, width - 2**bit)
        there = (shift_in >> bit) & 1 == 1
        edge = jnp.where(there, edge_in, jnp.where(here, none, edge))
        shift = jnp.where(there, shift_in, jnp.where(here, 0, shift))
    rel_id_out[:, 0, :] = edge >> (head_bits + tail_bits)
    head, tail = edge & (2**head_bits - 1), (edge >> head_bits) & (2**tail_bits - 1)
    margin = jnp.zeros((share.shape[0], BLOCK), jnp.int32)
    word_out[:, 0, :] = beside([margin, (row_address(head) << (tail_bits + 2)) | row_address(tail), margin])
    for copy, (_, here) in zip(to_users, users):
        @pl.when(jnp.logical_not(here))
        def _():
            copy.wait_send()

    between = [neg_copy, ent_copy, *(table_copy(q) for q in TILES)]

    @pl.when(home)
    def _():
        for copy in between:
            copy.wait_send()

    @pl.when(jnp.logical_not(home))
    def _():
        for copy in between:
            copy.wait_recv()


def setup_call(cfg, head, tail, rel_ids, mask, neg, reps, ent, rel):
    vmem, hbm = pl.BlockSpec(memory_space=pltpu.VMEM), pl.BlockSpec(memory_space=pl.ANY)
    groups, share = head.shape
    width, rows = ent.shape
    chunks = rows // CHUNK
    return pl.pallas_call(
        functools.partial(setup_kernel, cfg),
        out_shape=(*(jax.ShapeDtypeStruct(shape, jnp.int32) for shape in ((groups, 1, reps * share + 2 * BLOCK), (groups, 1, reps * share), (groups, LANES), (groups, 1, neg.shape[1]))),
                   jax.ShapeDtypeStruct((chunks, wire_rows(CHUNK), LANES), BF16), jax.ShapeDtypeStruct((rows, LANES), F32), jax.ShapeDtypeStruct((REL_PAD, 4 * LANES), F32)),
        in_specs=[*[vmem] * 5, hbm, vmem],
        out_specs=(vmem,) * 7,
        scratch_shapes=[pltpu.VMEM(head.shape, jnp.int32), pltpu.VMEM((reps, *head.shape), jnp.int32), pltpu.VMEM((groups, 1, neg.shape[1]), jnp.int32),
                        pltpu.VMEM((AHEAD + 2, width, CHUNK), F32), pltpu.VMEM((rows, LANES), F32), *[dma_sems(4)] * 2, *[dma_sems(2)] * 2, dma_sems(AHEAD + 2), *[dma_sems(4)] * 2],
        compiler_params=pltpu.CompilerParams(collective_id=20, has_side_effects=True),
        name='setup',
    )(head, tail, rel_ids, mask, neg, ent, rel)


def finish_kernel(wire_ref, rel_ref, ent_out, state_out, rel_out):
    chunk = CHUNK
    for n in range(wire_ref.shape[0]):
        tiles = [wire_ref[n, band(t, chunk), :] for t in TILES[:-1]]
        tiles.append(below(unfold_last(wire_ref[n, 3 * chunk:wire_rows(chunk), :])))
        ent_out[:, band(n, chunk)] = tiles_to_columns(tiles)
        state = below([part[:, :1] for part in unfold_last(wire_ref[n, wire_rows(chunk):, :])])
        state_out[:, band(n, chunk)] = column_sum(jnp.where(on_diagonal(chunk), state, 0.0))

    @pl.when(pl.program_id(0) == 0)
    def _():
        rel_out[...] = tiles_to_columns(tiles_of(rel_ref[...]))


def finish_call(wire, rel, width):
    chunks = wire.shape[0]
    size = chunks // 8
    whole = lambda n: (0, 0)
    return pl.pallas_call(
        finish_kernel,
        out_shape=tuple(jax.ShapeDtypeStruct(shape, F32) for shape in ((width, chunks * CHUNK), (1, chunks * CHUNK), (width, REL_PAD))),
        grid=(chunks // size,),
        in_specs=[pl.BlockSpec((size, *wire.shape[1:]), lambda n: (n, 0, 0)), pl.BlockSpec(rel.shape, whole)],
        out_specs=(pl.BlockSpec((width, size * CHUNK), lambda n: (0, n)), pl.BlockSpec((1, size * CHUNK), lambda n: (0, n)), pl.BlockSpec((width, REL_PAD), whole)),
        name='finish',
    )(wire, rel)


def solution(mesh):
    groups = mesh.shape['ent']
    data_reps = mesh.shape['data']
    row_spec = P(('sweep', 'ent'), None)
    edge_spec = P(('sweep', 'ent'), None, 'data')

    def device_fn(ent_table, ent_state, rel_table, head_idx, tail_idx, rel_idx, edge_mask, neg_idx):
        part_rows, emb_width = ent_table.shape
        rel_rows = rel_table.shape[0]
        bucket_edges = head_idx.shape[2] * data_reps
        shard = part_rows // 4
        tail_bits = (part_rows - 1).bit_length()
        head_bits = (shard - 1).bit_length()
        spare = 2**(REL_PAD - 1).bit_length() - 1
        ent = lax.axis_index('ent')
        _, _, core, top, bot = where_here()

        words, rel_ids, counts, neg, table, ent_now, rel_now = setup_call(
            (head_bits, tail_bits, spare), head_idx[0], tail_idx[0], rel_idx[0], edge_mask[0], neg_idx[0], data_reps,
            ent_table.T, jnp.pad(rel_table.T, ((0, 0), (0, REL_PAD - rel_rows))))
        to_core = lambda c: lax.dynamic_slice_in_dim(ent_state, (2 * bot + c) * shard, shard)
        away = [(d * groups + 2 * (n // 2) + d // 2, d * groups + 2 * (n // 2) + 1 - d // 2) for d in range(data_reps) for n in range(0, groups, 2)]
        state_now = jnp.where(core == top, to_core(core), lax.ppermute(to_core(1 - core), ('data', 'ent'), away))[:, None]
        rel_state = jnp.zeros((REL_PAD, 1), F32)
        losses = []
        for step in range(groups):
            tail, head, rel_grad = bucket_call(step, tail_bits + 2, words, counts, neg, rel_ids, ent_now, rel_now, table)
            out = exchange_call(step, groups, emb_width, tail, head, rel_grad, ent_now, state_now, rel_now, rel_state)
            if step + 1 < groups:
                ent_now, state_now, rel_now, rel_state, loss, table = out
            else:
                wire, rel_now, loss = out
            losses.append(loss)
        ent_out, state_out, rel_out = finish_call(wire, rel_now, emb_width)
        loss_rows = below(losses) / bucket_edges
        bucket_loss = lax.dynamic_slice_in_dim(loss_rows, ent, 1, axis=1).reshape(1, groups)
        return ent_out.T, state_out[0], rel_out[:, :rel_rows].T, bucket_loss

    return jax.shard_map(device_fn, mesh=mesh, in_specs=(row_spec, P(('sweep', 'ent')), P('sweep', None), edge_spec, edge_spec, edge_spec, edge_spec, P(('sweep', 'ent'), None, None)), out_specs=(row_spec, P(('sweep', 'ent')), P('sweep', None), row_spec), check_vma=False)
```

```python
import functools

import jax
import jax.numpy as jnp
from jax import lax
from jax.experimental import pallas as pl
from jax.experimental.pallas import tpu as pltpu
from jax.sharding import PartitionSpec as P

LR_SCALE = 0.2
EPSILON = 1e-8
LANES = 128
HALF = 64
LEFT = 8
BLOCK = 256
CHUNK = 128
UNROLL = 64
ROLLED = 32
TOGETHER = 8
AHEAD = 6
LAGS = (0, 3, 6, 9)
FAR_LAGS = (0, 5, 7, 9)
PARTS = 4
REL_HOPS = 6
STRIP = 32
REL_PAD = 128
TILES = range(4)
CORES = range(2)
ROW_COL, ROW_ROW, COL_COL = (((1,), (0,)), ((1,), (1,)), ((0,), (0,)))
F32 = jnp.float32
BF16 = jnp.bfloat16
VMEM_LIMIT = 60 * 2**20


def roll(x, by):
    return pltpu.roll(x, by, 1)


def beside(parts):
    return jnp.concatenate(parts, axis=1)


def below(parts):
    return jnp.concatenate(parts, axis=0)


def lanes(shape):
    return lax.broadcasted_iota(jnp.int32, shape, 1)


def sublanes(shape):
    return lax.broadcasted_iota(jnp.int32, shape, 0)


def one_where(mask):
    return jnp.where(mask, 1.0, 0.0)


def on_diagonal(size):
    return sublanes((size, size)) == lanes((size, size))


def row_sum(x):
    return jnp.sum(x, axis=1, keepdims=True)


def column_sum(x):
    return jnp.sum(x, axis=0, keepdims=True)


def wire_rows(rows):
    return 3 * rows + rows // LEFT


def flipped(tiles):
    rows, columns = tiles[0].shape
    unit = one_where(on_diagonal(columns)).astype(BF16)
    high, mid, low = (dot(unit, piece, ROW_ROW) for piece in in_three(below(tiles)))
    both = high + mid + low
    return [both[:, band(t, rows)] for t in TILES]


def columns_to_tiles(x):
    half = x.shape[0] // 2
    a, c, d = slice(0, LANES), slice(LANES, LANES + HALF), slice(LANES + HALF, half)
    re, im = x[:half], x[half:]
    zero = jnp.zeros((HALF - LEFT, x.shape[1]), x.dtype)
    return flipped([re[a], im[a], below([re[c], im[c]]), below([re[d], zero, im[d], zero])])


def tiles_to_columns(tiles):
    a, b, c, d = flipped(tiles)
    high = slice(HALF, HALF + LEFT)
    return below([a, c[:HALF], d[:LEFT], b, c[HALF:], d[high]])


def each_row(count, body):
    for u in range(count):
        body(u)


def band(n, size):
    return slice(n * size, (n + 1) * size)


def where_here():
    y, ent = lax.axis_index('data'), lax.axis_index('ent')
    return y, ent // 2, ent % 2, y // 2, y % 2


def fold_last(tile):
    n = tile.shape[0] // LEFT
    out = tile[:n]
    for k in range(1, LEFT):
        out = out + roll(tile[band(k, n)], LEFT * k)
    return out


def unfold_last(packed):
    keep = lanes(packed.shape) % HALF < LEFT
    return [jnp.where(keep, packed if k == 0 else roll(packed, LANES - LEFT * k), 0.0) for k in range(LEFT)]


def tiles_of(x):
    return [x[:, band(t, LANES)] for t in TILES]


def times(x, y):
    out = [x[0] * y[0] - x[1] * y[1], x[0] * y[1] + x[1] * y[0]]
    for a, b in zip(x[2:], y[2:]):
        low = lanes(a.shape) < HALF
        a_swap, b_swap = roll(a, HALF), roll(b, HALF)
        out.append(jnp.where(low, a * b - a_swap * b_swap, a_swap * b + a * b_swap))
    return out


def times_conj(x, y):
    out = [x[0] * y[0] + x[1] * y[1], x[1] * y[0] - x[0] * y[1]]
    for a, b in zip(x[2:], y[2:]):
        low = lanes(a.shape) < HALF
        a_swap, b_swap = roll(a, HALF), roll(b, HALF)
        out.append(jnp.where(low, a * b + a_swap * b_swap, a * b_swap - a_swap * b))
    return out


def tiles_at(ref, row, rows):
    block = ref[pl.ds(row * 4, rows * 4), :].reshape(rows // 8, 32, LANES)
    return [block[:, 8 * t:8 * t + 8].reshape(rows, LANES) for t in TILES]


def stack_tiles(tiles):
    rows = tiles[0].shape[0]
    return beside([t.reshape(rows // 8, 8, LANES) for t in tiles]).reshape(rows * 4, LANES)


def row_at(address):
    return pl.ds(address, 4, stride=8)


def row_address(row):
    return (row >> 3 << 5) | (row & 7)


def in_three(x):
    pieces = []
    for _ in range(3):
        piece = x.astype(BF16)
        pieces.append(piece)
        x = x - piece.astype(F32)
    return pieces


def dot(x, y, dims):
    return lax.dot_general(x, y, (dims, ((), ())), preferred_element_type=F32)


def bucket_kernel(cfg, edges_hbm, count_ref, negs_hbm, rel_ids_hbm, ent_hbm, rel_ref, table_hbm, tail_hbm, head_hbm, rel_out,
                  tail_rows, head_next, tail_next, head_buf, tail_buf, gh_last, gt_last, rel_buf, query_buf, pos_buf, score_buf, d_neg_buf, grad_buf, piece_buf,
                  neg_rows, neg_grad, rel_three, tail_acc0, tail_acc1, head_acc0, head_acc1, rel_acc, loss_acc,
                  edge_ref, neg_ref, rel_id_ref, ent_ref, table_ref, tail_out, head_out, sems, table_sems, tail_sems):
    step, tail_bits = cfg
    chunk = CHUNK
    part = chunk // LEFT
    tail_acc, head_acc = (tail_acc0, tail_acc1), (head_acc0, head_acc1)
    count = count_ref[step, 0]
    negs = neg_ref.shape[0]
    loads = [
        pltpu.make_async_copy(negs_hbm.at[step, 0], neg_ref, sems.at[0]),
        pltpu.make_async_copy(rel_ids_hbm.at[step], rel_id_ref, sems.at[2]),
        pltpu.make_async_copy(ent_hbm, ent_ref, sems.at[3]),
    ]
    parts = table_sems.shape[0]
    size = table_ref.shape[0] // parts
    tables = [pltpu.make_async_copy(table_hbm.at[band(n, size)], table_ref.at[band(n, size)], table_sems.at[n]) for n in range(parts)]
    blocks = pl.cdiv(count, BLOCK)

    def edge_pieces(act):
        def one(n, carry):
            span = pl.ds(pl.multiple_of(n * 2 * BLOCK, 2 * BLOCK), 2 * BLOCK)
            act(pltpu.make_async_copy(edges_hbm.at[step, 0, span], edge_ref.at[span], sems.at[1]))
            return carry

        lax.fori_loop(0, (blocks + 3) // 2, one, 0)

    edge_pieces(lambda copy: copy.start())
    for load in loads + tables:
        load.start()

    def head_of(e):
        return row_at(e >> tail_bits)

    def tail_of(e):
        return row_at(e & (2**tail_bits - 1))

    def clear(accs, n, carry):
        for acc in accs:
            acc[pl.ds(pl.multiple_of(n * chunk * 4, chunk * 4), chunk * 4), :] = jnp.zeros((chunk * 4, LANES), F32)
        return carry

    lax.fori_loop(0, table_ref.shape[0], functools.partial(clear, tail_acc), 0)
    lax.fori_loop(0, head_out.shape[0], functools.partial(clear, head_acc), 0)
    neg_grad[...] = jnp.zeros_like(neg_grad)
    gh_last[...] = jnp.zeros_like(gh_last)
    gt_last[...] = jnp.zeros_like(gt_last)
    rel_acc[...] = jnp.zeros_like(rel_acc)
    loss_acc[...] = jnp.zeros_like(loss_acc)
    for n, piece in enumerate(in_three(rel_ref[...])):
        rel_three[band(n, REL_PAD), :] = piece
    for load in loads:
        load.wait()
    edge_pieces(lambda copy: copy.wait())

    def widen(i, carry):
        for n in (i * TOGETHER + k for k in range(TOGETHER)):
            tiles = [table_ref[n, band(t, chunk), :].astype(F32) for t in TILES[:-1]]
            tiles.append(below(unfold_last(table_ref[n, 3 * chunk:, :].astype(F32))))
            tail_rows[pl.ds(pl.multiple_of(n * chunk * 4, chunk * 4), chunk * 4), :] = stack_tiles(tiles)
        return carry

    for n, load in enumerate(tables):
        load.wait()
        lax.fori_loop(n * size // TOGETHER, (n + 1) * size // TOGETHER, widen, 0)

    def take_negs(n, carry):
        base = pl.multiple_of(n * UNROLL, UNROLL)

        def take(u):
            head_buf[row_at(row_address(u)), :] = tail_rows[row_at(neg_ref[base + u]), :]

        each_row(UNROLL, take)
        for t, tile in enumerate(tiles_at(head_buf, 0, UNROLL)):
            neg_rows[pl.ds(base, UNROLL), band(t, LANES)] = tile.astype(BF16)
        return carry

    lax.fori_loop(0, negs // UNROLL, take_negs, 0)

    def take_edges(base, row=0):
        def take(u):
            e = edge_ref[base + u]
            place = row_at(row * 4 + row_address(u))
            head_next[place, :] = ent_ref[head_of(e), :]
            tail_next[place, :] = tail_rows[tail_of(e), :]

        return take

    def put_edges(base, row=0):
        def put(pair):
            for lane in range(2):
                u = 2 * pair + lane
                e = edge_ref[base + u]
                place = row_at(row * 4 + row_address(u))
                head_acc[lane][head_of(e), :] += gh_last[place, :]
                tail_acc[lane][tail_of(e), :] += gt_last[place, :]

        return put


    def take_first(n, carry):
        row = pl.multiple_of(n * ROLLED, ROLLED)
        each_row(ROLLED, take_edges(BLOCK + row, row))
        return carry

    lax.fori_loop(0, BLOCK // ROLLED, take_first, 0)
    spans = [slice(r, r + STRIP) for r in range(0, BLOCK, STRIP)]

    def block(n, carry):
        base = pl.multiple_of(n * BLOCK, BLOCK)
        hot = sublanes((REL_PAD, BLOCK)) == rel_id_ref[:, pl.ds(base, BLOCK)]
        hot = one_where(hot).astype(BF16)
        rel_buf[...] = dot(below([hot] * 3), rel_three[...], COL_COL)
        for span in spans:
            head, tail, rel = tiles_at(head_next, span.start, STRIP), tiles_at(tail_next, span.start, STRIP), tiles_of(rel_buf[span, :])
            wide = slice(4 * span.start, 4 * span.stop)
            head_buf[wide, :], tail_buf[wide, :] = stack_tiles(head), stack_tiles(tail)
            total = None
            for t, q in enumerate(times(head, rel)):
                q = q.astype(BF16)
                query_buf[span, band(t, LANES)] = q
                product = q.astype(F32) * tail[t]
                total = product if total is None else total + product
            pos_buf[span, :] = row_sum(total)
        each_row(BLOCK, take_edges(base + 2 * BLOCK))
        each_row(BLOCK // 2, put_edges(base))
        score_buf[...] = dot(query_buf[...], neg_rows[...], ROW_ROW)
        for span in spans:
            weight = one_where(sublanes((STRIP, 1)) + (base + span.start) < count)
            score, pos = score_buf[span, :], pos_buf[span, :]
            top = jnp.maximum(jnp.max(score, axis=1, keepdims=True), pos)
            pos_exp = jnp.exp(pos - top)
            neg_exp = jnp.exp(score - top)
            total = pos_exp + row_sum(neg_exp)
            loss_acc[...] += column_sum(weight * (top + jnp.log(total) - pos))
            pos_buf[span, :] = weight * (pos_exp / total - 1.0)
            d_neg_buf[span, :] = ((weight / total) * neg_exp).astype(BF16)
        grad_buf[...] = dot(d_neg_buf[...], neg_rows[...], ROW_COL)
        neg_grad[...] += dot(d_neg_buf[...], query_buf[...], COL_COL)
        for span in spans:
            wide = slice(4 * span.start, 4 * span.stop)
            d_pos = pos_buf[span, :]
            tail, rel = tiles_at(tail_buf, span.start, STRIP), tiles_of(rel_buf[span, :])
            grad_q = [d_pos * x + y for x, y in zip(tail, tiles_of(grad_buf[span, :]))]
            gt_last[wide, :] = stack_tiles([d_pos * q.astype(F32) for q in tiles_of(query_buf[span, :])])
            gh_last[wide, :] = stack_tiles(times_conj(grad_q, rel))
            for t, grad in enumerate(times_conj(grad_q, tiles_at(head_buf, span.start, STRIP))):
                for k, piece in enumerate(in_three(grad)):
                    piece_buf[k * BLOCK + span.start:k * BLOCK + span.stop, band(t, LANES)] = piece
        rel_acc[...] += dot(beside([hot] * 3), piece_buf[...], ROW_COL)
        return carry

    lax.fori_loop(0, blocks, block, 0)

    def put_last(n, carry):
        row = pl.multiple_of(n * ROLLED, ROLLED)
        each_row(ROLLED // 2, put_edges(blocks * BLOCK + row, row))
        return carry

    lax.fori_loop(0, BLOCK // ROLLED, put_last, 0)

    def put_negs(n, carry):
        base = pl.multiple_of(n * UNROLL, UNROLL)
        gt_last[:4 * UNROLL, :] = stack_tiles(tiles_of(neg_grad[pl.ds(base, UNROLL), :]))

        def put(pair):
            for lane in range(2):
                u = 2 * pair + lane
                tail_acc[lane][row_at(neg_ref[base + u]), :] += gt_last[row_at(row_address(u)), :]

        each_row(UNROLL // 2, put)
        return carry

    lax.fori_loop(0, negs // UNROLL, put_negs, 0)

    def emit(out_ref, acc, i, carry):
        for n in (i * TOGETHER + k for k in range(TOGETHER)):
            base = pl.multiple_of(n * chunk, chunk)
            tiles = [a + b for a, b in zip(tiles_at(acc[0], base, chunk), tiles_at(acc[1], base, chunk))]
            for t in TILES[:-1]:
                out_ref[n, band(t, chunk), :] = tiles[t]
            out_ref[n, 3 * chunk:, :] = fold_last(tiles[3])
        return carry

    stores = []
    for n in range(tail_sems.shape[0]):
        out, dst, acc, span = (head_out, head_hbm, head_acc, range(head_out.shape[0])) if n == parts else (tail_out, tail_hbm, tail_acc, range(n * size, (n + 1) * size))
        lax.fori_loop(span.start // TOGETHER, span.stop // TOGETHER, functools.partial(emit, out, acc), 0)
        part_of = pl.ds(span.start, len(span))
        stores.append(pltpu.make_async_copy(out.at[part_of], dst.at[part_of], tail_sems.at[n]))
        stores[-1].start()
    _, x, _, top, _ = where_here()
    group = 2 * x + top
    row = sublanes((REL_PAD, LANES))
    lane = lanes((REL_PAD, LANES))
    loss = jnp.where(lane == group, loss_acc[...], 0.0)
    for t in TILES[:-1]:
        rows = rel_acc[:, band(t, LANES)]
        rel_out[band(t, REL_PAD), :] = jnp.where(row == REL_PAD - 1, loss, rows) if t == 0 else rows
    rel_out[3 * REL_PAD:, :] = fold_last(rel_acc[:, 3 * LANES:])
    for store in stores:
        store.wait()


def dma_sems(n):
    return pltpu.SemaphoreType.DMA((n,))


def bucket_call(step, tail_bits, edges, counts, negs, rel_ids, ent, rel, table):
    smem, vmem, hbm = (pl.BlockSpec(memory_space=m) for m in (pltpu.SMEM, pltpu.VMEM, pl.ANY))
    rows, neg_count, chunks = ent.shape[0] // 4, negs.shape[-1], table.shape[0]
    width = 4 * LANES
    wire = wire_rows(CHUNK)
    block = pltpu.VMEM((BLOCK * 4, LANES), F32)
    table_rows = pltpu.VMEM((chunks * CHUNK * 4, LANES), F32)
    head_rows = pltpu.VMEM((rows * 4, LANES), F32)
    return pl.pallas_call(
        functools.partial(bucket_kernel, (step, tail_bits)),
        out_shape=(
            jax.ShapeDtypeStruct((chunks, wire, LANES), F32),
            jax.ShapeDtypeStruct((rows // CHUNK, wire, LANES), F32),
            jax.ShapeDtypeStruct((wire_rows(REL_PAD), LANES), F32),
        ),
        in_specs=[hbm, smem, hbm, hbm, hbm, vmem, hbm],
        out_specs=(hbm, hbm, vmem),
        scratch_shapes=[
            table_rows, *[block] * 6, pltpu.VMEM((BLOCK, width), F32), pltpu.VMEM((BLOCK, width), BF16), pltpu.VMEM((BLOCK, 1), F32),
            pltpu.VMEM((BLOCK, neg_count), F32), pltpu.VMEM((BLOCK, neg_count), BF16), pltpu.VMEM((BLOCK, width), F32), pltpu.VMEM((3 * BLOCK, width), BF16),
            pltpu.VMEM((neg_count, width), BF16), pltpu.VMEM((neg_count, width), F32), pltpu.VMEM((3 * REL_PAD, width), BF16),
            table_rows, table_rows, head_rows, head_rows,
            pltpu.VMEM((REL_PAD, width), F32), pltpu.VMEM((1, 1), F32),
            pltpu.SMEM((edges.shape[-1],), jnp.int32), pltpu.SMEM((neg_count,), jnp.int32), pltpu.VMEM(rel_ids.shape[1:], jnp.int32),
            pltpu.VMEM(ent.shape, F32), pltpu.VMEM(table.shape, BF16), pltpu.VMEM((chunks, wire, LANES), F32), pltpu.VMEM((rows // CHUNK, wire, LANES), F32),
            dma_sems(4), dma_sems(PARTS), dma_sems(PARTS + 1),
        ],
        compiler_params=pltpu.CompilerParams(vmem_limit_bytes=VMEM_LIMIT),
        name='bucket',
    )(edges, counts, negs, rel_ids, ent, rel, table)


def entry(peers):
    barrier = pltpu.get_barrier_semaphore()
    for peer in peers:
        pl.semaphore_signal(barrier, inc=1, device_id=peer, device_id_type=pl.DeviceIdType.MESH)
    pl.semaphore_wait(barrier, len(peers))


def remote(src, dst, send, recv, peer):
    return pltpu.make_async_remote_copy(src_ref=src, dst_ref=dst, send_sem=send, recv_sem=recv, device_id=peer, device_id_type=pl.DeviceIdType.MESH)


def adagrad(rows, state, grad, mean_of, learn_rate):
    square = sum(g * g for g in grad)
    state = state + row_sum(square) / mean_of
    root = jnp.sqrt(state + EPSILON)
    return [r - learn_rate * (g / root) for r, g in zip(rows, grad)], state


def exchange_kernel(cfg, tail_ref, head_hbm, rel_grad_ref, ent_hbm, state_ref, rel_ref, rel_state_ref, *refs):
    step, groups, chunks, emb_width, last = cfg
    if last:
        ent_wire, rel_out, loss_out, *refs = refs
    else:
        ent_out, state_out, rel_out, rel_state_out, loss_out, table_hbm, *refs, table, store_sem = refs
    (own, from_core, from_y, from_group, rel_sum, rel_from, send_buf,
     own_sem, core_send, core_recv, y_send, y_recv, group_send, group_recv, rel_send, rel_recv, out_send, out_recv, head_ref, ent_ref, row_sem) = refs
    learn_rate = LR_SCALE * emb_width ** -0.25
    chunk = CHUNK
    y, x, core, top, bot = where_here()
    mine = 2 * x + top
    x_size = groups // 2

    def place(group, low, c):
        return {'data': 2 * (group % 2) + low, 'ent': 2 * (group // 2) + c}

    def at(dy, dx, c):
        return {'data': dy, 'ent': 2 * dx + c}

    def slot_of(low, c, k):
        return (low * 2 + c) * chunks + k

    def turned(shift):
        return (bot + shift) % 2

    other_core = at(y, x, 1 - core)
    other_y = at(2 * top + 1 - bot, x, core)
    rel_peers = (other_core, other_y, at(3 - y, x, core), at(y, x + 1 - 2 * (x % 2), core), at(y, x_size - 1 - x, core), other_core)
    grad_to = place((mine + step) % groups, turned(step), core)
    grad_from = place((mine + groups - step) % groups, turned(step), core)
    nxt = step + 1
    table_to = place((mine + groups - nxt) % groups, turned(nxt), core)
    table_from = place((mine + nxt) % groups, turned(nxt), core)
    peers = list(rel_peers)
    if step:
        peers += [grad_to, grad_from]
    if last:
        for turn in range(4):
            peers.append(at((y + turn) % 4, x, top))
        senders = [at((2 * core + d), x, c) for d in range(2) for c in range(2)]
        peers += senders
    else:
        peers += [table_to, table_from]
    entry(peers)
    keep = turned(step)
    pending = []

    def start(copy):
        copy.start()
        pending.append(copy)
        return copy

    shards = [(1 - keep, k) for k in range(chunks)] + [(keep, k) for k in range(chunks)]
    loads, cores = [], []
    row_loads = [pltpu.make_async_copy(src, dst, row_sem.at[n]) for n, (src, dst) in enumerate(((head_hbm, head_ref), (ent_hbm, ent_ref)))]
    for load in row_loads:
        load.start()
    stores = []

    def store(n, src, dst):
        copy = pltpu.make_async_copy(src, dst, store_sem.at[n])
        copy.start()
        stores.append(copy)

    def store_table(low, c, k):
        slot = slot_of(low, c, k)
        store(slot, table.at[slot], table_hbm.at[slot])

    rel_copies = [start(remote(rel_grad_ref.at[1 - core], rel_from.at[0], rel_send.at[0], rel_recv.at[0], rel_peers[0]))]
    for n, (low, k) in enumerate(shards):
        cores.append(start(remote(tail_ref.at[slot_of(low, 1 - core, k)], from_core.at[n], core_send.at[n], core_recv.at[n], other_core)))
        load = pltpu.make_async_copy(tail_ref.at[slot_of(low, core, k)], own.at[n], own_sem.at[n])
        load.start()
        loads.append(load)

    def rel_step(n):
        rel_copies[n].wait_recv()
        rel_sum[n] = (rel_grad_ref[core] if n == 0 else rel_sum[n - 1]) + rel_from[n]
        rel_copies.append(start(remote(rel_sum.at[n], rel_from.at[n + 1], rel_send.at[n + 1], rel_recv.at[n + 1], rel_peers[n + 1])))

    ys = []
    for k in range(chunks):
        loads[k].wait()
        cores[k].wait_recv()
        own[k] = own[k] + from_core[k]
        ys.append(start(remote(own.at[k], from_y.at[k], y_send.at[k], y_recv.at[k], other_y)))
        if k == 1:
            rel_step(0)
    for k in range(chunks, 2 * chunks):
        loads[k].wait()
        cores[k].wait_recv()
        own[k] = own[k] + from_core[k]
    gs, outs, forwards, crosses = [], [], [], []

    def stage_group(k):
        ys[k].wait_recv()
        own[chunks + k] = own[chunks + k] + from_y[k]
        if step:
            gs.append(start(remote(own.at[chunks + k], from_group.at[k], group_send.at[k], group_recv.at[k], grad_to)))

    def cross_copy(k):
        slot = slot_of(bot, core, k)
        return remote(send_buf.at[k], ent_wire.at[slot], out_send.at[2 * chunks + k], out_recv.at[slot], other_core)

    turn = (y + 4 - 2 * core) % 4
    near = 1 - turn % 2
    back = jnp.where((turn == 1) | (turn == 2), 0, 1)
    onward = at((y + 1 + 2 * back) % 4, x, core)

    def landed(low, c, k):
        slot = slot_of(low, c, k)
        remote(ent_wire.at[slot], ent_wire.at[slot], out_send.at[0], out_recv.at[slot], other_core).wait_recv()

    def stage_relay(k):
        if k % 2 == 0:
            return
        for c in CORES:
            landed(near, c, k - 1)
            landed(near, c, k)
            slot = slot_of(near, c, k) - 1 + back
            start(remote(ent_wire.at[slot], ent_wire.at[slot], out_send.at[(3 + c) * chunks + k], out_recv.at[slot], onward))

    def stage_update(k):
        if k == 0:
            for load in row_loads:
                load.wait()
        if step:
            gs[k].wait_recv()
        total = from_group if step else own
        base = k if step else chunks + k
        grad = [total[base, band(t, chunk), :] + head_ref[k, band(t, chunk), :] for t in TILES[:-1]]
        grad.append(below(unfold_last(total[base, 3 * chunk:, :] + head_ref[k, 3 * chunk:, :])))
        span = band(k, chunk)
        rows, state = adagrad(tiles_at(ent_ref, k * chunk, chunk), state_ref[span, :], grad, emb_width, learn_rate)
        wire = rows[:3] + [fold_last(rows[3])]
        if last:
            lane = lanes((chunk, LANES))
            wire.append(fold_last(jnp.where(lane < 1, state, 0.0)))
        else:
            wide = band(k, 4 * chunk)
            ent_ref[wide, :] = stack_tiles(rows)
            store(4 * chunks + k, ent_ref.at[wide], ent_out.at[wide])
            state_out[span, :] = state
        offset = 0
        for piece in wire:
            send_buf[k, offset:offset + piece.shape[0], :] = piece.astype(send_buf.dtype)
            offset += piece.shape[0]
        slot = slot_of(bot, core, k)
        if last:
            for n, turn in enumerate((1, 3)):
                start(remote(send_buf.at[k], ent_wire.at[slot], out_send.at[n * chunks + k], out_recv.at[slot], at((y + turn) % 4, x, top)))

            @pl.when(core == top)
            def _():
                pltpu.make_async_copy(send_buf.at[k], ent_wire.at[slot], out_recv.at[slot]).start()

            @pl.when(core != top)
            def _():
                cross_copy(k).start()
        else:
            outs.append(start(remote(send_buf.at[k], table.at[slot], out_send.at[k], out_recv.at[k], table_to)))

    def forward(n, low, k, peer):
        slot = slot_of(low, core, k)
        return start(remote(table.at[slot], table.at[slot], out_send.at[n * chunks + k], out_recv.at[n * chunks + k], peer))

    def stage_forward(k):
        outs[k].wait_recv()
        store_table(turned(nxt), core, k)
        forwards.append(forward(1, turned(nxt), k, other_y))
        crosses.append((forward(2, turned(nxt), k, other_core), turned(nxt), k))

    def stage_cross(k):
        forwards[k].wait_recv()
        store_table(1 - turned(nxt), core, k)
        crosses.append((forward(3, 1 - turned(nxt), k, other_core), 1 - turned(nxt), k))

    stages = (stage_group, stage_update, stage_relay) if last else (stage_group, stage_update, stage_forward, stage_cross)
    rel_steps = len(rel_peers) - 1
    far = groups <= 4 * step < 3 * groups
    lags = FAR_LAGS if far else LAGS
    for tick in range(chunks + lags[len(stages) - 1]):
        for lag, stage in zip(lags, stages):
            if 0 <= tick - lag < chunks:
                stage(tick - lag)
        if tick % 2 == 1 and tick < 2 * rel_steps - 1:
            rel_step(tick // 2 + 1)

    rel_copies[rel_steps].wait_recv()
    halves = rel_sum[rel_steps - 1], rel_from[rel_steps]
    summed = below([jnp.where(core == n, halves[0], halves[1]) for n in CORES])
    rel_grad = [summed[band(t, REL_PAD)] for t in TILES[:-1]] + [below(unfold_last(summed[3 * REL_PAD:]))]
    loss_out[...] = rel_grad[0][REL_PAD - 1:, :]
    row = sublanes((REL_PAD, LANES))
    rel_grad[0] = jnp.where(row < REL_PAD - 1, rel_grad[0], 0.0)
    rel_rows, rel_state = adagrad(tiles_of(rel_ref[...]), rel_state_ref[...], rel_grad, emb_width, learn_rate)
    for t in TILES:
        rel_out[:, band(t, LANES)] = rel_rows[t]
    if not last:
        rel_state_out[...] = rel_state

    if last:
        for c in CORES:
            for k in range(chunks):
                landed(1 - near, c, k)

        @pl.when(core != top)
        def _():
            for k in range(chunks):
                cross_copy(k).wait_send()
    else:
        for copy, low, k in crosses:
            copy.wait_recv()
            store_table(low, 1 - core, k)
        for copy in stores:
            copy.wait()
    for copy in pending:
        copy.wait_send()


def exchange_call(step, groups, emb_width, tail, head, rel_grad, ent, state, rel, rel_state):
    vmem, hbm = pl.BlockSpec(memory_space=pltpu.VMEM), pl.BlockSpec(memory_space=pl.ANY)
    chunks = head.shape[0]
    rel_grad = rel_grad.reshape(2, -1, LANES)
    wire = wire_rows(CHUNK)
    last = step == groups - 1
    like = lambda x: jax.ShapeDtypeStruct(x.shape, x.dtype)
    loss = jax.ShapeDtypeStruct((1, LANES), F32)
    out_wire = wire + (CHUNK // LEFT if last else 0)
    out_type = F32 if last else BF16
    gathered = jax.ShapeDtypeStruct((4 * chunks, out_wire, LANES), out_type)
    out_shape = (gathered, like(rel), loss) if last else (like(ent), like(state), like(rel), like(rel_state), loss, gathered)
    return pl.pallas_call(
        functools.partial(exchange_kernel, (step, groups, chunks, emb_width, last)),
        out_shape=out_shape,
        in_specs=[hbm, hbm, vmem, hbm, vmem, vmem, vmem],
        out_specs=(vmem,) * 3 if last else (hbm, vmem, vmem, vmem, vmem, hbm),
        scratch_shapes=[
            pltpu.VMEM((2 * chunks, wire, LANES), F32), pltpu.VMEM((2 * chunks, wire, LANES), F32),
            pltpu.VMEM((chunks, wire, LANES), F32), pltpu.VMEM((chunks, wire, LANES), F32),
            pltpu.VMEM((REL_HOPS - 1, *rel_grad.shape[1:]), F32), pltpu.VMEM((REL_HOPS, *rel_grad.shape[1:]), F32),
            pltpu.VMEM((chunks, out_wire, LANES), out_type),
            *[dma_sems(2 * chunks)] * 3, *[dma_sems(chunks)] * 4,
            dma_sems(REL_HOPS), dma_sems(REL_HOPS), dma_sems(5 * chunks), dma_sems(4 * chunks),
            pltpu.VMEM(head.shape, F32), pltpu.VMEM(ent.shape, F32), dma_sems(2),
            *(() if last else (pltpu.VMEM(gathered.shape, BF16), dma_sems(5 * chunks))),
        ],
        compiler_params=pltpu.CompilerParams(vmem_limit_bytes=VMEM_LIMIT, collective_id=step, has_side_effects=True),
        name='exchange',
    )(tail, head, rel_grad, ent, state, rel, rel_state)


def setup_kernel(cfg, head_ref, tail_ref, rel_id_ref, mask_ref, neg_ref, ent_hbm, rel_ref, word_out, rel_id_out, count_out, neg_out, table, ent_out, rel_out,
                 packed, shares, neg_buf, rows_buf, away, send_sem, recv_sem, core_send, core_recv, load_sem, table_send, table_recv):
    head_bits, tail_bits, spare = cfg
    y, x, core, top, bot = where_here()
    home = core == top
    own_shard, other_shard = 2 * bot + core, 2 * bot + 1 - core
    other_core = {'data': y, 'ent': 2 * x + 1 - core}
    users = [(c, 2 * core + d) for c in CORES for d in CORES]
    users = [({'data': row, 'ent': 2 * x + c}, (core == c) & (y == row)) for c, row in users]
    entry([peer for peer, _ in users] + [{'data': row, 'ent': 2 * x + top} for row in TILES] + [other_core])
    edges = head_ref[...] | (tail_ref[...] << tail_bits) | (rel_id_ref[...] << (2 * tail_bits))
    packed[...] = jnp.where(mask_ref[...] > 0, edges, spare << (2 * tail_bits))
    neg_buf[:, 0, :] = row_address(neg_ref[...])
    to_users = [remote(packed, shares.at[y], send_sem.at[n], recv_sem.at[y], peer) for n, (peer, _) in enumerate(users)]
    for copy, (_, here) in zip(to_users, users):
        @pl.when(jnp.logical_not(here))
        def _():
            copy.start()

    chunks, chunk = table.shape[0], CHUNK
    shard = chunks // 4

    def load(n):
        return pltpu.make_async_copy(ent_hbm.at[:, pl.ds(pl.multiple_of(n * chunk, chunk), chunk)], rows_buf.at[n % rows_buf.shape[0]], load_sem.at[n % rows_buf.shape[0]])

    def table_copy(q):
        part = table.at[pl.ds(q * shard, shard)]
        return remote(part, part, table_send.at[q], table_recv.at[q], other_core)

    neg_copy = remote(neg_buf, neg_out, core_send.at[0], core_recv.at[0], other_core)
    ent_copy = remote(away, ent_out, core_send.at[1], core_recv.at[1], other_core)

    @pl.when(home)
    def _():
        pltpu.make_async_copy(packed, shares.at[y], recv_sem.at[y]).start()
        neg_copy.start()
        neg_out[...] = neg_buf[...]
        for n in range(AHEAD):
            load(n).start()
        for q in TILES:
            def one(pair, carry):
                first = 2 * pair
                for c in CORES:
                    n = q * shard + first + c

                    @pl.when(n + AHEAD < chunks)
                    def _():
                        load(n + AHEAD).start()

                    load(n).wait()
                both = [(first + c, columns_to_tiles(rows_buf[(q * shard + first + c) % rows_buf.shape[0]])) for c in CORES]
                for k, tiles in both:
                    n = q * shard + k
                    for t in TILES[:-1]:
                        table[n, band(t, chunk), :] = tiles[t].astype(BF16)
                    table[n, 3 * chunk:, :] = fold_last(tiles[3]).astype(BF16)
                    rows = stack_tiles(tiles)
                    place = pl.ds(pl.multiple_of(k * chunk * 4, chunk * 4), chunk * 4)

                    @pl.when(own_shard == q)
                    def _():
                        ent_out[place, :] = rows

                    @pl.when(other_shard == q)
                    def _():
                        away[place, :] = rows

                return carry

            lax.fori_loop(0, shard // 2, one, 0)
            table_copy(q).start()

            @pl.when(other_shard == q)
            def _():
                ent_copy.start()

    for t, tile in enumerate(columns_to_tiles(rel_ref[...])):
        rel_out[:, band(t, LANES)] = tile
    for row in TILES:
        remote(packed, shares.at[row], send_sem.at[0], recv_sem.at[row], other_core).wait_recv()
    share = beside([shares[row] for row in TILES])
    mine = ((share >> head_bits) & 3 == own_shard) & (share >> (2 * tail_bits) != spare)
    lane = lanes(share.shape)
    width = share.shape[1]
    steps = (width - 1).bit_length()
    other = jnp.where(mine, 0, 1)
    before = other
    for bit in range(steps):
        before = before + jnp.where(lane < 2**bit, 0, roll(before, 2**bit))
    count_out[...] = jnp.broadcast_to(width - before[:, width - 1:], count_out.shape)
    none = spare << (head_bits + tail_bits)
    edge = jnp.where(mine, (share & (2**head_bits - 1)) | (share >> tail_bits << head_bits), none)
    shift = jnp.where(mine, before - other, 0)
    for bit in range(steps):
        here = (shift >> bit) & 1 == 1
        edge_in, shift_in = roll(edge, width - 2**bit), roll(shift, width - 2**bit)
        there = (shift_in >> bit) & 1 == 1
        edge = jnp.where(there, edge_in, jnp.where(here, none, edge))
        shift = jnp.where(there, shift_in, jnp.where(here, 0, shift))
    rel_id_out[:, 0, :] = edge >> (head_bits + tail_bits)
    head, tail = edge & (2**head_bits - 1), (edge >> head_bits) & (2**tail_bits - 1)
    margin = jnp.zeros((share.shape[0], BLOCK), jnp.int32)
    word_out[:, 0, :] = beside([margin, (row_address(head) << (tail_bits + 2)) | row_address(tail), margin])
    for copy, (_, here) in zip(to_users, users):
        @pl.when(jnp.logical_not(here))
        def _():
            copy.wait_send()

    between = [neg_copy, ent_copy, *(table_copy(q) for q in TILES)]

    @pl.when(home)
    def _():
        for copy in between:
            copy.wait_send()

    @pl.when(jnp.logical_not(home))
    def _():
        for copy in between:
            copy.wait_recv()


def setup_call(cfg, head, tail, rel_ids, mask, neg, reps, ent, rel):
    vmem, hbm = pl.BlockSpec(memory_space=pltpu.VMEM), pl.BlockSpec(memory_space=pl.ANY)
    groups, share = head.shape
    width, rows = ent.shape
    chunks = rows // CHUNK
    return pl.pallas_call(
        functools.partial(setup_kernel, cfg),
        out_shape=(*(jax.ShapeDtypeStruct(shape, jnp.int32) for shape in ((groups, 1, reps * share + 2 * BLOCK), (groups, 1, reps * share), (groups, LANES), (groups, 1, neg.shape[1]))),
                   jax.ShapeDtypeStruct((chunks, wire_rows(CHUNK), LANES), BF16), jax.ShapeDtypeStruct((rows, LANES), F32), jax.ShapeDtypeStruct((REL_PAD, 4 * LANES), F32)),
        in_specs=[*[vmem] * 5, hbm, vmem],
        out_specs=(vmem,) * 7,
        scratch_shapes=[pltpu.VMEM(head.shape, jnp.int32), pltpu.VMEM((reps, *head.shape), jnp.int32), pltpu.VMEM((groups, 1, neg.shape[1]), jnp.int32),
                        pltpu.VMEM((AHEAD + 2, width, CHUNK), F32), pltpu.VMEM((rows, LANES), F32), *[dma_sems(4)] * 2, *[dma_sems(2)] * 2, dma_sems(AHEAD + 2), *[dma_sems(4)] * 2],
        compiler_params=pltpu.CompilerParams(collective_id=20, has_side_effects=True),
        name='setup',
    )(head, tail, rel_ids, mask, neg, ent, rel)


def finish_kernel(wire_ref, rel_ref, ent_out, state_out, rel_out):
    chunk = CHUNK
    for n in range(wire_ref.shape[0]):
        tiles = [wire_ref[n, band(t, chunk), :] for t in TILES[:-1]]
        tiles.append(below(unfold_last(wire_ref[n, 3 * chunk:wire_rows(chunk), :])))
        ent_out[:, band(n, chunk)] = tiles_to_columns(tiles)
        state = below([part[:, :1] for part in unfold_last(wire_ref[n, wire_rows(chunk):, :])])
        state_out[:, band(n, chunk)] = column_sum(jnp.where(on_diagonal(chunk), state, 0.0))

    @pl.when(pl.program_id(0) == 0)
    def _():
        rel_out[...] = tiles_to_columns(tiles_of(rel_ref[...]))


def finish_call(wire, rel, width):
    chunks = wire.shape[0]
    size = chunks // 8
    whole = lambda n: (0, 0)
    return pl.pallas_call(
        finish_kernel,
        out_shape=tuple(jax.ShapeDtypeStruct(shape, F32) for shape in ((width, chunks * CHUNK), (1, chunks * CHUNK), (width, REL_PAD))),
        grid=(chunks // size,),
        in_specs=[pl.BlockSpec((size, *wire.shape[1:]), lambda n: (n, 0, 0)), pl.BlockSpec(rel.shape, whole)],
        out_specs=(pl.BlockSpec((width, size * CHUNK), lambda n: (0, n)), pl.BlockSpec((1, size * CHUNK), lambda n: (0, n)), pl.BlockSpec((width, REL_PAD), whole)),
        name='finish',
    )(wire, rel)


def solution(mesh):
    groups = mesh.shape['ent']
    data_reps = mesh.shape['data']
    row_spec = P(('sweep', 'ent'), None)
    edge_spec = P(('sweep', 'ent'), None, 'data')

    def device_fn(ent_table, ent_state, rel_table, head_idx, tail_idx, rel_idx, edge_mask, neg_idx):
        part_rows, emb_width = ent_table.shape
        rel_rows = rel_table.shape[0]
        bucket_edges = head_idx.shape[2] * data_reps
        shard = part_rows // 4
        tail_bits = (part_rows - 1).bit_length()
        head_bits = (shard - 1).bit_length()
        spare = 2**(REL_PAD - 1).bit_length() - 1
        ent = lax.axis_index('ent')
        _, _, core, top, bot = where_here()

        words, rel_ids, counts, neg, table, ent_now, rel_now = setup_call(
            (head_bits, tail_bits, spare), head_idx[0], tail_idx[0], rel_idx[0], edge_mask[0], neg_idx[0], data_reps,
            ent_table.T, jnp.pad(rel_table.T, ((0, 0), (0, REL_PAD - rel_rows))))
        to_core = lambda c: lax.dynamic_slice_in_dim(ent_state, (2 * bot + c) * shard, shard)
        away = [(d * groups + 2 * (n // 2) + d // 2, d * groups + 2 * (n // 2) + 1 - d // 2) for d in range(data_reps) for n in range(0, groups, 2)]
        state_now = jnp.where(core == top, to_core(core), lax.ppermute(to_core(1 - core), ('data', 'ent'), away))[:, None]
        rel_state = jnp.zeros((REL_PAD, 1), F32)
        losses = []
        for step in range(groups):
            tail, head, rel_grad = bucket_call(step, tail_bits + 2, words, counts, neg, rel_ids, ent_now, rel_now, table)
            out = exchange_call(step, groups, emb_width, tail, head, rel_grad, ent_now, state_now, rel_now, rel_state)
            if step + 1 < groups:
                ent_now, state_now, rel_now, rel_state, loss, table = out
            else:
                wire, rel_now, loss = out
            losses.append(loss)
        ent_out, state_out, rel_out = finish_call(wire, rel_now, emb_width)
        loss_rows = below(losses) / bucket_edges
        bucket_loss = lax.dynamic_slice_in_dim(loss_rows, ent, 1, axis=1).reshape(1, groups)
        return ent_out.T, state_out[0], rel_out[:, :rel_rows].T, bucket_loss

    return jax.shard_map(device_fn, mesh=mesh, in_specs=(row_spec, P(('sweep', 'ent')), P('sweep', None), edge_spec, edge_spec, edge_spec, edge_spec, P(('sweep', 'ent'), None, None)), out_specs=(row_spec, P(('sweep', 'ent')), P('sweep', None), row_spec), check_vma=False)
```

```python
import functools

import jax
import jax.numpy as jnp
from jax import lax
from jax.experimental import pallas as pl
from jax.experimental.pallas import tpu as pltpu
from jax.sharding import PartitionSpec as P

LR_SCALE = 0.2
EPSILON = 1e-8
LANES = 128
HALF = 64
LEFT = 8
BLOCK = 256
CHUNK = 128
UNROLL = 64
ROLLED = 32
TOGETHER = 8
AHEAD = 6
LAGS = (0, 3, 6, 9)
FAR_LAGS = (0, 5, 7, 9)
PARTS = 4
REL_HOPS = 6
STRIP = 32
REL_PAD = 128
TILES = range(4)
CORES = range(2)
ROW_COL, ROW_ROW, COL_COL = (((1,), (0,)), ((1,), (1,)), ((0,), (0,)))
F32 = jnp.float32
BF16 = jnp.bfloat16
VMEM_LIMIT = 60 * 2**20


def roll(x, by):
    return pltpu.roll(x, by, 1)


def beside(parts):
    return jnp.concatenate(parts, axis=1)


def below(parts):
    return jnp.concatenate(parts, axis=0)


def lanes(shape):
    return lax.broadcasted_iota(jnp.int32, shape, 1)


def sublanes(shape):
    return lax.broadcasted_iota(jnp.int32, shape, 0)


def one_where(mask):
    return jnp.where(mask, 1.0, 0.0)


def on_diagonal(size):
    return sublanes((size, size)) == lanes((size, size))


def row_sum(x):
    return jnp.sum(x, axis=1, keepdims=True)


def column_sum(x):
    return jnp.sum(x, axis=0, keepdims=True)


def wire_rows(rows):
    return 3 * rows + rows // LEFT


def flipped(tiles):
    rows, columns = tiles[0].shape
    unit = one_where(on_diagonal(columns)).astype(BF16)
    high, mid, low = (dot(unit, piece, ROW_ROW) for piece in in_three(below(tiles)))
    both = high + mid + low
    return [both[:, band(t, rows)] for t in TILES]


def columns_to_tiles(x):
    half = x.shape[0] // 2
    a, c, d = slice(0, LANES), slice(LANES, LANES + HALF), slice(LANES + HALF, half)
    re, im = x[:half], x[half:]
    zero = jnp.zeros((HALF - LEFT, x.shape[1]), x.dtype)
    return flipped([re[a], im[a], below([re[c], im[c]]), below([re[d], zero, im[d], zero])])


def tiles_to_columns(tiles):
    a, b, c, d = flipped(tiles)
    high = slice(HALF, HALF + LEFT)
    return below([a, c[:HALF], d[:LEFT], b, c[HALF:], d[high]])


def each_row(count, body):
    for u in range(count):
        body(u)


def band(n, size):
    return slice(n * size, (n + 1) * size)


def where_here():
    y, ent = lax.axis_index('data'), lax.axis_index('ent')
    return y, ent // 2, ent % 2, y // 2, y % 2


def fold_last(tile):
    n = tile.shape[0] // LEFT
    out = tile[:n]
    for k in range(1, LEFT):
        out = out + roll(tile[band(k, n)], LEFT * k)
    return out


def unfold_last(packed):
    keep = lanes(packed.shape) % HALF < LEFT
    return [jnp.where(keep, packed if k == 0 else roll(packed, LANES - LEFT * k), 0.0) for k in range(LEFT)]


def tiles_of(x):
    return [x[:, band(t, LANES)] for t in TILES]


def times(x, y):
    out = [x[0] * y[0] - x[1] * y[1], x[0] * y[1] + x[1] * y[0]]
    for a, b in zip(x[2:], y[2:]):
        low = lanes(a.shape) < HALF
        a_swap, b_swap = roll(a, HALF), roll(b, HALF)
        out.append(jnp.where(low, a * b - a_swap * b_swap, a_swap * b + a * b_swap))
    return out


def times_conj(x, y):
    out = [x[0] * y[0] + x[1] * y[1], x[1] * y[0] - x[0] * y[1]]
    for a, b in zip(x[2:], y[2:]):
        low = lanes(a.shape) < HALF
        a_swap, b_swap = roll(a, HALF), roll(b, HALF)
        out.append(jnp.where(low, a * b + a_swap * b_swap, a * b_swap - a_swap * b))
    return out


def tiles_at(ref, row, rows):
    block = ref[pl.ds(row * 4, rows * 4), :].reshape(rows // 8, 32, LANES)
    return [block[:, 8 * t:8 * t + 8].reshape(rows, LANES) for t in TILES]


def stack_tiles(tiles):
    rows = tiles[0].shape[0]
    return beside([t.reshape(rows // 8, 8, LANES) for t in tiles]).reshape(rows * 4, LANES)


def row_at(address):
    return pl.ds(address, 4, stride=8)


def row_address(row):
    return (row >> 3 << 5) | (row & 7)


def in_three(x):
    pieces = []
    for _ in range(3):
        piece = x.astype(BF16)
        pieces.append(piece)
        x = x - piece.astype(F32)
    return pieces


def dot(x, y, dims):
    return lax.dot_general(x, y, (dims, ((), ())), preferred_element_type=F32)


def bucket_kernel(cfg, edges_hbm, count_ref, negs_hbm, rel_ids_hbm, ent_hbm, rel_ref, table_hbm, tail_hbm, head_hbm, rel_out,
                  tail_rows, head_next, tail_next, head_buf, tail_buf, gh_last, gt_last, rel_buf, query_buf, pos_buf, score_buf, d_neg_buf, grad_buf, piece_buf,
                  neg_rows, neg_grad, rel_three, tail_acc0, tail_acc1, head_acc0, head_acc1, rel_acc, loss_acc,
                  edge_ref, neg_ref, rel_id_ref, ent_ref, table_ref, tail_out, head_out, sems, table_sems, tail_sems):
    step, tail_bits = cfg
    chunk = CHUNK
    part = chunk // LEFT
    tail_acc, head_acc = (tail_acc0, tail_acc1), (head_acc0, head_acc1)
    count = count_ref[step, 0]
    negs = neg_ref.shape[0]
    loads = [
        pltpu.make_async_copy(negs_hbm.at[step, 0], neg_ref, sems.at[0]),
        pltpu.make_async_copy(rel_ids_hbm.at[step], rel_id_ref, sems.at[2]),
        pltpu.make_async_copy(ent_hbm, ent_ref, sems.at[3]),
    ]
    parts = table_sems.shape[0]
    size = table_ref.shape[0] // parts
    tables = [pltpu.make_async_copy(table_hbm.at[band(n, size)], table_ref.at[band(n, size)], table_sems.at[n]) for n in range(parts)]
    blocks = pl.cdiv(count, BLOCK)

    def edge_pieces(act):
        def one(n, carry):
            span = pl.ds(pl.multiple_of(n * 2 * BLOCK, 2 * BLOCK), 2 * BLOCK)
            act(pltpu.make_async_copy(edges_hbm.at[step, 0, span], edge_ref.at[span], sems.at[1]))
            return carry

        lax.fori_loop(0, (blocks + 3) // 2, one, 0)

    edge_pieces(lambda copy: copy.start())
    for load in loads + tables:
        load.start()

    def head_of(e):
        return row_at(e >> tail_bits)

    def tail_of(e):
        return row_at(e & (2**tail_bits - 1))

    def clear(accs, n, carry):
        for acc in accs:
            acc[pl.ds(pl.multiple_of(n * chunk * 4, chunk * 4), chunk * 4), :] = jnp.zeros((chunk * 4, LANES), F32)
        return carry

    lax.fori_loop(0, table_ref.shape[0], functools.partial(clear, tail_acc), 0)
    lax.fori_loop(0, head_out.shape[0], functools.partial(clear, head_acc), 0)
    neg_grad[...] = jnp.zeros_like(neg_grad)
    gh_last[...] = jnp.zeros_like(gh_last)
    gt_last[...] = jnp.zeros_like(gt_last)
    rel_acc[...] = jnp.zeros_like(rel_acc)
    loss_acc[...] = jnp.zeros_like(loss_acc)
    for n, piece in enumerate(in_three(rel_ref[...])):
        rel_three[band(n, REL_PAD), :] = piece
    for load in loads:
        load.wait()
    edge_pieces(lambda copy: copy.wait())

    def widen(i, carry):
        for n in (i * TOGETHER + k for k in range(TOGETHER)):
            tiles = [table_ref[n, band(t, chunk), :].astype(F32) for t in TILES[:-1]]
            tiles.append(below(unfold_last(table_ref[n, 3 * chunk:, :].astype(F32))))
            tail_rows[pl.ds(pl.multiple_of(n * chunk * 4, chunk * 4), chunk * 4), :] = stack_tiles(tiles)
        return carry

    for n, load in enumerate(tables):
        load.wait()
        lax.fori_loop(n * size // TOGETHER, (n + 1) * size // TOGETHER, widen, 0)

    def take_negs(n, carry):
        base = pl.multiple_of(n * UNROLL, UNROLL)

        def take(u):
            head_buf[row_at(row_address(u)), :] = tail_rows[row_at(neg_ref[base + u]), :]

        each_row(UNROLL, take)
        for t, tile in enumerate(tiles_at(head_buf, 0, UNROLL)):
            neg_rows[pl.ds(base, UNROLL), band(t, LANES)] = tile.astype(BF16)
        return carry

    lax.fori_loop(0, negs // UNROLL, take_negs, 0)

    def take_edges(base, row=0):
        def take(u):
            e = edge_ref[base + u]
            place = row_at(row * 4 + row_address(u))
            head_next[place, :] = ent_ref[head_of(e), :]
            tail_next[place, :] = tail_rows[tail_of(e), :]

        return take

    def put_edges(base, row=0):
        def put(pair):
            for lane in range(2):
                u = 2 * pair + lane
                e = edge_ref[base + u]
                place = row_at(row * 4 + row_address(u))
                head_acc[lane][head_of(e), :] += gh_last[place, :]
                tail_acc[lane][tail_of(e), :] += gt_last[place, :]

        return put


    def take_first(n, carry):
        row = pl.multiple_of(n * ROLLED, ROLLED)
        each_row(ROLLED, take_edges(BLOCK + row, row))
        return carry

    lax.fori_loop(0, BLOCK // ROLLED, take_first, 0)
    spans = [slice(r, r + STRIP) for r in range(0, BLOCK, STRIP)]

    def block(n, carry):
        base = pl.multiple_of(n * BLOCK, BLOCK)
        hot = sublanes((REL_PAD, BLOCK)) == rel_id_ref[:, pl.ds(base, BLOCK)]
        hot = one_where(hot).astype(BF16)
        rel_buf[...] = dot(below([hot] * 3), rel_three[...], COL_COL)
        for span in spans:
            head, tail, rel = tiles_at(head_next, span.start, STRIP), tiles_at(tail_next, span.start, STRIP), tiles_of(rel_buf[span, :])
            wide = slice(4 * span.start, 4 * span.stop)
            head_buf[wide, :], tail_buf[wide, :] = stack_tiles(head), stack_tiles(tail)
            total = None
            for t, q in enumerate(times(head, rel)):
                q = q.astype(BF16)
                query_buf[span, band(t, LANES)] = q
                product = q.astype(F32) * tail[t]
                total = product if total is None else total + product
            pos_buf[span, :] = row_sum(total)
        each_row(BLOCK, take_edges(base + 2 * BLOCK))
        each_row(BLOCK // 2, put_edges(base))
        score_buf[...] = dot(query_buf[...], neg_rows[...], ROW_ROW)
        for span in spans:
            weight = one_where(sublanes((STRIP, 1)) + (base + span.start) < count)
            score, pos = score_buf[span, :], pos_buf[span, :]
            top = jnp.maximum(jnp.max(score, axis=1, keepdims=True), pos)
            pos_exp = jnp.exp(pos - top)
            neg_exp = jnp.exp(score - top)
            total = pos_exp + row_sum(neg_exp)
            loss_acc[...] += column_sum(weight * (top + jnp.log(total) - pos))
            pos_buf[span, :] = weight * (pos_exp / total - 1.0)
            d_neg_buf[span, :] = ((weight / total) * neg_exp).astype(BF16)
        grad_buf[...] = dot(d_neg_buf[...], neg_rows[...], ROW_COL)
        neg_grad[...] += dot(d_neg_buf[...], query_buf[...], COL_COL)
        for span in spans:
            wide = slice(4 * span.start, 4 * span.stop)
            d_pos = pos_buf[span, :]
            tail, rel = tiles_at(tail_buf, span.start, STRIP), tiles_of(rel_buf[span, :])
            grad_q = [d_pos * x + y for x, y in zip(tail, tiles_of(grad_buf[span, :]))]
            gt_last[wide, :] = stack_tiles([d_pos * q.astype(F32) for q in tiles_of(query_buf[span, :])])
            gh_last[wide, :] = stack_tiles(times_conj(grad_q, rel))
            for t, grad in enumerate(times_conj(grad_q, tiles_at(head_buf, span.start, STRIP))):
                for k, piece in enumerate(in_three(grad)):
                    piece_buf[k * BLOCK + span.start:k * BLOCK + span.stop, band(t, LANES)] = piece
        rel_acc[...] += dot(beside([hot] * 3), piece_buf[...], ROW_COL)
        return carry

    lax.fori_loop(0, blocks, block, 0)

    def put_last(n, carry):
        row = pl.multiple_of(n * ROLLED, ROLLED)
        each_row(ROLLED // 2, put_edges(blocks * BLOCK + row, row))
        return carry

    lax.fori_loop(0, BLOCK // ROLLED, put_last, 0)

    def put_negs(n, carry):
        base = pl.multiple_of(n * UNROLL, UNROLL)
        gt_last[:4 * UNROLL, :] = stack_tiles(tiles_of(neg_grad[pl.ds(base, UNROLL), :]))

        def put(pair):
            for lane in range(2):
                u = 2 * pair + lane
                tail_acc[lane][row_at(neg_ref[base + u]), :] += gt_last[row_at(row_address(u)), :]

        each_row(UNROLL // 2, put)
        return carry

    lax.fori_loop(0, negs // UNROLL, put_negs, 0)

    def emit(out_ref, acc, i, carry):
        for n in (i * TOGETHER + k for k in range(TOGETHER)):
            base = pl.multiple_of(n * chunk, chunk)
            tiles = [a + b for a, b in zip(tiles_at(acc[0], base, chunk), tiles_at(acc[1], base, chunk))]
            for t in TILES[:-1]:
                out_ref[n, band(t, chunk), :] = tiles[t]
            out_ref[n, 3 * chunk:, :] = fold_last(tiles[3])
        return carry

    stores = []
    for n in range(tail_sems.shape[0]):
        out, dst, acc, span = (head_out, head_hbm, head_acc, range(head_out.shape[0])) if n == parts else (tail_out, tail_hbm, tail_acc, range(n * size, (n + 1) * size))
        lax.fori_loop(span.start // TOGETHER, span.stop // TOGETHER, functools.partial(emit, out, acc), 0)
        part_of = pl.ds(span.start, len(span))
        stores.append(pltpu.make_async_copy(out.at[part_of], dst.at[part_of], tail_sems.at[n]))
        stores[-1].start()
    _, x, _, top, _ = where_here()
    group = 2 * x + top
    row = sublanes((REL_PAD, LANES))
    lane = lanes((REL_PAD, LANES))
    loss = jnp.where(lane == group, loss_acc[...], 0.0)
    for t in TILES[:-1]:
        rows = rel_acc[:, band(t, LANES)]
        rel_out[band(t, REL_PAD), :] = jnp.where(row == REL_PAD - 1, loss, rows) if t == 0 else rows
    rel_out[3 * REL_PAD:, :] = fold_last(rel_acc[:, 3 * LANES:])
    for store in stores:
        store.wait()


def dma_sems(n):
    return pltpu.SemaphoreType.DMA((n,))


def bucket_call(step, tail_bits, edges, counts, negs, rel_ids, ent, rel, table):
    smem, vmem, hbm = (pl.BlockSpec(memory_space=m) for m in (pltpu.SMEM, pltpu.VMEM, pl.ANY))
    rows, neg_count, chunks = ent.shape[0] // 4, negs.shape[-1], table.shape[0]
    width = 4 * LANES
    wire = wire_rows(CHUNK)
    block = pltpu.VMEM((BLOCK * 4, LANES), F32)
    table_rows = pltpu.VMEM((chunks * CHUNK * 4, LANES), F32)
    head_rows = pltpu.VMEM((rows * 4, LANES), F32)
    return pl.pallas_call(
        functools.partial(bucket_kernel, (step, tail_bits)),
        out_shape=(
            jax.ShapeDtypeStruct((chunks, wire, LANES), F32),
            jax.ShapeDtypeStruct((rows // CHUNK, wire, LANES), F32),
            jax.ShapeDtypeStruct((wire_rows(REL_PAD), LANES), F32),
        ),
        in_specs=[hbm, smem, hbm, hbm, hbm, vmem, hbm],
        out_specs=(hbm, hbm, vmem),
        scratch_shapes=[
            table_rows, *[block] * 6, pltpu.VMEM((BLOCK, width), F32), pltpu.VMEM((BLOCK, width), BF16), pltpu.VMEM((BLOCK, 1), F32),
            pltpu.VMEM((BLOCK, neg_count), F32), pltpu.VMEM((BLOCK, neg_count), BF16), pltpu.VMEM((BLOCK, width), F32), pltpu.VMEM((3 * BLOCK, width), BF16),
            pltpu.VMEM((neg_count, width), BF16), pltpu.VMEM((neg_count, width), F32), pltpu.VMEM((3 * REL_PAD, width), BF16),
            table_rows, table_rows, head_rows, head_rows,
            pltpu.VMEM((REL_PAD, width), F32), pltpu.VMEM((1, 1), F32),
            pltpu.SMEM((edges.shape[-1],), jnp.int32), pltpu.SMEM((neg_count,), jnp.int32), pltpu.VMEM(rel_ids.shape[1:], jnp.int32),
            pltpu.VMEM(ent.shape, F32), pltpu.VMEM(table.shape, BF16), pltpu.VMEM((chunks, wire, LANES), F32), pltpu.VMEM((rows // CHUNK, wire, LANES), F32),
            dma_sems(4), dma_sems(PARTS), dma_sems(PARTS + 1),
        ],
        compiler_params=pltpu.CompilerParams(vmem_limit_bytes=VMEM_LIMIT),
        name='bucket',
    )(edges, counts, negs, rel_ids, ent, rel, table)


def entry(peers):
    barrier = pltpu.get_barrier_semaphore()
    for peer in peers:
        pl.semaphore_signal(barrier, inc=1, device_id=peer, device_id_type=pl.DeviceIdType.MESH)
    pl.semaphore_wait(barrier, len(peers))


def remote(src, dst, send, recv, peer):
    return pltpu.make_async_remote_copy(src_ref=src, dst_ref=dst, send_sem=send, recv_sem=recv, device_id=peer, device_id_type=pl.DeviceIdType.MESH)


def adagrad(rows, state, grad, mean_of, learn_rate):
    square = sum(g * g for g in grad)
    state = state + row_sum(square) / mean_of
    root = jnp.sqrt(state + EPSILON)
    return [r - learn_rate * (g / root) for r, g in zip(rows, grad)], state


def exchange_kernel(cfg, tail_ref, head_hbm, rel_grad_ref, ent_hbm, state_ref, rel_ref, rel_state_ref, *refs):
    step, groups, chunks, emb_width, last = cfg
    if last:
        ent_wire, rel_out, loss_out, *refs = refs
    else:
        ent_out, state_out, rel_out, rel_state_out, loss_out, table_hbm, *refs, table, store_sem = refs
    (own, from_core, from_y, from_group, rel_sum, rel_from, send_buf,
     own_sem, core_send, core_recv, y_send, y_recv, group_send, group_recv, rel_send, rel_recv, out_send, out_recv, head_ref, ent_ref, row_sem) = refs
    learn_rate = LR_SCALE * emb_width ** -0.25
    chunk = CHUNK
    y, x, core, top, bot = where_here()
    mine = 2 * x + top
    x_size = groups // 2

    def place(group, low, c):
        return {'data': 2 * (group % 2) + low, 'ent': 2 * (group // 2) + c}

    def at(dy, dx, c):
        return {'data': dy, 'ent': 2 * dx + c}

    def slot_of(low, c, k):
        return (low * 2 + c) * chunks + k

    def turned(shift):
        return (bot + shift) % 2

    other_core = at(y, x, 1 - core)
    other_y = at(2 * top + 1 - bot, x, core)
    rel_peers = (other_core, other_y, at(3 - y, x, core), at(y, x + 1 - 2 * (x % 2), core), at(y, x_size - 1 - x, core), other_core)
    grad_to = place((mine + step) % groups, turned(step), core)
    grad_from = place((mine + groups - step) % groups, turned(step), core)
    nxt = step + 1
    table_to = place((mine + groups - nxt) % groups, turned(nxt), core)
    table_from = place((mine + nxt) % groups, turned(nxt), core)
    peers = list(rel_peers)
    if step:
        peers += [grad_to, grad_from]
    if last:
        for turn in range(4):
            peers.append(at((y + turn) % 4, x, top))
        senders = [at((2 * core + d), x, c) for d in range(2) for c in range(2)]
        peers += senders
    else:
        peers += [table_to, table_from]
    entry(peers)
    keep = turned(step)
    pending = []

    def start(copy):
        copy.start()
        pending.append(copy)
        return copy

    shards = [(1 - keep, k) for k in range(chunks)] + [(keep, k) for k in range(chunks)]
    loads, cores = [], []
    row_loads = [pltpu.make_async_copy(src, dst, row_sem.at[n]) for n, (src, dst) in enumerate(((head_hbm, head_ref), (ent_hbm, ent_ref)))]
    for load in row_loads:
        load.start()
    stores = []

    def store(n, src, dst):
        copy = pltpu.make_async_copy(src, dst, store_sem.at[n])
        copy.start()
        stores.append(copy)

    def store_table(low, c, k):
        slot = slot_of(low, c, k)
        store(slot, table.at[slot], table_hbm.at[slot])

    rel_copies = [start(remote(rel_grad_ref.at[1 - core], rel_from.at[0], rel_send.at[0], rel_recv.at[0], rel_peers[0]))]
    for n, (low, k) in enumerate(shards):
        cores.append(start(remote(tail_ref.at[slot_of(low, 1 - core, k)], from_core.at[n], core_send.at[n], core_recv.at[n], other_core)))
        load = pltpu.make_async_copy(tail_ref.at[slot_of(low, core, k)], own.at[n], own_sem.at[n])
        load.start()
        loads.append(load)

    def rel_step(n):
        rel_copies[n].wait_recv()
        rel_sum[n] = (rel_grad_ref[core] if n == 0 else rel_sum[n - 1]) + rel_from[n]
        rel_copies.append(start(remote(rel_sum.at[n], rel_from.at[n + 1], rel_send.at[n + 1], rel_recv.at[n + 1], rel_peers[n + 1])))

    ys = []
    for k in range(chunks):
        loads[k].wait()
        cores[k].wait_recv()
        own[k] = own[k] + from_core[k]
        ys.append(start(remote(own.at[k], from_y.at[k], y_send.at[k], y_recv.at[k], other_y)))
        if k == 1:
            rel_step(0)
    for k in range(chunks, 2 * chunks):
        loads[k].wait()
        cores[k].wait_recv()
        own[k] = own[k] + from_core[k]
    gs, outs, forwards, crosses = [], [], [], []

    def stage_group(k):
        ys[k].wait_recv()
        own[chunks + k] = own[chunks + k] + from_y[k]
        if step:
            gs.append(start(remote(own.at[chunks + k], from_group.at[k], group_send.at[k], group_recv.at[k], grad_to)))

    def cross_copy(k):
        slot = slot_of(bot, core, k)
        return remote(send_buf.at[k], ent_wire.at[slot], out_send.at[2 * chunks + k], out_recv.at[slot], other_core)

    turn = (y + 4 - 2 * core) % 4
    near = 1 - turn % 2
    back = jnp.where((turn == 1) | (turn == 2), 0, 1)
    onward = at((y + 1 + 2 * back) % 4, x, core)

    def landed(low, c, k):
        slot = slot_of(low, c, k)
        remote(ent_wire.at[slot], ent_wire.at[slot], out_send.at[0], out_recv.at[slot], other_core).wait_recv()

    def stage_relay(k):
        if k % 2 == 0:
            return
        for c in CORES:
            landed(near, c, k - 1)
            landed(near, c, k)
            slot = slot_of(near, c, k) - 1 + back
            start(remote(ent_wire.at[slot], ent_wire.at[slot], out_send.at[(3 + c) * chunks + k], out_recv.at[slot], onward))

    def stage_update(k):
        if k == 0:
            for load in row_loads:
                load.wait()
        if step:
            gs[k].wait_recv()
        total = from_group if step else own
        base = k if step else chunks + k
        grad = [total[base, band(t, chunk), :] + head_ref[k, band(t, chunk), :] for t in TILES[:-1]]
        grad.append(below(unfold_last(total[base, 3 * chunk:, :] + head_ref[k, 3 * chunk:, :])))
        span = band(k, chunk)
        rows, state = adagrad(tiles_at(ent_ref, k * chunk, chunk), state_ref[span, :], grad, emb_width, learn_rate)
        wire = rows[:3] + [fold_last(rows[3])]
        if last:
            lane = lanes((chunk, LANES))
            wire.append(fold_last(jnp.where(lane < 1, state, 0.0)))
        else:
            wide = band(k, 4 * chunk)
            ent_ref[wide, :] = stack_tiles(rows)
            store(4 * chunks + k, ent_ref.at[wide], ent_out.at[wide])
            state_out[span, :] = state
        offset = 0
        for piece in wire:
            send_buf[k, offset:offset + piece.shape[0], :] = piece.astype(send_buf.dtype)
            offset += piece.shape[0]
        slot = slot_of(bot, core, k)
        if last:
            for n, turn in enumerate((1, 3)):
                start(remote(send_buf.at[k], ent_wire.at[slot], out_send.at[n * chunks + k], out_recv.at[slot], at((y + turn) % 4, x, top)))

            @pl.when(core == top)
            def _():
                pltpu.make_async_copy(send_buf.at[k], ent_wire.at[slot], out_recv.at[slot]).start()

            @pl.when(core != top)
            def _():
                cross_copy(k).start()
        else:
            outs.append(start(remote(send_buf.at[k], table.at[slot], out_send.at[k], out_recv.at[k], table_to)))

    def forward(n, low, k, peer):
        slot = slot_of(low, core, k)
        return start(remote(table.at[slot], table.at[slot], out_send.at[n * chunks + k], out_recv.at[n * chunks + k], peer))

    def stage_forward(k):
        outs[k].wait_recv()
        store_table(turned(nxt), core, k)
        forwards.append(forward(1, turned(nxt), k, other_y))
        crosses.append((forward(2, turned(nxt), k, other_core), turned(nxt), k))

    def stage_cross(k):
        forwards[k].wait_recv()
        store_table(1 - turned(nxt), core, k)
        crosses.append((forward(3, 1 - turned(nxt), k, other_core), 1 - turned(nxt), k))

    stages = (stage_group, stage_update, stage_relay) if last else (stage_group, stage_update, stage_forward, stage_cross)
    rel_steps = len(rel_peers) - 1
    far = groups <= 4 * step < 3 * groups
    lags = FAR_LAGS if far else LAGS
    rel_ticks = (1, 3, chunks, chunks + 3)
    for tick in range(chunks + lags[len(stages) - 1]):
        for lag, stage in zip(lags, stages):
            if 0 <= tick - lag < chunks:
                stage(tick - lag)
        if tick in rel_ticks:
            rel_step(rel_ticks.index(tick) + 1)

    rel_copies[rel_steps].wait_recv()
    halves = rel_sum[rel_steps - 1], rel_from[rel_steps]
    summed = below([jnp.where(core == n, halves[0], halves[1]) for n in CORES])
    rel_grad = [summed[band(t, REL_PAD)] for t in TILES[:-1]] + [below(unfold_last(summed[3 * REL_PAD:]))]
    loss_out[...] = rel_grad[0][REL_PAD - 1:, :]
    row = sublanes((REL_PAD, LANES))
    rel_grad[0] = jnp.where(row < REL_PAD - 1, rel_grad[0], 0.0)
    rel_rows, rel_state = adagrad(tiles_of(rel_ref[...]), rel_state_ref[...], rel_grad, emb_width, learn_rate)
    for t in TILES:
        rel_out[:, band(t, LANES)] = rel_rows[t]
    if not last:
        rel_state_out[...] = rel_state

    if last:
        for c in CORES:
            for k in range(chunks):
                landed(1 - near, c, k)

        @pl.when(core != top)
        def _():
            for k in range(chunks):
                cross_copy(k).wait_send()
    else:
        for copy, low, k in crosses:
            copy.wait_recv()
            store_table(low, 1 - core, k)
        for copy in stores:
            copy.wait()
    for copy in pending:
        copy.wait_send()


def exchange_call(step, groups, emb_width, tail, head, rel_grad, ent, state, rel, rel_state):
    vmem, hbm = pl.BlockSpec(memory_space=pltpu.VMEM), pl.BlockSpec(memory_space=pl.ANY)
    chunks = head.shape[0]
    rel_grad = rel_grad.reshape(2, -1, LANES)
    wire = wire_rows(CHUNK)
    last = step == groups - 1
    like = lambda x: jax.ShapeDtypeStruct(x.shape, x.dtype)
    loss = jax.ShapeDtypeStruct((1, LANES), F32)
    out_wire = wire + (CHUNK // LEFT if last else 0)
    out_type = F32 if last else BF16
    gathered = jax.ShapeDtypeStruct((4 * chunks, out_wire, LANES), out_type)
    out_shape = (gathered, like(rel), loss) if last else (like(ent), like(state), like(rel), like(rel_state), loss, gathered)
    return pl.pallas_call(
        functools.partial(exchange_kernel, (step, groups, chunks, emb_width, last)),
        out_shape=out_shape,
        in_specs=[hbm, hbm, vmem, hbm, vmem, vmem, vmem],
        out_specs=(vmem,) * 3 if last else (hbm, vmem, vmem, vmem, vmem, hbm),
        scratch_shapes=[
            pltpu.VMEM((2 * chunks, wire, LANES), F32), pltpu.VMEM((2 * chunks, wire, LANES), F32),
            pltpu.VMEM((chunks, wire, LANES), F32), pltpu.VMEM((chunks, wire, LANES), F32),
            pltpu.VMEM((REL_HOPS - 1, *rel_grad.shape[1:]), F32), pltpu.VMEM((REL_HOPS, *rel_grad.shape[1:]), F32),
            pltpu.VMEM((chunks, out_wire, LANES), out_type),
            *[dma_sems(2 * chunks)] * 3, *[dma_sems(chunks)] * 4,
            dma_sems(REL_HOPS), dma_sems(REL_HOPS), dma_sems(5 * chunks), dma_sems(4 * chunks),
            pltpu.VMEM(head.shape, F32), pltpu.VMEM(ent.shape, F32), dma_sems(2),
            *(() if last else (pltpu.VMEM(gathered.shape, BF16), dma_sems(5 * chunks))),
        ],
        compiler_params=pltpu.CompilerParams(vmem_limit_bytes=VMEM_LIMIT, collective_id=step, has_side_effects=True),
        name='exchange',
    )(tail, head, rel_grad, ent, state, rel, rel_state)


def setup_kernel(cfg, head_ref, tail_ref, rel_id_ref, mask_ref, neg_ref, ent_hbm, rel_ref, word_out, rel_id_out, count_out, neg_out, table, ent_out, rel_out,
                 packed, shares, neg_buf, rows_buf, away, send_sem, recv_sem, core_send, core_recv, load_sem, table_send, table_recv):
    head_bits, tail_bits, spare = cfg
    y, x, core, top, bot = where_here()
    home = core == top
    own_shard, other_shard = 2 * bot + core, 2 * bot + 1 - core
    other_core = {'data': y, 'ent': 2 * x + 1 - core}
    users = [(c, 2 * core + d) for c in CORES for d in CORES]
    users = [({'data': row, 'ent': 2 * x + c}, (core == c) & (y == row)) for c, row in users]
    entry([peer for peer, _ in users] + [{'data': row, 'ent': 2 * x + top} for row in TILES] + [other_core])
    edges = head_ref[...] | (tail_ref[...] << tail_bits) | (rel_id_ref[...] << (2 * tail_bits))
    packed[...] = jnp.where(mask_ref[...] > 0, edges, spare << (2 * tail_bits))
    neg_buf[:, 0, :] = row_address(neg_ref[...])
    to_users = [remote(packed, shares.at[y], send_sem.at[n], recv_sem.at[y], peer) for n, (peer, _) in enumerate(users)]
    for copy, (_, here) in zip(to_users, users):
        @pl.when(jnp.logical_not(here))
        def _():
            copy.start()

    chunks, chunk = table.shape[0], CHUNK
    shard = chunks // 4

    def load(n):
        return pltpu.make_async_copy(ent_hbm.at[:, pl.ds(pl.multiple_of(n * chunk, chunk), chunk)], rows_buf.at[n % rows_buf.shape[0]], load_sem.at[n % rows_buf.shape[0]])

    def table_copy(q):
        part = table.at[pl.ds(q * shard, shard)]
        return remote(part, part, table_send.at[q], table_recv.at[q], other_core)

    neg_copy = remote(neg_buf, neg_out, core_send.at[0], core_recv.at[0], other_core)
    ent_copy = remote(away, ent_out, core_send.at[1], core_recv.at[1], other_core)

    @pl.when(home)
    def _():
        pltpu.make_async_copy(packed, shares.at[y], recv_sem.at[y]).start()
        neg_copy.start()
        neg_out[...] = neg_buf[...]
        for n in range(AHEAD):
            load(n).start()
        for q in TILES:
            def one(pair, carry):
                first = 2 * pair
                for c in CORES:
                    n = q * shard + first + c

                    @pl.when(n + AHEAD < chunks)
                    def _():
                        load(n + AHEAD).start()

                    load(n).wait()
                both = [(first + c, columns_to_tiles(rows_buf[(q * shard + first + c) % rows_buf.shape[0]])) for c in CORES]
                for k, tiles in both:
                    n = q * shard + k
                    for t in TILES[:-1]:
                        table[n, band(t, chunk), :] = tiles[t].astype(BF16)
                    table[n, 3 * chunk:, :] = fold_last(tiles[3]).astype(BF16)
                    rows = stack_tiles(tiles)
                    place = pl.ds(pl.multiple_of(k * chunk * 4, chunk * 4), chunk * 4)

                    @pl.when(own_shard == q)
                    def _():
                        ent_out[place, :] = rows

                    @pl.when(other_shard == q)
                    def _():
                        away[place, :] = rows

                return carry

            lax.fori_loop(0, shard // 2, one, 0)
            table_copy(q).start()

            @pl.when(other_shard == q)
            def _():
                ent_copy.start()

    for t, tile in enumerate(columns_to_tiles(rel_ref[...])):
        rel_out[:, band(t, LANES)] = tile
    for row in TILES:
        remote(packed, shares.at[row], send_sem.at[0], recv_sem.at[row], other_core).wait_recv()
    share = beside([shares[row] for row in TILES])
    mine = ((share >> head_bits) & 3 == own_shard) & (share >> (2 * tail_bits) != spare)
    lane = lanes(share.shape)
    width = share.shape[1]
    steps = (width - 1).bit_length()
    other = jnp.where(mine, 0, 1)
    before = other
    for bit in range(steps):
        before = before + jnp.where(lane < 2**bit, 0, roll(before, 2**bit))
    count_out[...] = jnp.broadcast_to(width - before[:, width - 1:], count_out.shape)
    none = spare << (head_bits + tail_bits)
    edge = jnp.where(mine, (share & (2**head_bits - 1)) | (share >> tail_bits << head_bits), none)
    shift = jnp.where(mine, before - other, 0)
    for bit in range(steps):
        here = (shift >> bit) & 1 == 1
        edge_in, shift_in = roll(edge, width - 2**bit), roll(shift, width - 2**bit)
        there = (shift_in >> bit) & 1 == 1
        edge = jnp.where(there, edge_in, jnp.where(here, none, edge))
        shift = jnp.where(there, shift_in, jnp.where(here, 0, shift))
    rel_id_out[:, 0, :] = edge >> (head_bits + tail_bits)
    head, tail = edge & (2**head_bits - 1), (edge >> head_bits) & (2**tail_bits - 1)
    margin = jnp.zeros((share.shape[0], BLOCK), jnp.int32)
    word_out[:, 0, :] = beside([margin, (row_address(head) << (tail_bits + 2)) | row_address(tail), margin])
    for copy, (_, here) in zip(to_users, users):
        @pl.when(jnp.logical_not(here))
        def _():
            copy.wait_send()

    between = [neg_copy, ent_copy, *(table_copy(q) for q in TILES)]

    @pl.when(home)
    def _():
        for copy in between:
            copy.wait_send()

    @pl.when(jnp.logical_not(home))
    def _():
        for copy in between:
            copy.wait_recv()


def setup_call(cfg, head, tail, rel_ids, mask, neg, reps, ent, rel):
    vmem, hbm = pl.BlockSpec(memory_space=pltpu.VMEM), pl.BlockSpec(memory_space=pl.ANY)
    groups, share = head.shape
    width, rows = ent.shape
    chunks = rows // CHUNK
    return pl.pallas_call(
        functools.partial(setup_kernel, cfg),
        out_shape=(*(jax.ShapeDtypeStruct(shape, jnp.int32) for shape in ((groups, 1, reps * share + 2 * BLOCK), (groups, 1, reps * share), (groups, LANES), (groups, 1, neg.shape[1]))),
                   jax.ShapeDtypeStruct((chunks, wire_rows(CHUNK), LANES), BF16), jax.ShapeDtypeStruct((rows, LANES), F32), jax.ShapeDtypeStruct((REL_PAD, 4 * LANES), F32)),
        in_specs=[*[vmem] * 5, hbm, vmem],
        out_specs=(vmem,) * 7,
        scratch_shapes=[pltpu.VMEM(head.shape, jnp.int32), pltpu.VMEM((reps, *head.shape), jnp.int32), pltpu.VMEM((groups, 1, neg.shape[1]), jnp.int32),
                        pltpu.VMEM((AHEAD + 2, width, CHUNK), F32), pltpu.VMEM((rows, LANES), F32), *[dma_sems(4)] * 2, *[dma_sems(2)] * 2, dma_sems(AHEAD + 2), *[dma_sems(4)] * 2],
        compiler_params=pltpu.CompilerParams(collective_id=20, has_side_effects=True),
        name='setup',
    )(head, tail, rel_ids, mask, neg, ent, rel)


def finish_kernel(wire_ref, rel_ref, ent_out, state_out, rel_out):
    chunk = CHUNK
    for n in range(wire_ref.shape[0]):
        tiles = [wire_ref[n, band(t, chunk), :] for t in TILES[:-1]]
        tiles.append(below(unfold_last(wire_ref[n, 3 * chunk:wire_rows(chunk), :])))
        ent_out[:, band(n, chunk)] = tiles_to_columns(tiles)
        state = below([part[:, :1] for part in unfold_last(wire_ref[n, wire_rows(chunk):, :])])
        state_out[:, band(n, chunk)] = column_sum(jnp.where(on_diagonal(chunk), state, 0.0))

    @pl.when(pl.program_id(0) == 0)
    def _():
        rel_out[...] = tiles_to_columns(tiles_of(rel_ref[...]))


def finish_call(wire, rel, width):
    chunks = wire.shape[0]
    size = chunks // 8
    whole = lambda n: (0, 0)
    return pl.pallas_call(
        finish_kernel,
        out_shape=tuple(jax.ShapeDtypeStruct(shape, F32) for shape in ((width, chunks * CHUNK), (1, chunks * CHUNK), (width, REL_PAD))),
        grid=(chunks // size,),
        in_specs=[pl.BlockSpec((size, *wire.shape[1:]), lambda n: (n, 0, 0)), pl.BlockSpec(rel.shape, whole)],
        out_specs=(pl.BlockSpec((width, size * CHUNK), lambda n: (0, n)), pl.BlockSpec((1, size * CHUNK), lambda n: (0, n)), pl.BlockSpec((width, REL_PAD), whole)),
        name='finish',
    )(wire, rel)


def solution(mesh):
    groups = mesh.shape['ent']
    data_reps = mesh.shape['data']
    row_spec = P(('sweep', 'ent'), None)
    edge_spec = P(('sweep', 'ent'), None, 'data')

    def device_fn(ent_table, ent_state, rel_table, head_idx, tail_idx, rel_idx, edge_mask, neg_idx):
        part_rows, emb_width = ent_table.shape
        rel_rows = rel_table.shape[0]
        bucket_edges = head_idx.shape[2] * data_reps
        shard = part_rows // 4
        tail_bits = (part_rows - 1).bit_length()
        head_bits = (shard - 1).bit_length()
        spare = 2**(REL_PAD - 1).bit_length() - 1
        ent = lax.axis_index('ent')
        _, _, core, top, bot = where_here()

        words, rel_ids, counts, neg, table, ent_now, rel_now = setup_call(
            (head_bits, tail_bits, spare), head_idx[0], tail_idx[0], rel_idx[0], edge_mask[0], neg_idx[0], data_reps,
            ent_table.T, jnp.pad(rel_table.T, ((0, 0), (0, REL_PAD - rel_rows))))
        to_core = lambda c: lax.dynamic_slice_in_dim(ent_state, (2 * bot + c) * shard, shard)
        away = [(d * groups + 2 * (n // 2) + d // 2, d * groups + 2 * (n // 2) + 1 - d // 2) for d in range(data_reps) for n in range(0, groups, 2)]
        state_now = jnp.where(core == top, to_core(core), lax.ppermute(to_core(1 - core), ('data', 'ent'), away))[:, None]
        rel_state = jnp.zeros((REL_PAD, 1), F32)
        losses = []
        for step in range(groups):
            tail, head, rel_grad = bucket_call(step, tail_bits + 2, words, counts, neg, rel_ids, ent_now, rel_now, table)
            out = exchange_call(step, groups, emb_width, tail, head, rel_grad, ent_now, state_now, rel_now, rel_state)
            if step + 1 < groups:
                ent_now, state_now, rel_now, rel_state, loss, table = out
            else:
                wire, rel_now, loss = out
            losses.append(loss)
        ent_out, state_out, rel_out = finish_call(wire, rel_now, emb_width)
        loss_rows = below(losses) / bucket_edges
        bucket_loss = lax.dynamic_slice_in_dim(loss_rows, ent, 1, axis=1).reshape(1, groups)
        return ent_out.T, state_out[0], rel_out[:, :rel_rows].T, bucket_loss

    return jax.shard_map(device_fn, mesh=mesh, in_specs=(row_spec, P(('sweep', 'ent')), P('sweep', None), edge_spec, edge_spec, edge_spec, edge_spec, P(('sweep', 'ent'), None, None)), out_specs=(row_spec, P(('sweep', 'ent')), P('sweep', None), row_spec), check_vma=False)
```
